16 devices in a mesh: tp: 2 (over z), ep: 8 (over y, x, core).
Axes of the slice: x: 2, y: 2, z: 2, core: 2. Of those that a mesh axis runs over, the one named last changes fastest.
Arguments:
- hidden_in: bfloat16 [1536, 2048], P(('tp', 'ep'))
- cache0: bfloat16 [1536, 256, 576], P(('tp', 'ep'))
- cache1: bfloat16 [1536, 256, 576], P(('tp', 'ep'))
- kv_lens: int32 [1536], P(('tp', 'ep'))
- route_ids: int32 [1536, 6], P(('tp', 'ep'))
- route_wts: float32 [1536, 6], P(('tp', 'ep'))
- att0_q: bfloat16 [2048, 16, 192], replicated
- att0_uk: bfloat16 [16, 128, 512], replicated
- att0_uv: bfloat16 [16, 512, 128], replicated
- att0_o: bfloat16 [16, 128, 2048], replicated
- att1_q: bfloat16 [2048, 16, 192], replicated
- att1_uk: bfloat16 [16, 128, 512], replicated
- att1_uv: bfloat16 [16, 512, 128], replicated
- att1_o: bfloat16 [16, 128, 2048], replicated
- ffn0_gate: bfloat16 [2048, 10944], P(None, 'tp')
- ffn0_up: bfloat16 [2048, 10944], P(None, 'tp')
- ffn0_down: bfloat16 [10944, 2048], P('tp')
- ffn1_gate: bfloat16 [2048, 10944], P(None, 'tp')
- ffn1_up: bfloat16 [2048, 10944], P(None, 'tp')
- ffn1_down: bfloat16 [10944, 2048], P('tp')
- exp_gate: bfloat16 [16, 2048, 1408], P(('tp', 'ep'))
- exp_up: bfloat16 [16, 2048, 1408], P(('tp', 'ep'))
- exp_down: bfloat16 [16, 1408, 2048], P(('tp', 'ep'))
Outputs:
- output: bfloat16 [1536, 2048], P(('tp', 'ep'))
All inputs are finite; a program needn't handle non-finite values.
Results may differ from the reference program's by a relative error of at most 0.0155603.
Values are sent between devices in bfloat16 or wider.
A program may use at most 1 GiB of HBM per device.

```python
import jax
import jax.numpy as jnp
from jax import lax

HIDDEN = 2048
NUM_HEADS = 16
NOPE_DIM = 128
ROPE_DIM = 64
VALUE_DIM = 128
LATENT = 512
TOP_K = 6
FF_EXPERT = 1408
FF_DENSE = 10944
TOK_DEV = 96
KV_LEN = 256
ZERO_EXPERTS = 128
DEVICES = 16

NUM_TOKENS = TOK_DEV * DEVICES
SLOT_CAP = min(TOK_DEV, (2 * TOK_DEV * TOP_K + DEVICES - 1) // DEVICES)
ROWS_MAX = DEVICES * SLOT_CAP
NUM_HOT = max(1, DEVICES // 16)
COLD_SLOTS = (TOK_DEV * TOP_K * 3) // 5 - NUM_HOT * SLOT_CAP
SCALE = (NOPE_DIM + ROPE_DIM) ** -0.5


def draw_normal(key, shape, scale):
    return (jax.random.normal(key, shape, jnp.float32) * scale).astype(jnp.bfloat16)


def draw_routes(key):
    key_hot, key_src = jax.random.split(key)
    dev_order = jax.random.permutation(key_hot, DEVICES)
    hot_flag = jnp.zeros((DEVICES,), jnp.int32).at[dev_order[:NUM_HOT]].set(1)
    cold_devs = dev_order[NUM_HOT:]

    def one_source(src):
        src_key = jax.random.fold_in(key_src, src)
        key_pick, key_zero, key_perm = jax.random.split(src_key, 3)
        cold_pick = cold_devs[jax.random.randint(key_pick, (COLD_SLOTS,), 0, DEVICES - NUM_HOT)]
        dev_counts = jax.ops.segment_sum(jnp.ones((COLD_SLOTS,), jnp.int32), cold_pick, num_segments=DEVICES)
        dev_counts = jnp.where(hot_flag == 1, SLOT_CAP, jnp.minimum(dev_counts, SLOT_CAP))
        dev_bounds = jnp.cumsum(dev_counts)
        dest_dev = jnp.searchsorted(dev_bounds, jnp.arange(TOK_DEV * TOP_K), side='right').astype(jnp.int32)
        dest_dev = dest_dev.reshape(TOP_K, TOK_DEV).T
        zero_base = jax.random.randint(key_zero, (TOK_DEV, 1), 0, ZERO_EXPERTS)
        zero_ids = DEVICES + (jnp.arange(TOP_K)[None, :] + zero_base) % ZERO_EXPERTS
        slot_ids = jnp.where(dest_dev < DEVICES, dest_dev, zero_ids).astype(jnp.int32)
        return slot_ids[jax.random.permutation(key_perm, TOK_DEV)]

    return jax.vmap(one_source)(jnp.arange(DEVICES)).reshape(NUM_TOKENS, TOP_K)


def draw_lengths(key):
    lengths = jax.random.randint(key, (NUM_TOKENS,), KV_LEN // 8, KV_LEN + 1)
    return lengths.at[0].set(KV_LEN).astype(jnp.int32)


def setup_inputs(seed: int = 0) -> dict:
    keys = jax.random.split(jax.random.key(seed), 26)
    qk_dim = NOPE_DIM + ROPE_DIM
    uv_scale = LATENT ** -0.5 * KV_LEN ** 0.5 / 4.0
    return {
        'hidden_in': draw_normal(keys[0], (NUM_TOKENS, HIDDEN), 1.0),
        'cache0': draw_normal(keys[1], (NUM_TOKENS, KV_LEN, LATENT + ROPE_DIM), 1.0),
        'cache1': draw_normal(keys[2], (NUM_TOKENS, KV_LEN, LATENT + ROPE_DIM), 1.0),
        'kv_lens': draw_lengths(keys[3]),
        'route_ids': draw_routes(keys[4]),
        'route_wts': jax.random.uniform(keys[5], (NUM_TOKENS, TOP_K), jnp.float32, 0.5, 1.5) * (2.0 / TOP_K),
        'att0_q': draw_normal(keys[6], (HIDDEN, NUM_HEADS, qk_dim), HIDDEN ** -0.5),
        'att0_uk': draw_normal(keys[7], (NUM_HEADS, NOPE_DIM, LATENT), NOPE_DIM ** -0.5),
        'att0_uv': draw_normal(keys[8], (NUM_HEADS, LATENT, VALUE_DIM), uv_scale),
        'att0_o': draw_normal(keys[9], (NUM_HEADS, VALUE_DIM, HIDDEN), (NUM_HEADS * VALUE_DIM) ** -0.5),
        'att1_q': draw_normal(keys[10], (HIDDEN, NUM_HEADS, qk_dim), HIDDEN ** -0.5),
        'att1_uk': draw_normal(keys[11], (NUM_HEADS, NOPE_DIM, LATENT), NOPE_DIM ** -0.5),
        'att1_uv': draw_normal(keys[12], (NUM_HEADS, LATENT, VALUE_DIM), uv_scale),
        'att1_o': draw_normal(keys[13], (NUM_HEADS, VALUE_DIM, HIDDEN), (NUM_HEADS * VALUE_DIM) ** -0.5),
        'ffn0_gate': draw_normal(keys[14], (HIDDEN, FF_DENSE), HIDDEN ** -0.5),
        'ffn0_up': draw_normal(keys[15], (HIDDEN, FF_DENSE), HIDDEN ** -0.5),
        'ffn0_down': draw_normal(keys[16], (FF_DENSE, HIDDEN), FF_DENSE ** -0.5),
        'ffn1_gate': draw_normal(keys[17], (HIDDEN, FF_DENSE), HIDDEN ** -0.5),
        'ffn1_up': draw_normal(keys[18], (HIDDEN, FF_DENSE), HIDDEN ** -0.5),
        'ffn1_down': draw_normal(keys[19], (FF_DENSE, HIDDEN), FF_DENSE ** -0.5),
        'exp_gate': draw_normal(keys[20], (DEVICES, HIDDEN, FF_EXPERT), HIDDEN ** -0.5),
        'exp_up': draw_normal(keys[21], (DEVICES, HIDDEN, FF_EXPERT), HIDDEN ** -0.5),
        'exp_down': draw_normal(keys[22], (DEVICES, FF_EXPERT, HIDDEN), 2.0 * FF_EXPERT ** -0.5),
    }


def rms_norm(vec):
    vec32 = vec.astype(jnp.float32)
    return (vec32 * lax.rsqrt(jnp.mean(vec32 * vec32, axis=-1, keepdims=True) + 1e-6)).astype(jnp.bfloat16)


def rope_rotate(vals, pos):
    half_dim = vals.shape[-1] // 2
    inv_freq = 10000.0 ** (-2.0 * jnp.arange(half_dim, dtype=jnp.float32) / vals.shape[-1])
    rot_angle = pos.astype(jnp.float32)[..., None, None] * inv_freq
    cos_ang = jnp.cos(rot_angle)
    sin_ang = jnp.sin(rot_angle)
    lead_half = vals[..., :half_dim]
    tail_half = vals[..., half_dim:]
    return jnp.concatenate([lead_half * cos_ang - tail_half * sin_ang, tail_half * cos_ang + lead_half * sin_ang], axis=-1)


def swiglu(rows, w_gate, w_up, w_down):
    gate_val = jnp.dot(rows, w_gate, preferred_element_type=jnp.float32)
    up_val = jnp.dot(rows, w_up, preferred_element_type=jnp.float32)
    act_val = (jax.nn.silu(gate_val) * up_val).astype(jnp.bfloat16)
    return jnp.dot(act_val, w_down, preferred_element_type=jnp.float32)


def attention(normed, cache, kv_lens, w_q, w_uk, w_uv, w_o):
    wq32 = w_q.astype(jnp.float32)
    wuk32 = w_uk.astype(jnp.float32)
    wuv32 = w_uv.astype(jnp.float32)
    wo32 = w_o.astype(jnp.float32)

    def one_token(item):
        vec, kv_rows, length = item
        q_full = jnp.einsum('d,dhc->hc', vec.astype(jnp.float32), wq32).astype(jnp.bfloat16)
        q_rope = rope_rotate(q_full[:, NOPE_DIM:].astype(jnp.float32), length).astype(jnp.bfloat16)
        q_lat = jnp.einsum('hn,hnl->hl', q_full[:, :NOPE_DIM].astype(jnp.float32), wuk32).astype(jnp.bfloat16)
        q_cat = jnp.concatenate([q_lat, q_rope], axis=1)
        scores = jnp.dot(q_cat, kv_rows.T, preferred_element_type=jnp.float32) * SCALE
        valid = jnp.arange(KV_LEN)[None, :] < length
        probs = jax.nn.softmax(jnp.where(valid, scores, -1e30), axis=-1).astype(jnp.bfloat16)
        o_lat = jnp.dot(probs, kv_rows[:, :LATENT], preferred_element_type=jnp.float32).astype(jnp.bfloat16)
        o_val = jnp.einsum('hl,hlv->hv', o_lat.astype(jnp.float32), wuv32).astype(jnp.bfloat16)
        return jnp.einsum('hv,hvd->d', o_val.astype(jnp.float32), wo32)

    return lax.map(one_token, (normed, cache, kv_lens))


def expert_mix(normed, route_ids, route_wts, exp_gate, exp_up, exp_down):
    flat_ids = route_ids.reshape(-1)
    flat_wts = route_wts.reshape(-1)
    num_slots = flat_ids.shape[0]
    key_ids = jnp.where(flat_ids < DEVICES, flat_ids, DEVICES)
    slot_order = jnp.argsort(key_ids, stable=True)
    counts = jax.ops.segment_sum(jnp.ones_like(key_ids), key_ids, num_segments=DEVICES + 1)
    starts = jnp.cumsum(counts) - counts
    local_pos = jnp.arange(ROWS_MAX)

    def one_expert(carry, item):
        start, count, w_gate, w_up, w_down = item
        slot_idx = slot_order[jnp.minimum(start + local_pos, num_slots - 1)]
        tok_idx = slot_idx // TOP_K
        exp_out = swiglu(normed[tok_idx], w_gate, w_up, w_down).astype(jnp.bfloat16)
        slot_wt = jnp.where(local_pos < count, flat_wts[slot_idx], 0.0)
        return carry.at[tok_idx].add(slot_wt[:, None] * exp_out.astype(jnp.float32)), None

    mix_init = jnp.zeros((NUM_TOKENS, HIDDEN), jnp.float32)
    mix, _ = lax.scan(one_expert, mix_init, (starts[:DEVICES], counts[:DEVICES], exp_gate, exp_up, exp_down))
    zero_wt = jnp.sum(jnp.where(route_ids >= DEVICES, route_wts, 0.0), axis=1)
    return mix + zero_wt[:, None] * normed.astype(jnp.float32)


def reference(hidden_in, cache0, cache1, kv_lens, route_ids, route_wts, att0_q, att0_uk, att0_uv, att0_o, att1_q, att1_uk, att1_uv, att1_o, ffn0_gate, ffn0_up, ffn0_down, ffn1_gate, ffn1_up, ffn1_down, exp_gate, exp_up, exp_down):
    att_zero = attention(rms_norm(hidden_in), cache0, kv_lens, att0_q, att0_uk, att0_uv, att0_o)
    h_zero = (hidden_in.astype(jnp.float32) + att_zero).astype(jnp.bfloat16)
    u_zero = rms_norm(h_zero)
    f_zero = (h_zero.astype(jnp.float32) + swiglu(u_zero, ffn0_gate, ffn0_up, ffn0_down)).astype(jnp.bfloat16)
    att_one = attention(rms_norm(f_zero), cache1, kv_lens, att1_q, att1_uk, att1_uv, att1_o)
    h_one = (f_zero.astype(jnp.float32) + att_one).astype(jnp.bfloat16)
    mix = expert_mix(u_zero, route_ids, route_wts, exp_gate, exp_up, exp_down)
    dense_one = swiglu(rms_norm(h_one), ffn1_gate, ffn1_up, ffn1_down)
    return (h_one.astype(jnp.float32) + dense_one + mix).astype(jnp.bfloat16)
```

```python
import functools

import jax
import jax.numpy as jnp
from jax import lax
from jax.experimental import pallas as pl
from jax.experimental.pallas import tpu as pltpu
from jax.sharding import PartitionSpec as P

FLAT_AXES = ('tp', 'ep')
MESH = pl.DeviceIdType.MESH
F32, BF16 = jnp.float32, jnp.bfloat16
SLOT_CAP = 72
VMEM_LIMIT = 66_000_000


def rms_norm(vec):
    vec32 = vec.astype(F32)
    return (vec32 * lax.rsqrt(jnp.mean(vec32 * vec32, axis=-1, keepdims=True) + 1e-6)).astype(BF16)


def rope_rotate(vals, pos):
    half_dim = vals.shape[-1] // 2
    inv_freq = 10000.0 ** (-2.0 * jnp.arange(half_dim, dtype=F32) / vals.shape[-1])
    rot_angle = pos.astype(F32)[..., None, None] * inv_freq
    cos_ang = jnp.cos(rot_angle)
    sin_ang = jnp.sin(rot_angle)
    lead_half = vals[..., :half_dim]
    tail_half = vals[..., half_dim:]
    return jnp.concatenate([lead_half * cos_ang - tail_half * sin_ang, tail_half * cos_ang + lead_half * sin_ang], axis=-1)


def attention(normed, cache, kv_lens, w_q, w_uk, w_uv, w_o):
    nope_dim = w_uk.shape[1]
    latent = w_uk.shape[2]
    scale = w_q.shape[2] ** -0.5
    q_full = jnp.einsum('bd,dhc->bhc', normed, w_q, preferred_element_type=F32).astype(BF16)
    q_rope = rope_rotate(q_full[..., nope_dim:].astype(F32), kv_lens).astype(BF16)
    q_lat = jnp.einsum('bhn,hnl->bhl', q_full[..., :nope_dim], w_uk, preferred_element_type=F32).astype(BF16)
    q_cat = jnp.concatenate([q_lat, q_rope], axis=-1)
    scores = jnp.einsum('bhc,bpc->bhp', q_cat, cache, preferred_element_type=F32) * scale
    valid = jnp.arange(cache.shape[1])[None, None, :] < kv_lens[:, None, None]
    probs = jax.nn.softmax(jnp.where(valid, scores, -1e30), axis=-1).astype(BF16)
    o_lat = jnp.einsum('bhp,bpl->bhl', probs, cache[:, :, :latent], preferred_element_type=F32).astype(BF16)
    o_val = jnp.einsum('bhl,hlv->bhv', o_lat, w_uv, preferred_element_type=F32).astype(BF16)
    return jnp.einsum('bhv,hvd->bd', o_val, w_o, preferred_element_type=F32)


def dot_t(lhs, rhs):
    return lax.dot_general(lhs, rhs, (((1,), (1,)), ((), ())), preferred_element_type=F32)


def dot_n(lhs, rhs):
    return jnp.dot(lhs, rhs, preferred_element_type=F32)


TILE = 512
COLS = 256


def ffn_kernel(with_expert, n_buf, d_buf, *refs):
    refs = list(refs)
    u_ref, h_ref, gate_hbm, up_hbm, down_hbm = refs[:5]
    del refs[:5]
    if with_expert:
        eg_hbm, eu_hbm, ed_hbm = refs[:3]
        del refs[:3]
    out_ref = refs.pop(0)
    if with_expert:
        eo_hbm = refs.pop(0)
    rows_ref, act_ref, gate_ring, up_ring, down_ring, send_buf, recv_buf, part_buf = refs[:8]
    ring_sem, down_sem, ex_send, ex_recv, rs_send, rs_recv = refs[8:14]
    if with_expert:
        blocks, eg, eu, ed, x_buf, h_buf, e_buf, ew_sem, eo_sem = refs[14:]
    else:
        blocks, = refs[14:]

    tok, hid = h_ref.shape
    ff = gate_hbm.shape[0]
    n_full, tail = ff // TILE, ff % TILE
    n_step = n_full + 1
    n_col = hid // COLS
    k_main = (ff // 256) * 256

    z = lax.axis_index('tp')
    e = lax.axis_index('ep')
    y, x, c = e // 4, (e // 2) % 2, e % 2
    zn = (1 - z, e)
    me = z * 8 + e
    z_blk = (1 - z) * 8 + e

    def ring_copies(step, slot, rows):
        src = pl.ds(step * TILE, rows)
        return [pltpu.make_async_copy(hbm.at[src], ring.at[slot, pl.ds(0, rows)], ring_sem.at[k, slot])
                for k, (hbm, ring) in enumerate(((gate_hbm, gate_ring), (up_hbm, up_ring)))]

    def down_copy(col, slot):
        return pltpu.make_async_copy(down_hbm.at[:, pl.ds(col * COLS, COLS)], down_ring.at[slot], down_sem.at[slot])

    for step in range(n_buf):
        for cp in ring_copies(step, step, TILE):
            cp.start()
    for col in range(d_buf):
        down_copy(col, col).start()
    if with_expert:
        expert_cps = [pltpu.make_async_copy(s.at[0], d, ew_sem.at[k])
                      for k, (s, d) in enumerate(((eg_hbm, eg), (eu_hbm, eu), (ed_hbm, ed)))]
        for cp in expert_cps:
            cp.start()

    if with_expert:
        xn = (z, e + 2 - 4 * x)
        yn = (z, e + 4 - 8 * y)
        cn = (z, e + 1 - 2 * c)
        peers = (zn, xn, yn, cn)
    else:
        peers = (zn,)
    barrier = pltpu.get_barrier_semaphore()
    for peer in peers:
        pl.semaphore_signal(barrier, inc=1, device_id=peer, device_id_type=MESH)
    pl.semaphore_wait(barrier, len(peers))

    def remote(k, src, dst, peer):
        return pltpu.make_async_remote_copy(src_ref=src, dst_ref=dst, send_sem=ex_send.at[k], recv_sem=ex_recv.at[k],
                                            device_id=peer, device_id_type=MESH)

    if with_expert:
        half = tok // 2
        lo, hi = pl.ds(0, half), pl.ds(half, half)

        def plane(z_at):
            base = z_at * 8
            own = base + e
            xb = base + e + 2 - 4 * x
            yb = base + e + 4 - 8 * y
            db = base + (1 - y) * 4 + (1 - x) * 2 + c
            return own, xb, yb, db

        pa = plane(z)
        pb = plane(1 - z)
        z_copy = remote(0, u_ref, blocks.at[me], zn)
        z_copy.start()
        own_cp = pltpu.make_async_copy(u_ref, blocks.at[me], eo_sem.at[0])
        own_cp.start()

        def plane_sends(first, blks, own_src):
            own, xb, yb, db = blks
            return {
                'x': remote(first, own_src, blocks.at[own], xn),
                'y': remote(first + 1, own_src, blocks.at[own], yn),
                'xr': remote(first + 2, blocks.at[yb, hi], blocks.at[yb, hi], xn),
                'yr': remote(first + 3, blocks.at[xb, lo], blocks.at[xb, lo], yn),
                'c0': remote(first + 4, own_src, blocks.at[own], cn),
                'c1': remote(first + 5, blocks.at[xb], blocks.at[xb], cn),
                'c2': remote(first + 6, blocks.at[yb], blocks.at[yb], cn),
                'c3': remote(first + 7, blocks.at[db], blocks.at[db], cn),
            }

        sa = plane_sends(1, pa, u_ref)
        sb = plane_sends(9, pb, blocks.at[z_blk])

        def start_a0():
            sa['x'].start()
            sa['y'].start()
            sa['c0'].start()

        def start_relay(s):
            s['x'].wait_recv()
            s['y'].wait_recv()
            s['xr'].start()
            s['yr'].start()
            s['c1'].start()
            s['c2'].start()

        def start_last(s):
            s['xr'].wait_recv()
            s['yr'].wait_recv()
            s['c3'].start()

        start_a0()
        rows_ref[pl.ds(0, tok)] = u_ref[:, pl.ds(0, hid)]
        z_copy.wait_recv()
        rows_ref[pl.ds(tok, tok)] = blocks[z_blk, :, pl.ds(0, hid)]
        start_relay(sa)
        sb['x'].start()
        sb['y'].start()
        sb['c0'].start()
    else:
        z_copy = remote(0, u_ref, blocks, zn)
        z_copy.start()
        rows_ref[pl.ds(0, tok)] = u_ref[...]
        z_copy.wait_recv()
        rows_ref[pl.ds(tok, tok)] = blocks[...]

    def swiglu_tile(slot, rows, offset):
        gate_val = dot_t(rows_ref[...], gate_ring[slot, pl.ds(0, rows)])
        up_val = dot_t(rows_ref[...], up_ring[slot, pl.ds(0, rows)])
        act_ref[:, pl.ds(offset, rows)] = (jax.nn.silu(gate_val) * up_val).astype(BF16)

    @pl.loop(0, n_full)
    def _(step):
        slot = lax.rem(step, n_buf)
        for cp in ring_copies(step, slot, TILE):
            cp.wait()
        swiglu_tile(slot, TILE, pl.multiple_of(step * TILE, TILE))

        @pl.when(step + n_buf < n_full)
        def _():
            for cp in ring_copies(step + n_buf, slot, TILE):
                cp.start()

        @pl.when(step + n_buf == n_full)
        def _():
            for cp in ring_copies(n_full, slot, tail):
                cp.start()

        if with_expert:
            @pl.when(step == 5)
            def _():
                start_last(sa)

    tail_slot = n_full % n_buf
    for cp in ring_copies(n_full, tail_slot, tail):
        cp.wait()
    swiglu_tile(tail_slot, tail, n_full * TILE)

    if with_expert:
        start_relay(sb)

    def rs_copy(col):
        return pltpu.make_async_remote_copy(src_ref=send_buf.at[col], dst_ref=recv_buf.at[col], send_sem=rs_send.at[col],
                                            recv_sem=rs_recv.at[col], device_id=zn, device_id_type=MESH)

    @pl.loop(0, n_col)
    def _(col):
        slot = lax.rem(col, d_buf)
        down_copy(col, slot).wait()
        val = dot_n(act_ref[:, pl.ds(0, k_main)], down_ring[slot, pl.ds(0, k_main)])
        val += dot_n(act_ref[:, pl.ds(k_main, ff - k_main)], down_ring[slot, pl.ds(k_main, ff - k_main)])
        send_buf[col] = val[tok:]
        part_buf[col] = val[:tok]
        rs_copy(col).start()

        @pl.when(col + d_buf < n_col)
        def _():
            down_copy(col + d_buf, slot).start()

    if with_expert:
        start_last(sb)
        own_cp.wait()
        for cp in expert_cps:
            cp.wait()
        for s in (sa, sb):
            for k in ('c0', 'c1', 'c2', 'c3'):
                s[k].wait_recv()
        lane = lax.broadcasted_iota(jnp.int32, (tok, 128), 1)
        slot_id = lax.broadcasted_iota(jnp.int32, (tok, 2 * SLOT_CAP), 1).astype(F32)
        q_rows = 4 * SLOT_CAP

        def eo_copy(quad, buf):
            return pltpu.make_async_copy(e_buf.at[buf], eo_hbm.at[pl.ds(pl.multiple_of(quad * q_rows, q_rows), q_rows)],
                                         eo_sem.at[buf])

        @pl.loop(0, 4)
        def _(it):
            zq = lax.rem(z + it // 2, 2)
            yq = lax.rem(y + it, 2)
            quad = zq * 2 + yq
            buf = lax.rem(it, 2)
            for pair in range(2):
                acc = None
                for k in range(2):
                    blk = quad * 4 + pair * 2 + k
                    table = blocks[blk, :, pl.ds(hid, 128)].astype(F32)
                    rank = jnp.sum(jnp.where(lane == me, table, 0.0), axis=1, keepdims=True)
                    want = jnp.where(rank >= 0.0, rank + k * SLOT_CAP, -1.0)
                    hot = jnp.where(slot_id == want, 1.0, 0.0).astype(BF16)
                    got = lax.dot_general(hot, blocks[blk, :, pl.ds(0, hid)], (((0,), (0,)), ((), ())),
                                          preferred_element_type=F32)
                    acc = got if acc is None else acc + got
                x_buf[pl.ds(pair * 2 * SLOT_CAP, 2 * SLOT_CAP)] = acc.astype(BF16)
            for off, width in ((0, 512), (512, 512), (1024, 384)):
                gate_val = dot_n(x_buf[...], eg[:, pl.ds(off, width)])
                up_val = dot_n(x_buf[...], eu[:, pl.ds(off, width)])
                h_buf[:, pl.ds(off, width)] = (jax.nn.silu(gate_val) * up_val).astype(BF16)

            @pl.when(it >= 2)
            def _():
                eo_copy(0, buf).wait()

            for off in range(0, hid, 512):
                e_buf[buf, :, pl.ds(off, 512)] = dot_n(h_buf[...], ed[:, pl.ds(off, 512)]).astype(BF16)
            eo_copy(quad, buf).start()

        eo_copy(0, 0).wait()
        eo_copy(0, 1).wait()

    @pl.loop(0, n_col)
    def _(col):
        rs_copy(col).wait()
        cols = pl.ds(pl.multiple_of(col * COLS, COLS), COLS)
        total = h_ref[:, cols].astype(F32) + (part_buf[col] + recv_buf[col])
        out_ref[:, cols] = total.astype(out_ref.dtype)

    z_copy.wait_send()
    if with_expert:
        for s in (sa, sb):
            for cp in s.values():
                cp.wait_send()


def dense_call(u, h, w_gate_t, w_up_t, w_down, out_dtype, expert=None):
    tok, hid = h.shape
    ff = w_gate_t.shape[0]
    width = u.shape[1]
    with_expert = expert is not None
    n_buf, d_buf = (3, 3) if with_expert else (7, 4)
    vmem, hbm = pl.BlockSpec(memory_space=pltpu.VMEM), pl.BlockSpec(memory_space=pl.ANY)
    n_col = hid // COLS
    args = [u, h, w_gate_t, w_up_t, w_down]
    in_specs = [vmem, vmem, hbm, hbm, hbm]
    out_shape = [jax.ShapeDtypeStruct((tok, hid), out_dtype)]
    out_specs = [vmem]
    ff_pad = (ff // TILE + 1) * TILE
    n_ex = 17 if with_expert else 1
    scratch = [
        pltpu.VMEM((2 * tok, hid), BF16),
        pltpu.VMEM((2 * tok, ff_pad), BF16),
        pltpu.VMEM((n_buf, TILE, hid), BF16),
        pltpu.VMEM((n_buf, TILE, hid), BF16),
        pltpu.VMEM((d_buf, ff, COLS), BF16),
        pltpu.VMEM((n_col, tok, COLS), F32),
        pltpu.VMEM((n_col, tok, COLS), F32),
        pltpu.VMEM((n_col, tok, COLS), F32),
        pltpu.SemaphoreType.DMA((2, n_buf)),
        pltpu.SemaphoreType.DMA((d_buf,)),
        pltpu.SemaphoreType.DMA((n_ex,)),
        pltpu.SemaphoreType.DMA((n_ex,)),
        pltpu.SemaphoreType.DMA((n_col,)),
        pltpu.SemaphoreType.DMA((n_col,)),
    ]
    if with_expert:
        inner = expert[0].shape[2]
        args += list(expert)
        in_specs += [hbm, hbm, hbm]
        out_shape.append(jax.ShapeDtypeStruct((16 * SLOT_CAP, hid), BF16))
        out_specs.append(hbm)
        scratch += [
            pltpu.VMEM((16, tok, width), BF16),
            pltpu.VMEM((hid, inner), BF16),
            pltpu.VMEM((hid, inner), BF16),
            pltpu.VMEM((inner, hid), BF16),
            pltpu.VMEM((4 * SLOT_CAP, hid), BF16),
            pltpu.VMEM((4 * SLOT_CAP, inner), BF16),
            pltpu.VMEM((2, 4 * SLOT_CAP, hid), BF16),
            pltpu.SemaphoreType.DMA((3,)),
            pltpu.SemaphoreType.DMA((2,)),
        ]
    else:
        scratch.append(pltpu.VMEM((tok, width), BF16))
    flops = 2 * 2 * tok * hid * ff * 3 + (2 * 16 * SLOT_CAP * hid * 1408 * 3 if with_expert else 0)
    return pl.pallas_call(
        functools.partial(ffn_kernel, with_expert, n_buf, d_buf),
        out_shape=out_shape, in_specs=in_specs, out_specs=out_specs, scratch_shapes=scratch,
        compiler_params=pltpu.CompilerParams(collective_id=0 if with_expert else 1, has_side_effects=True,
                                             vmem_limit_bytes=VMEM_LIMIT),
        cost_estimate=pl.CostEstimate(flops=flops, bytes_accessed=6 * hid * ff, transcendentals=0),
        name='dense_expert' if with_expert else 'dense',
    )(*args)


def slot_ranks(route_ids, n_dev):
    tok = route_ids.shape[0]
    member = jnp.any(route_ids[:, :, None] == jnp.arange(n_dev)[None, None, :], axis=1)
    before = (jnp.arange(tok)[:, None] > jnp.arange(tok)[None, :]).astype(BF16)
    rank = jnp.dot(before, member.astype(BF16), preferred_element_type=F32)
    return jnp.where(member, rank, -1.0)


def combine(back, ranks, route_ids, route_wts, normed, n_dev):
    tok = route_ids.shape[0]
    by_expert = jnp.sum(jnp.where(route_ids[:, :, None] == jnp.arange(n_dev)[None, None, :], route_wts[:, :, None], 0.0), axis=1)
    zero_wt = jnp.sum(jnp.where(route_ids >= n_dev, route_wts, 0.0), axis=1)
    pieces, rest = [], by_expert
    for _ in range(3):
        top = lax.reduce_precision(rest, 8, 7)
        pieces.append(top)
        rest = rest - top
    hit = ranks[:, :, None] == jnp.arange(SLOT_CAP, dtype=F32)[None, None, :]
    mats = [jnp.where(hit, p[:, :, None], 0.0).astype(BF16).reshape(tok, n_dev * SLOT_CAP) for p in pieces]
    mixed = jnp.dot(jnp.concatenate(mats, axis=0), back, preferred_element_type=F32)
    mixed = (mixed[2 * tok:] + mixed[tok:2 * tok]) + mixed[:tok]
    return mixed + zero_wt[:, None] * normed.astype(F32)


def solution(mesh):
    n_dev = mesh.shape['tp'] * mesh.shape['ep']
    rows_spec = P(FLAT_AXES, None)
    cube_spec = P(FLAT_AXES, None, None)
    whole_spec = P(None, None, None)
    col_split = P(None, 'tp')
    row_split = P('tp', None)
    in_specs = (rows_spec, cube_spec, cube_spec, P(FLAT_AXES), rows_spec, rows_spec,
                whole_spec, whole_spec, whole_spec, whole_spec, whole_spec, whole_spec, whole_spec, whole_spec,
                col_split, col_split, row_split, col_split, col_split, row_split,
                cube_spec, cube_spec, cube_spec)

    def body(hidden_in, cache0, cache1, kv_lens, route_ids, route_wts, att0_q, att0_uk, att0_uv, att0_o, att1_q, att1_uk, att1_uv, att1_o, ffn0_gate, ffn0_up, ffn0_down, ffn1_gate, ffn1_up, ffn1_down, exp_gate, exp_up, exp_down):
        ranks = slot_ranks(route_ids, n_dev)
        att_zero = attention(rms_norm(hidden_in), cache0, kv_lens, att0_q, att0_uk, att0_uv, att0_o)
        h_zero = (hidden_in.astype(F32) + att_zero).astype(BF16)
        u_zero = rms_norm(h_zero)
        table = jnp.pad(ranks, ((0, 0), (0, 128 - n_dev))).astype(BF16)
        u_ext = jnp.concatenate([u_zero, table], axis=1)
        f_zero, exp_out = dense_call(u_ext, h_zero, ffn0_gate.T, ffn0_up.T, ffn0_down, BF16, (exp_gate, exp_up, exp_down))
        back = lax.all_to_all(exp_out, FLAT_AXES, 0, 0, tiled=True)
        att_one = attention(rms_norm(f_zero), cache1, kv_lens, att1_q, att1_uk, att1_uv, att1_o)
        h_one = (f_zero.astype(F32) + att_one).astype(BF16)
        dense_one, = dense_call(rms_norm(h_one), h_one, ffn1_gate.T, ffn1_up.T, ffn1_down, F32)
        mix = combine(back, ranks, route_ids, route_wts, u_zero, n_dev)
        return (dense_one + mix).astype(BF16)

    return jax.shard_map(body, mesh=mesh, in_specs=in_specs, out_specs=rows_spec, check_vma=False)
```

```python
import functools

import jax
import jax.numpy as jnp
from jax import lax
from jax.experimental import pallas as pl
from jax.experimental.pallas import tpu as pltpu
from jax.sharding import PartitionSpec as P

FLAT_AXES = ('tp', 'ep')
MESH = pl.DeviceIdType.MESH
F32, BF16 = jnp.float32, jnp.bfloat16
SLOT_CAP = 72
VMEM_LIMIT = 66_000_000


def dot_t(lhs, rhs):
    return lax.dot_general(lhs, rhs, (((1,), (1,)), ((), ())), preferred_element_type=F32)


def dot_n(lhs, rhs):
    return jnp.dot(lhs, rhs, preferred_element_type=F32)


TILE = 512
COLS = 256


def ffn_kernel(with_expert, n_buf, d_buf, *refs):
    refs = list(refs)
    u_ref, h_ref, gate_hbm, up_hbm, down_hbm = refs[:5]
    del refs[:5]
    if with_expert:
        eg_hbm, eu_hbm, ed_hbm = refs[:3]
        del refs[:3]
    out_ref = refs.pop(0)
    if with_expert:
        eo_hbm = refs.pop(0)
    rows_ref, act_ref, gate_ring, up_ring, down_ring, send_buf, recv_buf, part_buf = refs[:8]
    ring_sem, down_sem, ex_send, ex_recv, rs_send, rs_recv = refs[8:14]
    if with_expert:
        blocks, eg, eu, ed, x_buf, h_buf, e_buf, ew_sem, eo_sem = refs[14:]
    else:
        blocks, = refs[14:]

    tok, hid = h_ref.shape
    ff = gate_hbm.shape[0]
    n_full, tail = ff // TILE, ff % TILE
    n_step = n_full + 1
    n_col = hid // COLS
    k_main = (ff // 256) * 256

    z = lax.axis_index('tp')
    e = lax.axis_index('ep')
    y, x, c = e // 4, (e // 2) % 2, e % 2
    zn = (1 - z, e)
    me = z * 8 + e
    z_blk = (1 - z) * 8 + e

    def ring_copies(step, slot, rows):
        src = pl.ds(step * TILE, rows)
        return [pltpu.make_async_copy(hbm.at[src], ring.at[slot, pl.ds(0, rows)], ring_sem.at[k, slot])
                for k, (hbm, ring) in enumerate(((gate_hbm, gate_ring), (up_hbm, up_ring)))]

    def down_copy(col, slot):
        return pltpu.make_async_copy(down_hbm.at[:, pl.ds(col * COLS, COLS)], down_ring.at[slot], down_sem.at[slot])

    for step in range(n_buf):
        for cp in ring_copies(step, step, TILE):
            cp.start()
    for col in range(d_buf):
        down_copy(col, col).start()
    if with_expert:
        expert_cps = [pltpu.make_async_copy(s.at[0], d, ew_sem.at[k])
                      for k, (s, d) in enumerate(((eg_hbm, eg), (eu_hbm, eu), (ed_hbm, ed)))]
        for cp in expert_cps:
            cp.start()

    if with_expert:
        xn = (z, e + 2 - 4 * x)
        yn = (z, e + 4 - 8 * y)
        cn = (z, e + 1 - 2 * c)
        peers = (zn, xn, yn, cn)
    else:
        peers = (zn,)
    barrier = pltpu.get_barrier_semaphore()
    for peer in peers:
        pl.semaphore_signal(barrier, inc=1, device_id=peer, device_id_type=MESH)
    pl.semaphore_wait(barrier, len(peers))

    def remote(k, src, dst, peer):
        return pltpu.make_async_remote_copy(src_ref=src, dst_ref=dst, send_sem=ex_send.at[k], recv_sem=ex_recv.at[k],
                                            device_id=peer, device_id_type=MESH)

    if with_expert:
        half = tok // 2
        lo, hi = pl.ds(0, half), pl.ds(half, half)

        def plane(z_at):
            base = z_at * 8
            own = base + e
            xb = base + e + 2 - 4 * x
            yb = base + e + 4 - 8 * y
            db = base + (1 - y) * 4 + (1 - x) * 2 + c
            return own, xb, yb, db

        pa = plane(z)
        pb = plane(1 - z)
        z_copy = remote(0, u_ref, blocks.at[me], zn)
        z_copy.start()
        own_cp = pltpu.make_async_copy(u_ref, blocks.at[me], eo_sem.at[0])
        own_cp.start()

        def plane_sends(first, blks, own_src):
            own, xb, yb, db = blks
            return {
                'x': remote(first, own_src, blocks.at[own], xn),
                'y': remote(first + 1, own_src, blocks.at[own], yn),
                'xr': remote(first + 2, blocks.at[yb, hi], blocks.at[yb, hi], xn),
                'yr': remote(first + 3, blocks.at[xb, lo], blocks.at[xb, lo], yn),
                'c0': remote(first + 4, own_src, blocks.at[own], cn),
                'c1': remote(first + 5, blocks.at[xb], blocks.at[xb], cn),
                'c2': remote(first + 6, blocks.at[yb], blocks.at[yb], cn),
                'c3': remote(first + 7, blocks.at[db], blocks.at[db], cn),
            }

        sa = plane_sends(1, pa, u_ref)
        sb = plane_sends(9, pb, blocks.at[z_blk])

        def start_a0():
            sa['x'].start()
            sa['y'].start()
            sa['c0'].start()

        def start_relay(s):
            s['x'].wait_recv()
            s['y'].wait_recv()
            s['xr'].start()
            s['yr'].start()
            s['c1'].start()
            s['c2'].start()

        def start_last(s):
            s['xr'].wait_recv()
            s['yr'].wait_recv()
            s['c3'].start()

        start_a0()
        rows_ref[pl.ds(0, tok)] = u_ref[:, pl.ds(0, hid)]
        z_copy.wait_recv()
        rows_ref[pl.ds(tok, tok)] = blocks[z_blk, :, pl.ds(0, hid)]
        start_relay(sa)
        sb['x'].start()
        sb['y'].start()
        sb['c0'].start()
    else:
        z_copy = remote(0, u_ref, blocks, zn)
        z_copy.start()
        rows_ref[pl.ds(0, tok)] = u_ref[...]
        z_copy.wait_recv()
        rows_ref[pl.ds(tok, tok)] = blocks[...]

    def swiglu_tile(slot, rows, offset):
        gate_val = dot_t(rows_ref[...], gate_ring[slot, pl.ds(0, rows)])
        up_val = dot_t(rows_ref[...], up_ring[slot, pl.ds(0, rows)])
        act_ref[:, pl.ds(offset, rows)] = (jax.nn.silu(gate_val) * up_val).astype(BF16)

    @pl.loop(0, n_full)
    def _(step):
        slot = lax.rem(step, n_buf)
        for cp in ring_copies(step, slot, TILE):
            cp.wait()
        swiglu_tile(slot, TILE, pl.multiple_of(step * TILE, TILE))

        @pl.when(step + n_buf < n_full)
        def _():
            for cp in ring_copies(step + n_buf, slot, TILE):
                cp.start()

        @pl.when(step + n_buf == n_full)
        def _():
            for cp in ring_copies(n_full, slot, tail):
                cp.start()

        if with_expert:
            @pl.when(step == 5)
            def _():
                start_last(sa)

    tail_slot = n_full % n_buf
    for cp in ring_copies(n_full, tail_slot, tail):
        cp.wait()
    swiglu_tile(tail_slot, tail, n_full * TILE)

    if with_expert:
        start_relay(sb)

    def rs_copy(col):
        return pltpu.make_async_remote_copy(src_ref=send_buf.at[col], dst_ref=recv_buf.at[col], send_sem=rs_send.at[col],
                                            recv_sem=rs_recv.at[col], device_id=zn, device_id_type=MESH)

    @pl.loop(0, n_col)
    def _(col):
        slot = lax.rem(col, d_buf)
        down_copy(col, slot).wait()
        val = dot_n(act_ref[:, pl.ds(0, k_main)], down_ring[slot, pl.ds(0, k_main)])
        val += dot_n(act_ref[:, pl.ds(k_main, ff - k_main)], down_ring[slot, pl.ds(k_main, ff - k_main)])
        send_buf[col] = val[tok:]
        part_buf[col] = val[:tok]
        rs_copy(col).start()

        @pl.when(col + d_buf < n_col)
        def _():
            down_copy(col + d_buf, slot).start()

    if with_expert:
        start_last(sb)
        own_cp.wait()
        for cp in expert_cps:
            cp.wait()
        for s in (sa, sb):
            for k in ('c0', 'c1', 'c2', 'c3'):
                s[k].wait_recv()
        lane = lax.broadcasted_iota(jnp.int32, (tok, 128), 1)
        slot_id = lax.broadcasted_iota(jnp.int32, (tok, 2 * SLOT_CAP), 1).astype(F32)
        q_rows = 4 * SLOT_CAP

        def eo_copy(quad, buf):
            return pltpu.make_async_copy(e_buf.at[buf], eo_hbm.at[pl.ds(pl.multiple_of(quad * q_rows, q_rows), q_rows)],
                                         eo_sem.at[buf])

        @pl.loop(0, 4)
        def _(it):
            zq = lax.rem(z + it // 2, 2)
            yq = lax.rem(y + it, 2)
            quad = zq * 2 + yq
            buf = lax.rem(it, 2)
            for pair in range(2):
                acc = None
                for k in range(2):
                    blk = quad * 4 + pair * 2 + k
                    table = blocks[blk, :, pl.ds(hid, 128)].astype(F32)
                    rank = jnp.sum(jnp.where(lane == me, table, 0.0), axis=1, keepdims=True)
                    want = jnp.where(rank >= 0.0, rank + k * SLOT_CAP, -1.0)
                    hot = jnp.where(slot_id == want, 1.0, 0.0).astype(BF16)
                    got = lax.dot_general(hot, blocks[blk, :, pl.ds(0, hid)], (((0,), (0,)), ((), ())),
                                          preferred_element_type=F32)
                    acc = got if acc is None else acc + got
                x_buf[pl.ds(pair * 2 * SLOT_CAP, 2 * SLOT_CAP)] = acc.astype(BF16)
            for off, width in ((0, 512), (512, 512), (1024, 384)):
                gate_val = dot_n(x_buf[...], eg[:, pl.ds(off, width)])
                up_val = dot_n(x_buf[...], eu[:, pl.ds(off, width)])
                h_buf[:, pl.ds(off, width)] = (jax.nn.silu(gate_val) * up_val).astype(BF16)

            @pl.when(it >= 2)
            def _():
                eo_copy(0, buf).wait()

            for off in range(0, hid, 512):
                e_buf[buf, :, pl.ds(off, 512)] = dot_n(h_buf[...], ed[:, pl.ds(off, 512)]).astype(BF16)
            eo_copy(quad, buf).start()

        eo_copy(0, 0).wait()
        eo_copy(0, 1).wait()

    @pl.loop(0, n_col)
    def _(col):
        rs_copy(col).wait()
        cols = pl.ds(pl.multiple_of(col * COLS, COLS), COLS)
        total = h_ref[:, cols].astype(F32) + (part_buf[col] + recv_buf[col])
        out_ref[:, cols] = total.astype(out_ref.dtype)

    z_copy.wait_send()
    if with_expert:
        for s in (sa, sb):
            for cp in s.values():
                cp.wait_send()


def dense_call(u, h, w_gate_t, w_up_t, w_down, out_dtype, expert=None):
    tok, hid = h.shape
    ff = w_gate_t.shape[0]
    width = u.shape[1]
    with_expert = expert is not None
    n_buf, d_buf = (3, 3) if with_expert else (7, 4)
    vmem, hbm = pl.BlockSpec(memory_space=pltpu.VMEM), pl.BlockSpec(memory_space=pl.ANY)
    n_col = hid // COLS
    args = [u, h, w_gate_t, w_up_t, w_down]
    in_specs = [vmem, vmem, hbm, hbm, hbm]
    out_shape = [jax.ShapeDtypeStruct((tok, hid), out_dtype)]
    out_specs = [vmem]
    ff_pad = (ff // TILE + 1) * TILE
    n_ex = 17 if with_expert else 1
    scratch = [
        pltpu.VMEM((2 * tok, hid), BF16),
        pltpu.VMEM((2 * tok, ff_pad), BF16),
        pltpu.VMEM((n_buf, TILE, hid), BF16),
        pltpu.VMEM((n_buf, TILE, hid), BF16),
        pltpu.VMEM((d_buf, ff, COLS), BF16),
        pltpu.VMEM((n_col, tok, COLS), F32),
        pltpu.VMEM((n_col, tok, COLS), F32),
        pltpu.VMEM((n_col, tok, COLS), F32),
        pltpu.SemaphoreType.DMA((2, n_buf)),
        pltpu.SemaphoreType.DMA((d_buf,)),
        pltpu.SemaphoreType.DMA((n_ex,)),
        pltpu.SemaphoreType.DMA((n_ex,)),
        pltpu.SemaphoreType.DMA((n_col,)),
        pltpu.SemaphoreType.DMA((n_col,)),
    ]
    if with_expert:
        inner = expert[0].shape[2]
        args += list(expert)
        in_specs += [hbm, hbm, hbm]
        out_shape.append(jax.ShapeDtypeStruct((16 * SLOT_CAP, hid), BF16))
        out_specs.append(hbm)
        scratch += [
            pltpu.VMEM((16, tok, width), BF16),
            pltpu.VMEM((hid, inner), BF16),
            pltpu.VMEM((hid, inner), BF16),
            pltpu.VMEM((inner, hid), BF16),
            pltpu.VMEM((4 * SLOT_CAP, hid), BF16),
            pltpu.VMEM((4 * SLOT_CAP, inner), BF16),
            pltpu.VMEM((2, 4 * SLOT_CAP, hid), BF16),
            pltpu.SemaphoreType.DMA((3,)),
            pltpu.SemaphoreType.DMA((2,)),
        ]
    else:
        scratch.append(pltpu.VMEM((tok, width), BF16))
    flops = 2 * 2 * tok * hid * ff * 3 + (2 * 16 * SLOT_CAP * hid * 1408 * 3 if with_expert else 0)
    return pl.pallas_call(
        functools.partial(ffn_kernel, with_expert, n_buf, d_buf),
        out_shape=out_shape, in_specs=in_specs, out_specs=out_specs, scratch_shapes=scratch,
        compiler_params=pltpu.CompilerParams(collective_id=0 if with_expert else 1, has_side_effects=True,
                                             vmem_limit_bytes=VMEM_LIMIT),
        cost_estimate=pl.CostEstimate(flops=flops, bytes_accessed=6 * hid * ff, transcendentals=0),
        name='dense_expert' if with_expert else 'dense',
    )(*args)


GROUP = 8
RING = 4


def att_kernel(with_table, *refs):
    refs = list(refs)
    lens_ref, x_ref, cos_ref, sin_ref = refs[:4]
    del refs[:4]
    table_ref = refs.pop(0) if with_table else None
    wq_hbm, uk_hbm, uv_hbm, wo_hbm, cache_hbm, h_ref, u_ref = refs[:7]
    wq, uk, uv, wo, ring, xn_buf, q_buf, o_buf, ov_buf, w_sem, ring_sem = refs[7:]
    tok, hid = x_ref.shape
    heads, nope, latent = uk.shape
    qk_dim = wq.shape[1]
    rope = qk_dim - nope
    scale = qk_dim ** -0.5
    n_group = tok // GROUP
    span = latent + rope

    def head_copy(quad):
        return pltpu.make_async_copy(wq_hbm.at[pl.ds(quad * 4, 4)], wq.at[pl.ds(quad * 4, 4)], w_sem.at[quad])

    def ring_copy(group, slot):
        return pltpu.make_async_copy(cache_hbm.at[pl.ds(group * GROUP, GROUP)], ring.at[slot], ring_sem.at[slot])

    uk_cp = pltpu.make_async_copy(uk_hbm, uk, w_sem.at[4])
    uv_cp = pltpu.make_async_copy(uv_hbm, uv, w_sem.at[5])
    wo_cp = pltpu.make_async_copy(wo_hbm, wo, w_sem.at[6])
    head_copy(0).start()
    uk_cp.start()
    for quad in range(1, heads // 4):
        head_copy(quad).start()
    for group in range(RING):
        ring_copy(group, group).start()

    def norm(val):
        return (val * lax.rsqrt(jnp.mean(val * val, axis=-1, keepdims=True) + 1e-6)).astype(BF16)

    xn_buf[...] = norm(x_ref[...].astype(F32))
    uk_cp.wait()
    lane = lax.broadcasted_iota(jnp.int32, (tok, 128), 1)
    first_half = lax.rem(lane, rope) < rope // 2

    @pl.loop(0, heads // 4)
    def _(quad):
        head_copy(quad).wait()
        w_nope = jnp.concatenate([wq[quad * 4 + k, pl.ds(0, nope)] for k in range(4)], axis=0)
        w_rope = jnp.concatenate([wq[quad * 4 + k, pl.ds(nope, rope)] for k in range(4)], axis=0)
        q_nope = dot_t(xn_buf[...], w_nope).astype(BF16)
        q_rope = dot_t(xn_buf[...], w_rope).astype(BF16).astype(F32)
        for k in range(4):
            q_lat = dot_n(q_nope[:, k * nope:(k + 1) * nope], uk[quad * 4 + k]).astype(BF16).astype(F32)
            for j in range(latent // 128):
                q_buf[j, pl.ds(quad * 4 + k, tok, stride=heads)] = q_lat[:, j * 128:(j + 1) * 128]
        for k in range(2):
            val = q_rope[:, k * 128:(k + 1) * 128]
            swap = jnp.where(first_half, pltpu.roll(val, 128 - rope // 2, 1), pltpu.roll(val, rope // 2, 1))
            rot = (val * cos_ref[...] + swap * sin_ref[...]).astype(BF16).astype(F32)
            q_buf[latent // 128, pl.ds(quad * 4 + 2 * k, tok, stride=heads)] = rot
            q_buf[latent // 128, pl.ds(quad * 4 + 2 * k + 1, tok, stride=heads)] = pltpu.roll(rot, rope, 1)

    place = lax.broadcasted_iota(jnp.int32, (heads, cache_hbm.shape[2]), 1)

    @pl.loop(0, n_group)
    def _(group):
        slot = lax.rem(group, RING)
        ring_copy(group, slot).wait()
        for k in range(GROUP):
            t = group * GROUP + k
            rows = pl.ds(pl.multiple_of(t * heads, heads), heads)
            q_cat = jnp.concatenate([q_buf[j, rows] for j in range(latent // 128 + 1)], axis=1)[:, :span].astype(BF16)
            score = dot_n(q_cat, ring[slot, k]) * scale
            score = jnp.where(place < lens_ref[t], score, -1e30)
            top = jnp.max(score, axis=1, keepdims=True)
            num = jnp.exp(score - top)
            prob = (num * (1.0 / jnp.sum(num, axis=1, keepdims=True))).astype(BF16)
            o_lat = dot_t(prob, ring[slot, k, pl.ds(0, latent)])
            for j in range(latent // 128):
                o_buf[j, rows] = o_lat[:, j * 128:(j + 1) * 128]

        @pl.when(group + RING < n_group)
        def _():
            ring_copy(group + RING, slot).start()

        @pl.when(group == 4)
        def _():
            uv_cp.start()
            wo_cp.start()

    uv_cp.wait()

    @pl.loop(0, heads)
    def _(h):
        o_lat = jnp.concatenate([o_buf[j, pl.ds(h, tok, stride=heads)] for j in range(latent // 128)], axis=1).astype(BF16)
        vals = dot_n(o_lat, uv[h]).astype(BF16)
        ov_buf[:, pl.ds(pl.multiple_of(h * nope, nope), nope)] = vals

    wo_cp.wait()
    for off in range(0, hid, 512):
        cols = pl.ds(off, 512)
        att = dot_n(ov_buf[...], wo[:, cols])
        h_ref[:, cols] = (x_ref[:, cols].astype(F32) + att).astype(BF16)
    u_ref[:, pl.ds(0, hid)] = norm(h_ref[...].astype(F32))
    if with_table:
        u_ref[:, pl.ds(hid, 128)] = table_ref[...]


def att_call(x, cache, kv_lens, cos, sin, w_q, w_uk, w_uv, w_o, table=None):
    tok, hid = x.shape
    heads, nope, latent = w_uk.shape
    val_dim = w_uv.shape[2]
    assert val_dim == nope
    qk_dim = w_q.shape[2]
    pos = cache.shape[1]
    span = cache.shape[2]
    with_table = table is not None
    vmem, hbm = pl.BlockSpec(memory_space=pltpu.VMEM), pl.BlockSpec(memory_space=pl.ANY)
    smem = pl.BlockSpec(memory_space=pltpu.SMEM)
    args = [kv_lens, x, cos, sin] + ([table] if with_table else [])
    args += [w_q.transpose(1, 2, 0), w_uk, w_uv, w_o.reshape(heads * val_dim, hid), cache.transpose(0, 2, 1)]
    width = hid + (128 if with_table else 0)
    return pl.pallas_call(
        functools.partial(att_kernel, with_table),
        out_shape=[jax.ShapeDtypeStruct((tok, hid), BF16), jax.ShapeDtypeStruct((tok, width), BF16)],
        in_specs=[smem] + [vmem] * (4 if with_table else 3) + [hbm] * 5,
        out_specs=[vmem, vmem],
        scratch_shapes=[
            pltpu.VMEM((heads, qk_dim, hid), BF16),
            pltpu.VMEM((heads, nope, latent), BF16),
            pltpu.VMEM((heads, latent, val_dim), BF16),
            pltpu.VMEM((heads * val_dim, hid), BF16),
            pltpu.VMEM((RING, GROUP, span, pos), BF16),
            pltpu.VMEM((tok, hid), BF16),
            pltpu.VMEM((latent // 128 + 1, tok * heads, 128), F32),
            pltpu.VMEM((latent // 128, tok * heads, 128), F32),
            pltpu.VMEM((tok, heads * val_dim), BF16),
            pltpu.SemaphoreType.DMA((7,)),
            pltpu.SemaphoreType.DMA((RING,)),
        ],
        compiler_params=pltpu.CompilerParams(vmem_limit_bytes=VMEM_LIMIT),
        cost_estimate=pl.CostEstimate(flops=6 * tok * hid * 3072, bytes_accessed=54_000_000, transcendentals=0),
        name='latent_attention',
    )(*args)


def rope_tables(kv_lens, rope):
    half = rope // 2
    inv_freq = 10000.0 ** (-2.0 * jnp.arange(half, dtype=F32) / rope)
    angle = kv_lens.astype(F32)[:, None] * inv_freq
    cos, sin = jnp.cos(angle), jnp.sin(angle)
    return jnp.concatenate([cos] * 4, axis=1), jnp.concatenate([-sin, sin, -sin, sin], axis=1)


def slot_ranks(route_ids, n_dev):
    tok = route_ids.shape[0]
    member = jnp.any(route_ids[:, :, None] == jnp.arange(n_dev)[None, None, :], axis=1)
    before = (jnp.arange(tok)[:, None] > jnp.arange(tok)[None, :]).astype(BF16)
    rank = jnp.dot(before, member.astype(BF16), preferred_element_type=F32)
    return jnp.where(member, rank, -1.0)


def combine(back, ranks, route_ids, route_wts, normed, n_dev):
    tok = route_ids.shape[0]
    by_expert = jnp.sum(jnp.where(route_ids[:, :, None] == jnp.arange(n_dev)[None, None, :], route_wts[:, :, None], 0.0), axis=1)
    zero_wt = jnp.sum(jnp.where(route_ids >= n_dev, route_wts, 0.0), axis=1)
    pieces, rest = [], by_expert
    for _ in range(3):
        top = lax.reduce_precision(rest, 8, 7)
        pieces.append(top)
        rest = rest - top
    hit = ranks[:, :, None] == jnp.arange(SLOT_CAP, dtype=F32)[None, None, :]
    mats = [jnp.where(hit, p[:, :, None], 0.0).astype(BF16).reshape(tok, n_dev * SLOT_CAP) for p in pieces]
    mixed = jnp.dot(jnp.concatenate(mats, axis=0), back, preferred_element_type=F32)
    mixed = (mixed[2 * tok:] + mixed[tok:2 * tok]) + mixed[:tok]
    return mixed + zero_wt[:, None] * normed.astype(F32)


def solution(mesh):
    n_dev = mesh.shape['tp'] * mesh.shape['ep']
    rows_spec = P(FLAT_AXES, None)
    cube_spec = P(FLAT_AXES, None, None)
    whole_spec = P(None, None, None)
    col_split = P(None, 'tp')
    row_split = P('tp', None)
    in_specs = (rows_spec, cube_spec, cube_spec, P(FLAT_AXES), rows_spec, rows_spec,
                whole_spec, whole_spec, whole_spec, whole_spec, whole_spec, whole_spec, whole_spec, whole_spec,
                col_split, col_split, row_split, col_split, col_split, row_split,
                cube_spec, cube_spec, cube_spec)

    def body(hidden_in, cache0, cache1, kv_lens, route_ids, route_wts, att0_q, att0_uk, att0_uv, att0_o, att1_q, att1_uk, att1_uv, att1_o, ffn0_gate, ffn0_up, ffn0_down, ffn1_gate, ffn1_up, ffn1_down, exp_gate, exp_up, exp_down):
        ranks = slot_ranks(route_ids, n_dev)
        table = jnp.pad(ranks, ((0, 0), (0, 128 - n_dev))).astype(BF16)
        cos, sin = rope_tables(kv_lens, att0_q.shape[2] - att0_uk.shape[1])
        h_zero, u_ext = att_call(hidden_in, cache0, kv_lens, cos, sin, att0_q, att0_uk, att0_uv, att0_o, table)
        f_zero, exp_out = dense_call(u_ext, h_zero, ffn0_gate.T, ffn0_up.T, ffn0_down, BF16, (exp_gate, exp_up, exp_down))
        back = lax.all_to_all(exp_out, FLAT_AXES, 0, 0, tiled=True)
        h_one, u_one = att_call(f_zero, cache1, kv_lens, cos, sin, att1_q, att1_uk, att1_uv, att1_o)
        dense_one, = dense_call(u_one, h_one, ffn1_gate.T, ffn1_up.T, ffn1_down, F32)
        mix = combine(back, ranks, route_ids, route_wts, u_ext[:, :hidden_in.shape[1]], n_dev)
        return (dense_one + mix).astype(BF16)

    return jax.shard_map(body, mesh=mesh, in_specs=in_specs, out_specs=rows_spec, check_vma=False)
```

```python
import functools

import jax
import jax.numpy as jnp
from jax import lax
from jax.experimental import pallas as pl
from jax.experimental.pallas import tpu as pltpu
from jax.sharding import PartitionSpec as P

FLAT_AXES = ('tp', 'ep')
MESH = pl.DeviceIdType.MESH
F32, BF16 = jnp.float32, jnp.bfloat16
SLOT_CAP = 72
VMEM_LIMIT = 66_000_000


def dot_t(lhs, rhs):
    return lax.dot_general(lhs, rhs, (((1,), (1,)), ((), ())), preferred_element_type=F32)


def dot_n(lhs, rhs):
    return jnp.dot(lhs, rhs, preferred_element_type=F32)


TILE = 512
COLS = 256


def ffn_kernel(with_expert, n_buf, d_buf, *refs):
    refs = list(refs)
    u_ref, h_ref, gate_hbm, up_hbm, down_hbm = refs[:5]
    del refs[:5]
    if with_expert:
        eg_hbm, eu_hbm, ed_hbm = refs[:3]
        del refs[:3]
    out_ref = refs.pop(0)
    if with_expert:
        eo_hbm = refs.pop(0)
    rows_ref, act_ref, gate_ring, up_ring, down_ring, send_buf, recv_buf, part_buf = refs[:8]
    ring_sem, down_sem, ex_send, ex_recv, rs_send, rs_recv = refs[8:14]
    if with_expert:
        blocks, eg, eu, ed, x_buf, h_buf, e_buf, ew_sem, eo_sem = refs[14:]
    else:
        blocks, = refs[14:]

    tok, hid = h_ref.shape
    ff = gate_hbm.shape[0]
    n_full, tail = ff // TILE, ff % TILE
    n_step = n_full + 1
    n_col = hid // COLS
    k_main = (ff // 256) * 256

    z = lax.axis_index('tp')
    e = lax.axis_index('ep')
    y, x, c = e // 4, (e // 2) % 2, e % 2
    zn = (1 - z, e)
    me = z * 8 + e
    z_blk = (1 - z) * 8 + e

    def ring_copies(step, slot, rows):
        src = pl.ds(step * TILE, rows)
        return [pltpu.make_async_copy(hbm.at[src], ring.at[slot, pl.ds(0, rows)], ring_sem.at[k, slot])
                for k, (hbm, ring) in enumerate(((gate_hbm, gate_ring), (up_hbm, up_ring)))]

    def down_copy(col, slot):
        return pltpu.make_async_copy(down_hbm.at[:, pl.ds(col * COLS, COLS)], down_ring.at[slot], down_sem.at[slot])

    for step in range(n_buf):
        for cp in ring_copies(step, step, TILE):
            cp.start()
    for col in range(d_buf):
        down_copy(col, col).start()
    if with_expert:
        expert_cps = [pltpu.make_async_copy(s.at[0], d, ew_sem.at[k])
                      for k, (s, d) in enumerate(((eg_hbm, eg), (eu_hbm, eu), (ed_hbm, ed)))]
        for cp in expert_cps:
            cp.start()

    if with_expert:
        xn = (z, e + 2 - 4 * x)
        yn = (z, e + 4 - 8 * y)
        cn = (z, e + 1 - 2 * c)
        peers = (zn, xn, yn, cn)
    else:
        peers = (zn,)
    barrier = pltpu.get_barrier_semaphore()
    for peer in peers:
        pl.semaphore_signal(barrier, inc=1, device_id=peer, device_id_type=MESH)
    pl.semaphore_wait(barrier, len(peers))

    def remote(k, src, dst, peer):
        return pltpu.make_async_remote_copy(src_ref=src, dst_ref=dst, send_sem=ex_send.at[k], recv_sem=ex_recv.at[k],
                                            device_id=peer, device_id_type=MESH)

    if with_expert:
        half = tok // 2
        lo, hi = pl.ds(0, half), pl.ds(half, half)

        def plane(z_at):
            base = z_at * 8
            own = base + e
            xb = base + e + 2 - 4 * x
            yb = base + e + 4 - 8 * y
            db = base + (1 - y) * 4 + (1 - x) * 2 + c
            return own, xb, yb, db

        pa = plane(z)
        pb = plane(1 - z)
        z_copy = remote(0, u_ref, blocks.at[me], zn)
        z_copy.start()
        own_cp = pltpu.make_async_copy(u_ref, blocks.at[me], eo_sem.at[0])
        own_cp.start()

        def plane_sends(first, blks, own_src):
            own, xb, yb, db = blks
            return {
                'x': remote(first, own_src, blocks.at[own], xn),
                'y': remote(first + 1, own_src, blocks.at[own], yn),
                'xr': remote(first + 2, blocks.at[yb, hi], blocks.at[yb, hi], xn),
                'yr': remote(first + 3, blocks.at[xb, lo], blocks.at[xb, lo], yn),
                'c0': remote(first + 4, own_src, blocks.at[own], cn),
                'c1': remote(first + 5, blocks.at[xb], blocks.at[xb], cn),
                'c2': remote(first + 6, blocks.at[yb], blocks.at[yb], cn),
                'c3': remote(first + 7, blocks.at[db], blocks.at[db], cn),
            }

        sa = plane_sends(1, pa, u_ref)
        sb = plane_sends(9, pb, blocks.at[z_blk])

        def start_a0():
            sa['x'].start()
            sa['y'].start()
            sa['c0'].start()

        def start_relay(s):
            s['x'].wait_recv()
            s['y'].wait_recv()
            s['xr'].start()
            s['yr'].start()
            s['c1'].start()
            s['c2'].start()

        def start_last(s):
            s['xr'].wait_recv()
            s['yr'].wait_recv()
            s['c3'].start()

        start_a0()
        rows_ref[pl.ds(0, tok)] = u_ref[:, pl.ds(0, hid)]
        z_copy.wait_recv()
        rows_ref[pl.ds(tok, tok)] = blocks[z_blk, :, pl.ds(0, hid)]
        start_relay(sa)
        sb['x'].start()
        sb['y'].start()
        sb['c0'].start()
    else:
        z_copy = remote(0, u_ref, blocks, zn)
        z_copy.start()
        rows_ref[pl.ds(0, tok)] = u_ref[...]
        z_copy.wait_recv()
        rows_ref[pl.ds(tok, tok)] = blocks[...]

    def swiglu_tile(slot, rows, offset):
        gate_val = dot_t(rows_ref[...], gate_ring[slot, pl.ds(0, rows)])
        up_val = dot_t(rows_ref[...], up_ring[slot, pl.ds(0, rows)])
        act_ref[:, pl.ds(offset, rows)] = (jax.nn.silu(gate_val) * up_val).astype(BF16)

    @pl.loop(0, n_full)
    def _(step):
        slot = lax.rem(step, n_buf)
        for cp in ring_copies(step, slot, TILE):
            cp.wait()
        swiglu_tile(slot, TILE, pl.multiple_of(step * TILE, TILE))

        @pl.when(step + n_buf < n_full)
        def _():
            for cp in ring_copies(step + n_buf, slot, TILE):
                cp.start()

        @pl.when(step + n_buf == n_full)
        def _():
            for cp in ring_copies(n_full, slot, tail):
                cp.start()

        if with_expert:
            @pl.when(step == 5)
            def _():
                start_last(sa)

    tail_slot = n_full % n_buf
    for cp in ring_copies(n_full, tail_slot, tail):
        cp.wait()
    swiglu_tile(tail_slot, tail, n_full * TILE)

    if with_expert:
        start_relay(sb)

    def rs_copy(col):
        return pltpu.make_async_remote_copy(src_ref=send_buf.at[col], dst_ref=recv_buf.at[col], send_sem=rs_send.at[col],
                                            recv_sem=rs_recv.at[col], device_id=zn, device_id_type=MESH)

    @pl.loop(0, n_col)
    def _(col):
        slot = lax.rem(col, d_buf)
        down_copy(col, slot).wait()
        val = dot_n(act_ref[:, pl.ds(0, k_main)], down_ring[slot, pl.ds(0, k_main)])
        val += dot_n(act_ref[:, pl.ds(k_main, ff - k_main)], down_ring[slot, pl.ds(k_main, ff - k_main)])
        send_buf[col] = val[tok:]
        part_buf[col] = val[:tok]
        rs_copy(col).start()

        @pl.when(col + d_buf < n_col)
        def _():
            down_copy(col + d_buf, slot).start()

    if with_expert:
        start_last(sb)
        own_cp.wait()
        for cp in expert_cps:
            cp.wait()
        for s in (sa, sb):
            for k in ('c0', 'c1', 'c2', 'c3'):
                s[k].wait_recv()
        lane = lax.broadcasted_iota(jnp.int32, (tok, 128), 1)
        slot_id = lax.broadcasted_iota(jnp.int32, (tok, 2 * SLOT_CAP), 1).astype(F32)
        q_rows = 4 * SLOT_CAP

        def eo_copy(quad, buf):
            return pltpu.make_async_copy(e_buf.at[buf], eo_hbm.at[pl.ds(pl.multiple_of(quad * q_rows, q_rows), q_rows)],
                                         eo_sem.at[buf])

        @pl.loop(0, 4)
        def _(it):
            zq = lax.rem(z + it // 2, 2)
            yq = lax.rem(y + it, 2)
            quad = zq * 2 + yq
            buf = lax.rem(it, 2)
            for pair in range(2):
                acc = None
                for k in range(2):
                    blk = quad * 4 + pair * 2 + k
                    table = blocks[blk, :, pl.ds(hid, 128)].astype(F32)
                    rank = jnp.sum(jnp.where(lane == me, table, 0.0), axis=1, keepdims=True)
                    want = jnp.where(rank >= 0.0, rank + k * SLOT_CAP, -1.0)
                    hot = jnp.where(slot_id == want, 1.0, 0.0).astype(BF16)
                    got = lax.dot_general(hot, blocks[blk, :, pl.ds(0, hid)], (((0,), (0,)), ((), ())),
                                          preferred_element_type=F32)
                    acc = got if acc is None else acc + got
                x_buf[pl.ds(pair * 2 * SLOT_CAP, 2 * SLOT_CAP)] = acc.astype(BF16)
            for off, width in ((0, 512), (512, 512), (1024, 384)):
                gate_val = dot_n(x_buf[...], eg[:, pl.ds(off, width)])
                up_val = dot_n(x_buf[...], eu[:, pl.ds(off, width)])
                h_buf[:, pl.ds(off, width)] = (jax.nn.silu(gate_val) * up_val).astype(BF16)

            @pl.when(it >= 2)
            def _():
                eo_copy(0, buf).wait()

            for off in range(0, hid, 512):
                e_buf[buf, :, pl.ds(off, 512)] = dot_n(h_buf[...], ed[:, pl.ds(off, 512)]).astype(BF16)
            eo_copy(quad, buf).start()

        eo_copy(0, 0).wait()
        eo_copy(0, 1).wait()

    @pl.loop(0, n_col)
    def _(col):
        rs_copy(col).wait()
        cols = pl.ds(pl.multiple_of(col * COLS, COLS), COLS)
        total = h_ref[:, cols].astype(F32) + (part_buf[col] + recv_buf[col])
        out_ref[:, cols] = total.astype(out_ref.dtype)

    z_copy.wait_send()
    if with_expert:
        for s in (sa, sb):
            for cp in s.values():
                cp.wait_send()


def dense_call(u, h, w_gate_t, w_up_t, w_down, out_dtype, expert=None):
    tok, hid = h.shape
    ff = w_gate_t.shape[0]
    width = u.shape[1]
    with_expert = expert is not None
    n_buf, d_buf = (3, 3) if with_expert else (7, 4)
    vmem, hbm = pl.BlockSpec(memory_space=pltpu.VMEM), pl.BlockSpec(memory_space=pl.ANY)
    n_col = hid // COLS
    args = [u, h, w_gate_t, w_up_t, w_down]
    in_specs = [vmem, vmem, hbm, hbm, hbm]
    out_shape = [jax.ShapeDtypeStruct((tok, hid), out_dtype)]
    out_specs = [vmem]
    ff_pad = (ff // TILE + 1) * TILE
    n_ex = 17 if with_expert else 1
    scratch = [
        pltpu.VMEM((2 * tok, hid), BF16),
        pltpu.VMEM((2 * tok, ff_pad), BF16),
        pltpu.VMEM((n_buf, TILE, hid), BF16),
        pltpu.VMEM((n_buf, TILE, hid), BF16),
        pltpu.VMEM((d_buf, ff, COLS), BF16),
        pltpu.VMEM((n_col, tok, COLS), F32),
        pltpu.VMEM((n_col, tok, COLS), F32),
        pltpu.VMEM((n_col, tok, COLS), F32),
        pltpu.SemaphoreType.DMA((2, n_buf)),
        pltpu.SemaphoreType.DMA((d_buf,)),
        pltpu.SemaphoreType.DMA((n_ex,)),
        pltpu.SemaphoreType.DMA((n_ex,)),
        pltpu.SemaphoreType.DMA((n_col,)),
        pltpu.SemaphoreType.DMA((n_col,)),
    ]
    if with_expert:
        inner = expert[0].shape[2]
        args += list(expert)
        in_specs += [hbm, hbm, hbm]
        out_shape.append(jax.ShapeDtypeStruct((16 * SLOT_CAP, hid), BF16))
        out_specs.append(hbm)
        scratch += [
            pltpu.VMEM((16, tok, width), BF16),
            pltpu.VMEM((hid, inner), BF16),
            pltpu.VMEM((hid, inner), BF16),
            pltpu.VMEM((inner, hid), BF16),
            pltpu.VMEM((4 * SLOT_CAP, hid), BF16),
            pltpu.VMEM((4 * SLOT_CAP, inner), BF16),
            pltpu.VMEM((2, 4 * SLOT_CAP, hid), BF16),
            pltpu.SemaphoreType.DMA((3,)),
            pltpu.SemaphoreType.DMA((2,)),
        ]
    else:
        scratch.append(pltpu.VMEM((tok, width), BF16))
    flops = 2 * 2 * tok * hid * ff * 3 + (2 * 16 * SLOT_CAP * hid * 1408 * 3 if with_expert else 0)
    return pl.pallas_call(
        functools.partial(ffn_kernel, with_expert, n_buf, d_buf),
        out_shape=out_shape, in_specs=in_specs, out_specs=out_specs, scratch_shapes=scratch,
        compiler_params=pltpu.CompilerParams(collective_id=0 if with_expert else 1, has_side_effects=True,
                                             vmem_limit_bytes=VMEM_LIMIT),
        cost_estimate=pl.CostEstimate(flops=flops, bytes_accessed=6 * hid * ff, transcendentals=0),
        name='dense_expert' if with_expert else 'dense',
    )(*args)


GROUP = 16
RING = 4
SUB = 16


def att_kernel(with_table, *refs):
    refs = list(refs)
    lens_ref, x_ref, cos_ref, sin_ref = refs[:4]
    del refs[:4]
    table_ref = refs.pop(0) if with_table else None
    wq_hbm, uk_hbm, uv_hbm, wo_hbm, cache_hbm, h_ref, u_ref = refs[:7]
    wq, uk, uv, wo, ring, xn_buf, q_buf, o_buf, ov_buf, p_buf, w_sem, ring_sem = refs[7:]
    tok, hid = x_ref.shape
    heads, nope, latent = uk.shape
    qk_dim = wq.shape[1]
    rope = qk_dim - nope
    scale = qk_dim ** -0.5
    n_group = tok // GROUP
    span = latent + rope

    def head_copy(quad):
        return pltpu.make_async_copy(wq_hbm.at[pl.ds(quad * 4, 4)], wq.at[pl.ds(quad * 4, 4)], w_sem.at[quad])

    def ring_copy(group, slot):
        return pltpu.make_async_copy(cache_hbm.at[pl.ds(group * GROUP, GROUP)], ring.at[slot], ring_sem.at[slot])

    uk_cp = pltpu.make_async_copy(uk_hbm, uk, w_sem.at[4])
    uv_cp = pltpu.make_async_copy(uv_hbm, uv, w_sem.at[5])
    wo_cp = pltpu.make_async_copy(wo_hbm, wo, w_sem.at[6])
    head_copy(0).start()
    uk_cp.start()
    for quad in range(1, heads // 4):
        head_copy(quad).start()

    def norm(val):
        return (val * lax.rsqrt(jnp.mean(val * val, axis=-1, keepdims=True) + 1e-6)).astype(BF16)

    xn_buf[...] = norm(x_ref[...].astype(F32))
    uk_cp.wait()
    lane = lax.broadcasted_iota(jnp.int32, (tok, 128), 1)
    first_half = lax.rem(lane, rope) < rope // 2

    @pl.loop(0, heads // 4)
    def _(quad):
        head_copy(quad).wait()

        @pl.when(quad == 0)
        def _():
            for group in range(RING):
                ring_copy(group, group).start()

        @pl.when(quad == 3)
        def _():
            uv_cp.start()
            wo_cp.start()

        w_nope = jnp.concatenate([wq[quad * 4 + k, pl.ds(0, nope)] for k in range(4)], axis=0)
        w_rope = jnp.concatenate([wq[quad * 4 + k, pl.ds(nope, rope)] for k in range(4)], axis=0)
        q_nope = dot_t(xn_buf[...], w_nope).astype(BF16)
        q_rope = dot_t(xn_buf[...], w_rope).astype(BF16).astype(F32)
        for k in range(4):
            q_lat = dot_n(q_nope[:, k * nope:(k + 1) * nope], uk[quad * 4 + k]).astype(BF16).astype(F32)
            for j in range(latent // 128):
                q_buf[j, pl.ds(quad * 4 + k, tok, stride=heads)] = q_lat[:, j * 128:(j + 1) * 128]
        for k in range(2):
            val = q_rope[:, k * 128:(k + 1) * 128]
            swap = jnp.where(first_half, pltpu.roll(val, 128 - rope // 2, 1), pltpu.roll(val, rope // 2, 1))
            rot = (val * cos_ref[...] + swap * sin_ref[...]).astype(BF16).astype(F32)
            q_buf[latent // 128, pl.ds(quad * 4 + 2 * k, tok, stride=heads)] = rot
            q_buf[latent // 128, pl.ds(quad * 4 + 2 * k + 1, tok, stride=heads)] = pltpu.roll(rot, rope, 1)

    place = lax.broadcasted_iota(jnp.int32, (heads, cache_hbm.shape[2]), 1)

    @pl.loop(0, n_group)
    def _(group):
        slot = lax.rem(group, RING)
        ring_copy(group, slot).wait()
        @pl.loop(0, GROUP // SUB)
        def _(sub):
            for k in range(SUB):
                at = sub * SUB + k
                t = group * GROUP + at
                rows = pl.ds(pl.multiple_of(t * heads, heads), heads)
                q_cat = jnp.concatenate([q_buf[j, rows] for j in range(latent // 128 + 1)], axis=1)[:, :span].astype(BF16)
                score = dot_n(q_cat, ring[slot, at]) * scale
                score = jnp.where(place < lens_ref[t], score, -1e30)
                top = jnp.max(score, axis=1, keepdims=True)
                num = jnp.exp(score - top)
                p_buf[at] = (num * (1.0 / jnp.sum(num, axis=1, keepdims=True))).astype(BF16)

        @pl.loop(0, GROUP // SUB)
        def _(sub):
            for k in range(SUB):
                at = sub * SUB + k
                rows = pl.ds(pl.multiple_of((group * GROUP + at) * heads, heads), heads)
                o_lat = dot_t(p_buf[at], ring[slot, at, pl.ds(0, latent)])
                for j in range(latent // 128):
                    o_buf[j, rows] = o_lat[:, j * 128:(j + 1) * 128]

        @pl.when(group + RING < n_group)
        def _():
            ring_copy(group + RING, slot).start()


    uv_cp.wait()

    @pl.loop(0, heads, unroll=8)
    def _(h):
        o_lat = jnp.concatenate([o_buf[j, pl.ds(h, tok, stride=heads)] for j in range(latent // 128)], axis=1).astype(BF16)
        vals = dot_n(o_lat, uv[h]).astype(BF16)
        ov_buf[:, pl.ds(pl.multiple_of(h * nope, nope), nope)] = vals

    wo_cp.wait()
    for off in range(0, hid, 512):
        cols = pl.ds(off, 512)
        att = dot_n(ov_buf[...], wo[:, cols])
        h_ref[:, cols] = (x_ref[:, cols].astype(F32) + att).astype(BF16)
    u_ref[:, pl.ds(0, hid)] = norm(h_ref[...].astype(F32))
    if with_table:
        u_ref[:, pl.ds(hid, 128)] = table_ref[...]


def att_call(x, cache, kv_lens, cos, sin, w_q, w_uk, w_uv, w_o, table=None):
    tok, hid = x.shape
    heads, nope, latent = w_uk.shape
    val_dim = w_uv.shape[2]
    assert val_dim == nope
    qk_dim = w_q.shape[2]
    pos = cache.shape[1]
    span = cache.shape[2]
    with_table = table is not None
    vmem, hbm = pl.BlockSpec(memory_space=pltpu.VMEM), pl.BlockSpec(memory_space=pl.ANY)
    smem = pl.BlockSpec(memory_space=pltpu.SMEM)
    args = [kv_lens, x, cos, sin] + ([table] if with_table else [])
    args += [w_q.transpose(1, 2, 0), w_uk, w_uv, w_o.reshape(heads * val_dim, hid), cache.transpose(0, 2, 1)]
    width = hid + (128 if with_table else 0)
    return pl.pallas_call(
        functools.partial(att_kernel, with_table),
        out_shape=[jax.ShapeDtypeStruct((tok, hid), BF16), jax.ShapeDtypeStruct((tok, width), BF16)],
        in_specs=[smem] + [vmem] * (4 if with_table else 3) + [hbm] * 5,
        out_specs=[vmem, vmem],
        scratch_shapes=[
            pltpu.VMEM((heads, qk_dim, hid), BF16),
            pltpu.VMEM((heads, nope, latent), BF16),
            pltpu.VMEM((heads, latent, val_dim), BF16),
            pltpu.VMEM((heads * val_dim, hid), BF16),
            pltpu.VMEM((RING, GROUP, span, pos), BF16),
            pltpu.VMEM((tok, hid), BF16),
            pltpu.VMEM((latent // 128 + 1, tok * heads, 128), F32),
            pltpu.VMEM((latent // 128, tok * heads, 128), F32),
            pltpu.VMEM((tok, heads * val_dim), BF16),
            pltpu.VMEM((GROUP, heads, pos), BF16),
            pltpu.SemaphoreType.DMA((7,)),
            pltpu.SemaphoreType.DMA((RING,)),
        ],
        compiler_params=pltpu.CompilerParams(vmem_limit_bytes=VMEM_LIMIT),
        cost_estimate=pl.CostEstimate(flops=6 * tok * hid * 3072, bytes_accessed=54_000_000, transcendentals=0),
        name='latent_attention',
    )(*args)


def rope_tables(kv_lens, rope):
    half = rope // 2
    inv_freq = 10000.0 ** (-2.0 * jnp.arange(half, dtype=F32) / rope)
    angle = kv_lens.astype(F32)[:, None] * inv_freq
    cos, sin = jnp.cos(angle), jnp.sin(angle)
    return jnp.concatenate([cos] * 4, axis=1), jnp.concatenate([-sin, sin, -sin, sin], axis=1)


def slot_ranks(route_ids, n_dev):
    tok = route_ids.shape[0]
    member = jnp.any(route_ids[:, :, None] == jnp.arange(n_dev)[None, None, :], axis=1)
    before = (jnp.arange(tok)[:, None] > jnp.arange(tok)[None, :]).astype(BF16)
    rank = jnp.dot(before, member.astype(BF16), preferred_element_type=F32)
    return jnp.where(member, rank, -1.0)


def combine(back, ranks, route_ids, route_wts, normed, n_dev):
    tok = route_ids.shape[0]
    by_expert = jnp.sum(jnp.where(route_ids[:, :, None] == jnp.arange(n_dev)[None, None, :], route_wts[:, :, None], 0.0), axis=1)
    zero_wt = jnp.sum(jnp.where(route_ids >= n_dev, route_wts, 0.0), axis=1)
    pieces, rest = [], by_expert
    for _ in range(3):
        top = lax.reduce_precision(rest, 8, 7)
        pieces.append(top)
        rest = rest - top
    hit = ranks[:, :, None] == jnp.arange(SLOT_CAP, dtype=F32)[None, None, :]
    mats = [jnp.where(hit, p[:, :, None], 0.0).astype(BF16).reshape(tok, n_dev * SLOT_CAP) for p in pieces]
    mixed = jnp.dot(jnp.concatenate(mats, axis=0), back, preferred_element_type=F32)
    mixed = (mixed[2 * tok:] + mixed[tok:2 * tok]) + mixed[:tok]
    return mixed + zero_wt[:, None] * normed.astype(F32)


def solution(mesh):
    n_dev = mesh.shape['tp'] * mesh.shape['ep']
    rows_spec = P(FLAT_AXES, None)
    cube_spec = P(FLAT_AXES, None, None)
    whole_spec = P(None, None, None)
    col_split = P(None, 'tp')
    row_split = P('tp', None)
    in_specs = (rows_spec, cube_spec, cube_spec, P(FLAT_AXES), rows_spec, rows_spec,
                whole_spec, whole_spec, whole_spec, whole_spec, whole_spec, whole_spec, whole_spec, whole_spec,
                col_split, col_split, row_split, col_split, col_split, row_split,
                cube_spec, cube_spec, cube_spec)

    def body(hidden_in, cache0, cache1, kv_lens, route_ids, route_wts, att0_q, att0_uk, att0_uv, att0_o, att1_q, att1_uk, att1_uv, att1_o, ffn0_gate, ffn0_up, ffn0_down, ffn1_gate, ffn1_up, ffn1_down, exp_gate, exp_up, exp_down):
        ranks = slot_ranks(route_ids, n_dev)
        table = jnp.pad(ranks, ((0, 0), (0, 128 - n_dev))).astype(BF16)
        cos, sin = rope_tables(kv_lens, att0_q.shape[2] - att0_uk.shape[1])
        h_zero, u_ext = att_call(hidden_in, cache0, kv_lens, cos, sin, att0_q, att0_uk, att0_uv, att0_o, table)
        f_zero, exp_out = dense_call(u_ext, h_zero, ffn0_gate.T, ffn0_up.T, ffn0_down, BF16, (exp_gate, exp_up, exp_down))
        back = lax.all_to_all(exp_out, FLAT_AXES, 0, 0, tiled=True)
        h_one, u_one = att_call(f_zero, cache1, kv_lens, cos, sin, att1_q, att1_uk, att1_uv, att1_o)
        dense_one, = dense_call(u_one, h_one, ffn1_gate.T, ffn1_up.T, ffn1_down, F32)
        mix = combine(back, ranks, route_ids, route_wts, u_ext[:, :hidden_in.shape[1]], n_dev)
        return (dense_one + mix).astype(BF16)

    return jax.shard_map(body, mesh=mesh, in_specs=in_specs, out_specs=rows_spec, check_vma=False)
```

```python
import functools

import jax
import jax.numpy as jnp
from jax import lax
from jax.experimental import pallas as pl
from jax.experimental.pallas import tpu as pltpu
from jax.sharding import PartitionSpec as P

FLAT_AXES = ('tp', 'ep')
MESH = pl.DeviceIdType.MESH
F32, BF16 = jnp.float32, jnp.bfloat16
SLOT_CAP = 72
VMEM_LIMIT = 66_000_000


def dot_t(lhs, rhs):
    return lax.dot_general(lhs, rhs, (((1,), (1,)), ((), ())), preferred_element_type=F32)


def dot_n(lhs, rhs):
    return jnp.dot(lhs, rhs, preferred_element_type=F32)


TILE = 512
COLS = 256


def ffn_kernel(with_expert, *refs):
    refs = list(refs)
    u_ref, h_ref, gate_hbm, up_hbm, down_hbm = refs[:5]
    del refs[:5]
    if with_expert:
        eg_hbm, eu_hbm, ed_hbm = refs[:3]
        del refs[:3]
    else:
        mix_ref = refs.pop(0)
    out_ref = refs.pop(0)
    if with_expert:
        near_hbm, far_hbm = refs[:2]
        del refs[:2]
    blocks, rows_ref, act_ref, gate_w, up_w, down_w, part_buf, z_out, z_in, d_out, d_in, p_out, p_in = refs[:13]
    w_sem, ex_send, ex_recv, z_send, z_recv, d_send, d_recv, p_send, p_recv, own_sem = refs[13:23]
    if with_expert:
        x_buf, h_buf, e_buf, ew_sem, eo_sem = refs[23:]

    tok, hid = h_ref.shape
    ff = gate_w.shape[0]
    n_full, tail = ff // TILE, ff % TILE
    n_col = hid // COLS
    k_main = (ff // 256) * 256

    z = lax.axis_index('tp')
    e = lax.axis_index('ep')
    y, x, c = e // 4, (e // 2) % 2, e % 2
    zn = (1 - z, e)
    cn = (z, e + 1 - 2 * c)
    base = pl.multiple_of(c * ff, 16)

    def tile_copies(step, rows):
        at = pl.multiple_of(step * TILE, TILE)
        return [pltpu.make_async_copy(hbm.at[pl.ds(pl.multiple_of(base + at, 16), rows)], buf.at[pl.ds(at, rows)], w_sem.at[k, step])
                for k, (hbm, buf) in enumerate(((gate_hbm, gate_w), (up_hbm, up_w)))]

    down_cp = pltpu.make_async_copy(down_hbm.at[pl.ds(base, ff)], down_w, w_sem.at[2, 0])
    for step in range(n_full):
        for cp in tile_copies(step, TILE):
            cp.start()
    for cp in tile_copies(n_full, tail):
        cp.start()
    down_cp.start()

    if with_expert:
        me = z * 8 + e
        xn = (z, e + 2 - 4 * x)
        yn = (z, e + 4 - 8 * y)
        peers = (zn, cn, xn, yn)
    else:
        peers = (zn, cn)
    barrier = pltpu.get_barrier_semaphore()
    for peer in peers:
        pl.semaphore_signal(barrier, inc=1, device_id=peer, device_id_type=MESH)
    pl.semaphore_wait(barrier, len(peers))

    def remote(k, src, dst, peer):
        return pltpu.make_async_remote_copy(src_ref=src, dst_ref=dst, send_sem=ex_send.at[k], recv_sem=ex_recv.at[k],
                                            device_id=peer, device_id_type=MESH)

    if with_expert:
        half = tok // 2
        lo, hi = pl.ds(0, half), pl.ds(half, half)

        def plane(z_at):
            first = z_at * 8
            return (first + e, first + e + 2 - 4 * x, first + e + 4 - 8 * y,
                    first + (1 - y) * 4 + (1 - x) * 2 + c)

        def plane_sends(first, blks, own_src):
            own, xb, yb, db = blks
            return {
                'x': remote(first, own_src, blocks.at[own], xn),
                'y': remote(first + 1, own_src, blocks.at[own], yn),
                'xr': remote(first + 2, blocks.at[yb, hi], blocks.at[yb, hi], xn),
                'yr': remote(first + 3, blocks.at[xb, lo], blocks.at[xb, lo], yn),
                'c0': remote(first + 4, own_src, blocks.at[own], cn),
                'c1': remote(first + 5, blocks.at[xb], blocks.at[xb], cn),
                'c2': remote(first + 6, blocks.at[yb], blocks.at[yb], cn),
                'c3': remote(first + 7, blocks.at[db], blocks.at[db], cn),
            }

        def start_relay(s):
            s['x'].wait_recv()
            s['y'].wait_recv()
            s['xr'].start()
            s['yr'].start()
            s['c1'].start()
            s['c2'].start()

        def start_last(s):
            s['xr'].wait_recv()
            s['yr'].wait_recv()
            s['c3'].start()

        z_blk = (1 - z) * 8 + e
        c_blk = z * 8 + e + 1 - 2 * c
        zc_blk = (1 - z) * 8 + e + 1 - 2 * c
        sa = plane_sends(1, plane(z), u_ref)
        sb = plane_sends(9, plane(1 - z), blocks.at[z_blk])
        z_copy = remote(0, u_ref, blocks.at[me], zn)
        ca_copy, cb_copy = sa['c0'], sb['c0']
        own_cp = pltpu.make_async_copy(u_ref, blocks.at[me], own_sem.at[0])
        own_cp.start()
    else:
        z_blk, c_blk, zc_blk = 0, 1, 2
        z_copy = remote(0, u_ref, blocks.at[0], zn)
        ca_copy = remote(1, u_ref, blocks.at[1], cn)
        cb_copy = remote(2, blocks.at[0], blocks.at[2], cn)

    z_copy.start()
    ca_copy.start()
    if with_expert:
        sa['x'].start()
        sa['y'].start()
    rows_ref[pl.ds(0, tok)] = u_ref[:, pl.ds(0, hid)]
    ca_copy.wait_recv()
    rows_ref[pl.ds(tok, tok)] = blocks[c_blk, :, pl.ds(0, hid)]

    def swiglu_tile(first, at, rows):
        lhs = rows_ref[pl.ds(first, 2 * tok)]
        gate_val = dot_t(lhs, gate_w[pl.ds(at, rows)])
        up_val = dot_t(lhs, up_w[pl.ds(at, rows)])
        act_ref[pl.ds(first, 2 * tok), pl.ds(at, rows)] = (jax.nn.silu(gate_val) * up_val).astype(BF16)

    @pl.loop(0, n_full)
    def _(step):
        for cp in tile_copies(step, TILE):
            cp.wait()
        swiglu_tile(0, pl.multiple_of(step * TILE, TILE), TILE)

    for cp in tile_copies(n_full, tail):
        cp.wait()
    swiglu_tile(0, n_full * TILE, tail)

    z_copy.wait_recv()
    cb_copy.start()
    if with_expert:
        start_relay(sa)
        sb['x'].start()
        sb['y'].start()
    rows_ref[pl.ds(2 * tok, tok)] = blocks[z_blk, :, pl.ds(0, hid)]
    cb_copy.wait_recv()
    rows_ref[pl.ds(3 * tok, tok)] = blocks[zc_blk, :, pl.ds(0, hid)]

    @pl.loop(0, n_full)
    def _(step):
        swiglu_tile(2 * tok, pl.multiple_of(step * TILE, TILE), TILE)

    swiglu_tile(2 * tok, n_full * TILE, tail)

    if with_expert:
        eg, eu, ed = (gate_w.at[pl.ds(0, hid), pl.ds(0, eg_hbm.shape[2])], up_w.at[pl.ds(0, hid), pl.ds(0, eg_hbm.shape[2])],
                      down_w.at[pl.ds(0, ed_hbm.shape[1])])
        eg_cp, eu_cp, ed_cp = (pltpu.make_async_copy(s.at[0], d, ew_sem.at[k])
                               for k, (s, d) in enumerate(((eg_hbm, eg), (eu_hbm, eu), (ed_hbm, ed))))
        eg_cp.start()
        eu_cp.start()
        start_last(sa)

    def link(src, dst, sems, rems, col, peer):
        return pltpu.make_async_remote_copy(src_ref=src.at[col], dst_ref=dst.at[col], send_sem=sems.at[col],
                                            recv_sem=rems.at[col], device_id=peer, device_id_type=MESH)

    def z_link(col):
        return link(z_out, z_in, z_send, z_recv, col, zn)

    def d_link(col):
        return link(d_out, d_in, d_send, d_recv, col, cn)

    def p_link(col):
        return link(p_out, p_in, p_send, p_recv, col, cn)

    def down_tile(first, col):
        cols = pl.ds(pl.multiple_of(col * COLS, COLS), COLS)
        lhs = act_ref.at[pl.ds(first, 2 * tok)]
        val = dot_n(lhs[:, pl.ds(0, k_main)], down_w[pl.ds(0, k_main), cols])
        return val + dot_n(lhs[:, pl.ds(k_main, ff - k_main)], down_w[pl.ds(k_main, ff - k_main), cols])

    def send_z(col):
        d_link(col).wait_recv()
        total = z_out[col] + d_in[col]
        if not with_expert:
            total += mix_ref[:, pl.ds(pl.multiple_of(col * COLS, COLS), COLS)]
        z_out[col] = total
        z_link(col).start()

    down_cp.wait()

    @pl.loop(0, n_col)
    def _(col):
        val = down_tile(2 * tok, col)
        z_out[col] = val[:tok]
        d_out[col] = val[tok:]
        d_link(col).start()

        @pl.when(col >= 2)
        def _():
            send_z(col - 2)

    send_z(n_col - 2)
    send_z(n_col - 1)

    @pl.loop(0, n_col)
    def _(col):
        val = down_tile(0, col)
        part_buf[col] = val[:tok]
        p_out[col] = val[tok:]
        p_link(col).start()

    if with_expert:
        ed_cp.start()
        own_cp.wait()
        eg_cp.wait()
        eu_cp.wait()
        lane = lax.broadcasted_iota(jnp.int32, (tok, 128), 1)
        slot_id = lax.broadcasted_iota(jnp.int32, (tok, 2 * SLOT_CAP), 1).astype(F32)
        q_rows = 4 * SLOT_CAP

        def eo_copy(it, buf, dst, yq):
            return pltpu.make_async_copy(e_buf.at[buf], dst.at[pl.ds(pl.multiple_of(yq * q_rows, q_rows), q_rows)], eo_sem.at[buf])

        @pl.loop(0, 4)
        def _(it):
            @pl.when(it == 0)
            def _():
                sa['c1'].wait_recv()

            @pl.when(it == 1)
            def _():
                start_relay(sb)
                sa['c2'].wait_recv()
                sa['c3'].wait_recv()

            @pl.when(it == 2)
            def _():
                start_last(sb)
                sb['c1'].wait_recv()

            @pl.when(it == 3)
            def _():
                sb['c2'].wait_recv()
                sb['c3'].wait_recv()

            zq = lax.rem(z + it // 2, 2)
            yq = lax.rem(y + it, 2)
            buf = lax.rem(it, 2)
            for pair in range(2):
                acc = None
                for k in range(2):
                    blk = zq * 8 + yq * 4 + pair * 2 + k
                    table = blocks[blk, :, pl.ds(hid, 128)].astype(F32)
                    rank = jnp.sum(jnp.where(lane == me, table, 0.0), axis=1, keepdims=True)
                    want = jnp.where(rank >= 0.0, rank + k * SLOT_CAP, -1.0)
                    hot = jnp.where(slot_id == want, 1.0, 0.0).astype(BF16)
                    got = lax.dot_general(hot, blocks[blk, :, pl.ds(0, hid)], (((0,), (0,)), ((), ())),
                                          preferred_element_type=F32)
                    acc = got if acc is None else acc + got
                x_buf[pl.ds(pair * 2 * SLOT_CAP, 2 * SLOT_CAP)] = acc.astype(BF16)
            for off, width in ((0, 512), (512, 512), (1024, 384)):
                gate_val = dot_n(x_buf[...], eg[:, pl.ds(off, width)])
                up_val = dot_n(x_buf[...], eu[:, pl.ds(off, width)])
                h_buf[:, pl.ds(off, width)] = (jax.nn.silu(gate_val) * up_val).astype(BF16)

            @pl.when(it == 0)
            def _():
                ed_cp.wait()

            @pl.when(it >= 2)
            def _():
                eo_copy(it, buf, near_hbm, yq).wait()

            for off in range(0, hid, 512):
                e_buf[buf, :, pl.ds(off, 512)] = dot_n(h_buf[...], ed[:, pl.ds(off, 512)]).astype(BF16)

            @pl.when(it < 2)
            def _():
                eo_copy(it, buf, near_hbm, yq).start()

            @pl.when(it >= 2)
            def _():
                eo_copy(it, buf, far_hbm, yq).start()

        eo_copy(0, 0, far_hbm, 0).wait()
        eo_copy(0, 1, far_hbm, 0).wait()

    @pl.loop(0, n_col)
    def _(col):
        p_link(col).wait()
        d_link(col).wait_send()
        z_link(col).wait()
        cols = pl.ds(pl.multiple_of(col * COLS, COLS), COLS)
        total = h_ref[:, cols].astype(F32) + ((part_buf[col] + p_in[col]) + z_in[col])
        out_ref[:, cols] = total.astype(out_ref.dtype)

    z_copy.wait_send()
    if with_expert:
        for s in (sa, sb):
            for cp in s.values():
                cp.wait_send()
    else:
        ca_copy.wait_send()
        cb_copy.wait_send()


def dense_call(u, h, w_gate_t, w_up_t, w_down, out_dtype, expert=None, mix=None):
    tok, hid = h.shape
    ff = w_gate_t.shape[0] // 2
    width = u.shape[1]
    with_expert = expert is not None
    vmem, hbm = pl.BlockSpec(memory_space=pltpu.VMEM), pl.BlockSpec(memory_space=pl.ANY)
    n_col = hid // COLS
    n_step = ff // TILE + 1
    args = [u, h, w_gate_t, w_up_t, w_down]
    in_specs = [vmem, vmem, hbm, hbm, hbm]
    out_shape = [jax.ShapeDtypeStruct((tok, hid), out_dtype)]
    out_specs = [vmem]
    n_ex = 17 if with_expert else 3
    dma = pltpu.SemaphoreType.DMA
    scratch = [pltpu.VMEM((16 if with_expert else 3, tok, width), BF16), pltpu.VMEM((4 * tok, hid), BF16),
               pltpu.VMEM((4 * tok, n_step * TILE), BF16),
               pltpu.VMEM((ff, hid), BF16), pltpu.VMEM((ff, hid), BF16), pltpu.VMEM((ff, hid), BF16)]
    scratch += [pltpu.VMEM((n_col, tok, COLS), F32)] * 7
    scratch += [dma((3, n_step)), dma((n_ex,)), dma((n_ex,))] + [dma((n_col,))] * 6 + [dma((1,))]
    flops = 2 * 2 * tok * hid * ff * 6
    if with_expert:
        inner = expert[0].shape[2]
        args += list(expert)
        in_specs += [hbm, hbm, hbm]
        out_shape += [jax.ShapeDtypeStruct((8 * SLOT_CAP, hid), BF16)] * 2
        out_specs += [hbm, hbm]
        scratch += [pltpu.VMEM((4 * SLOT_CAP, hid), BF16), pltpu.VMEM((4 * SLOT_CAP, inner), BF16),
                    pltpu.VMEM((2, 4 * SLOT_CAP, hid), BF16), dma((3,)), dma((2,))]
        flops += 2 * 16 * SLOT_CAP * hid * inner * 3
    else:
        args.append(mix)
        in_specs.append(vmem)
    return pl.pallas_call(
        functools.partial(ffn_kernel, with_expert),
        out_shape=out_shape, in_specs=in_specs, out_specs=out_specs, scratch_shapes=scratch,
        compiler_params=pltpu.CompilerParams(collective_id=0 if with_expert else 1, has_side_effects=True,
                                             vmem_limit_bytes=VMEM_LIMIT),
        cost_estimate=pl.CostEstimate(flops=flops, bytes_accessed=6 * hid * ff, transcendentals=0),
        name='dense_expert' if with_expert else 'dense',
    )(*args)


GROUP = 16
RING = 4
SUB = 16


def att_kernel(with_table, *refs):
    refs = list(refs)
    lens_ref, x_ref, cos_ref, sin_ref = refs[:4]
    del refs[:4]
    table_ref = refs.pop(0) if with_table else None
    wq_hbm, uk_hbm, uv_hbm, wo_hbm, cache_hbm, h_ref, u_ref = refs[:7]
    wq, uk, uv, wo, ring, xn_buf, q_buf, o_buf, ov_buf, p_buf, w_sem, ring_sem = refs[7:]
    tok, hid = x_ref.shape
    heads, nope, latent = uk.shape
    qk_dim = wq.shape[1]
    rope = qk_dim - nope
    scale = qk_dim ** -0.5
    n_group = tok // GROUP
    span = latent + rope

    def head_copy(quad):
        return pltpu.make_async_copy(wq_hbm.at[pl.ds(quad * 4, 4)], wq.at[pl.ds(quad * 4, 4)], w_sem.at[quad])

    def ring_copy(group, slot):
        return pltpu.make_async_copy(cache_hbm.at[pl.ds(group * GROUP, GROUP)], ring.at[slot], ring_sem.at[slot])

    uk_cp = pltpu.make_async_copy(uk_hbm, uk, w_sem.at[4])
    uv_cp = pltpu.make_async_copy(uv_hbm, uv, w_sem.at[5])
    wo_cp = pltpu.make_async_copy(wo_hbm, wo, w_sem.at[6])
    head_copy(0).start()
    uk_cp.start()
    for quad in range(1, heads // 4):
        head_copy(quad).start()

    def norm(val):
        return (val * lax.rsqrt(jnp.mean(val * val, axis=-1, keepdims=True) + 1e-6)).astype(BF16)

    xn_buf[...] = norm(x_ref[...].astype(F32))
    uk_cp.wait()
    lane = lax.broadcasted_iota(jnp.int32, (tok, 128), 1)
    first_half = lax.rem(lane, rope) < rope // 2

    @pl.loop(0, heads // 4)
    def _(quad):
        head_copy(quad).wait()

        @pl.when(quad == 0)
        def _():
            for group in range(RING):
                ring_copy(group, group).start()

        @pl.when(quad == 3)
        def _():
            uv_cp.start()
            wo_cp.start()

        w_nope = jnp.concatenate([wq[quad * 4 + k, pl.ds(0, nope)] for k in range(4)], axis=0)
        w_rope = jnp.concatenate([wq[quad * 4 + k, pl.ds(nope, rope)] for k in range(4)], axis=0)
        q_nope = dot_t(xn_buf[...], w_nope).astype(BF16)
        q_rope = dot_t(xn_buf[...], w_rope).astype(BF16).astype(F32)
        for k in range(4):
            q_lat = dot_n(q_nope[:, k * nope:(k + 1) * nope], uk[quad * 4 + k]).astype(BF16).astype(F32)
            for j in range(latent // 128):
                q_buf[j, pl.ds(quad * 4 + k, tok, stride=heads)] = q_lat[:, j * 128:(j + 1) * 128]
        for k in range(2):
            val = q_rope[:, k * 128:(k + 1) * 128]
            swap = jnp.where(first_half, pltpu.roll(val, 128 - rope // 2, 1), pltpu.roll(val, rope // 2, 1))
            rot = (val * cos_ref[...] + swap * sin_ref[...]).astype(BF16).astype(F32)
            q_buf[latent // 128, pl.ds(quad * 4 + 2 * k, tok, stride=heads)] = rot
            q_buf[latent // 128, pl.ds(quad * 4 + 2 * k + 1, tok, stride=heads)] = pltpu.roll(rot, rope, 1)

    place = lax.broadcasted_iota(jnp.int32, (heads, cache_hbm.shape[2]), 1)

    @pl.loop(0, n_group)
    def _(group):
        slot = lax.rem(group, RING)
        ring_copy(group, slot).wait()
        @pl.loop(0, GROUP // SUB)
        def _(sub):
            for k in range(SUB):
                at = sub * SUB + k
                t = group * GROUP + at
                rows = pl.ds(pl.multiple_of(t * heads, heads), heads)
                q_cat = jnp.concatenate([q_buf[j, rows] for j in range(latent // 128 + 1)], axis=1)[:, :span].astype(BF16)
                score = dot_n(q_cat, ring[slot, at]) * scale
                score = jnp.where(place < lens_ref[t], score, -1e30)
                top = jnp.max(score, axis=1, keepdims=True)
                num = jnp.exp(score - top)
                p_buf[at] = (num * (1.0 / jnp.sum(num, axis=1, keepdims=True))).astype(BF16)

        @pl.loop(0, GROUP // SUB)
        def _(sub):
            for k in range(SUB):
                at = sub * SUB + k
                rows = pl.ds(pl.multiple_of((group * GROUP + at) * heads, heads), heads)
                o_lat = dot_t(p_buf[at], ring[slot, at, pl.ds(0, latent)])
                for j in range(latent // 128):
                    o_buf[j, rows] = o_lat[:, j * 128:(j + 1) * 128]

        @pl.when(group + RING < n_group)
        def _():
            ring_copy(group + RING, slot).start()


    uv_cp.wait()

    @pl.loop(0, heads, unroll=8)
    def _(h):
        o_lat = jnp.concatenate([o_buf[j, pl.ds(h, tok, stride=heads)] for j in range(latent // 128)], axis=1).astype(BF16)
        vals = dot_n(o_lat, uv[h]).astype(BF16)
        ov_buf[:, pl.ds(pl.multiple_of(h * nope, nope), nope)] = vals

    wo_cp.wait()
    for off in range(0, hid, 512):
        cols = pl.ds(off, 512)
        att = dot_n(ov_buf[...], wo[:, cols])
        h_ref[:, cols] = (x_ref[:, cols].astype(F32) + att).astype(BF16)
    u_ref[:, pl.ds(0, hid)] = norm(h_ref[...].astype(F32))
    if with_table:
        u_ref[:, pl.ds(hid, 128)] = table_ref[...]


def att_call(x, cache, kv_lens, cos, sin, w_q, w_uk, w_uv, w_o, table=None):
    tok, hid = x.shape
    heads, nope, latent = w_uk.shape
    val_dim = w_uv.shape[2]
    assert val_dim == nope
    qk_dim = w_q.shape[2]
    pos = cache.shape[1]
    span = cache.shape[2]
    with_table = table is not None
    vmem, hbm = pl.BlockSpec(memory_space=pltpu.VMEM), pl.BlockSpec(memory_space=pl.ANY)
    smem = pl.BlockSpec(memory_space=pltpu.SMEM)
    args = [kv_lens, x, cos, sin] + ([table] if with_table else [])
    args += [w_q.transpose(1, 2, 0), w_uk, w_uv, w_o.reshape(heads * val_dim, hid), cache.transpose(0, 2, 1)]
    width = hid + (128 if with_table else 0)
    return pl.pallas_call(
        functools.partial(att_kernel, with_table),
        out_shape=[jax.ShapeDtypeStruct((tok, hid), BF16), jax.ShapeDtypeStruct((tok, width), BF16)],
        in_specs=[smem] + [vmem] * (4 if with_table else 3) + [hbm] * 5,
        out_specs=[vmem, vmem],
        scratch_shapes=[
            pltpu.VMEM((heads, qk_dim, hid), BF16),
            pltpu.VMEM((heads, nope, latent), BF16),
            pltpu.VMEM((heads, latent, val_dim), BF16),
            pltpu.VMEM((heads * val_dim, hid), BF16),
            pltpu.VMEM((RING, GROUP, span, pos), BF16),
            pltpu.VMEM((tok, hid), BF16),
            pltpu.VMEM((latent // 128 + 1, tok * heads, 128), F32),
            pltpu.VMEM((latent // 128, tok * heads, 128), F32),
            pltpu.VMEM((tok, heads * val_dim), BF16),
            pltpu.VMEM((GROUP, heads, pos), BF16),
            pltpu.SemaphoreType.DMA((7,)),
            pltpu.SemaphoreType.DMA((RING,)),
        ],
        compiler_params=pltpu.CompilerParams(vmem_limit_bytes=VMEM_LIMIT),
        cost_estimate=pl.CostEstimate(flops=6 * tok * hid * 3072, bytes_accessed=54_000_000, transcendentals=0),
        name='latent_attention',
    )(*args)


def rope_tables(kv_lens, rope):
    half = rope // 2
    inv_freq = 10000.0 ** (-2.0 * jnp.arange(half, dtype=F32) / rope)
    angle = kv_lens.astype(F32)[:, None] * inv_freq
    cos, sin = jnp.cos(angle), jnp.sin(angle)
    return jnp.concatenate([cos] * 4, axis=1), jnp.concatenate([-sin, sin, -sin, sin], axis=1)


def by_expert(route_ids, vals, n_dev):
    return jnp.sum(jnp.where(route_ids[:, :, None] == jnp.arange(n_dev)[None, None, :], vals[:, :, None], 0.0), axis=1)


def slot_ranks(route_ids, n_dev):
    tok = route_ids.shape[0]
    member = jnp.any(route_ids[:, :, None] == jnp.arange(n_dev)[None, None, :], axis=1)
    before = (jnp.arange(tok)[:, None] > jnp.arange(tok)[None, :]).astype(BF16)
    rank = jnp.dot(before, member.astype(BF16), preferred_element_type=F32)
    return jnp.where(member, rank, -1.0)


def mix_matrix(ranks, wts):
    tok, n_exp = ranks.shape
    pieces, rest = [], wts
    for _ in range(3):
        top = lax.reduce_precision(rest, 8, 7)
        pieces.append(top)
        rest = rest - top
    hit = ranks[:, :, None] == jnp.arange(SLOT_CAP, dtype=F32)[None, None, :]
    return jnp.concatenate([jnp.where(hit, p[:, :, None], 0.0).astype(BF16).reshape(tok, n_exp * SLOT_CAP) for p in pieces], axis=0)


def apply_mix(mat, back):
    tok = mat.shape[0] // 3
    mixed = jnp.dot(mat, back, preferred_element_type=F32)
    return (mixed[2 * tok:] + mixed[tok:2 * tok]) + mixed[:tok]


def solution(mesh):
    n_dev = mesh.shape['tp'] * mesh.shape['ep']
    n_ep = mesh.shape['ep']
    rows_spec = P(FLAT_AXES, None)
    cube_spec = P(FLAT_AXES, None, None)
    whole_spec = P(None, None, None)
    col_split = P(None, 'tp')
    row_split = P('tp', None)
    in_specs = (rows_spec, cube_spec, cube_spec, P(FLAT_AXES), rows_spec, rows_spec,
                whole_spec, whole_spec, whole_spec, whole_spec, whole_spec, whole_spec, whole_spec, whole_spec,
                col_split, col_split, row_split, col_split, col_split, row_split,
                cube_spec, cube_spec, cube_spec)

    def body(hidden_in, cache0, cache1, kv_lens, route_ids, route_wts, att0_q, att0_uk, att0_uv, att0_o, att1_q, att1_uk, att1_uv, att1_o, ffn0_gate, ffn0_up, ffn0_down, ffn1_gate, ffn1_up, ffn1_down, exp_gate, exp_up, exp_down):
        hid = hidden_in.shape[1]
        ranks = slot_ranks(route_ids, n_dev)
        wts = by_expert(route_ids, route_wts, n_dev)
        zero_wt = jnp.sum(jnp.where(route_ids >= n_dev, route_wts, 0.0), axis=1)
        table = jnp.pad(ranks, ((0, 0), (0, 128 - n_dev))).astype(BF16)
        mine = jnp.concatenate([ranks, wts], axis=1)
        theirs = lax.ppermute(mine, 'tp', [(0, 1), (1, 0)])
        low_plane = lax.axis_index('tp') == 0

        def plane_matrix(pair):
            ranks_at = jnp.where(low_plane, pair[:, :n_ep], pair[:, n_ep:n_dev])
            wts_at = jnp.where(low_plane, pair[:, n_dev:n_dev + n_ep], pair[:, n_dev + n_ep:])
            return mix_matrix(ranks_at, wts_at)

        mat_near, mat_far = plane_matrix(mine), plane_matrix(theirs)
        cos, sin = rope_tables(kv_lens, att0_q.shape[2] - att0_uk.shape[1])
        h_zero, u_ext = att_call(hidden_in, cache0, kv_lens, cos, sin, att0_q, att0_uk, att0_uv, att0_o, table)
        f_zero, near, far = dense_call(u_ext, h_zero, ffn0_gate.T, ffn0_up.T, ffn0_down, BF16, expert=(exp_gate, exp_up, exp_down))
        back_far = lax.all_to_all(far, 'ep', 0, 0, tiled=True)
        h_one, u_one = att_call(f_zero, cache1, kv_lens, cos, sin, att1_q, att1_uk, att1_uv, att1_o)
        near, back_far, h_one = lax.optimization_barrier((near, back_far, h_one))
        back_near = lax.all_to_all(near, 'ep', 0, 0, tiled=True)
        dense_one, = dense_call(u_one, h_one, ffn1_gate.T, ffn1_up.T, ffn1_down, F32, mix=apply_mix(mat_far, back_far))
        mix = apply_mix(mat_near, back_near) + zero_wt[:, None] * u_ext[:, :hid].astype(F32)
        return (dense_one + mix).astype(BF16)

    return jax.shard_map(body, mesh=mesh, in_specs=in_specs, out_specs=rows_spec, check_vma=False)
```

```python
import functools

import jax
import jax.numpy as jnp
from jax import lax
from jax.experimental import pallas as pl
from jax.experimental.pallas import tpu as pltpu
from jax.sharding import PartitionSpec as P

FLAT_AXES = ('tp', 'ep')
MESH = pl.DeviceIdType.MESH
F32, BF16 = jnp.float32, jnp.bfloat16
SLOT_CAP = 72
VMEM_LIMIT = 66_000_000


def dot_t(lhs, rhs):
    return lax.dot_general(lhs, rhs, (((1,), (1,)), ((), ())), preferred_element_type=F32)


def dot_n(lhs, rhs):
    return jnp.dot(lhs, rhs, preferred_element_type=F32)


TILE = 512
COLS = 256


def exchange_copies(src, dst, send_sem, recv_sem, z, e):
    n_ep = src.shape[0] // SLOT_CAP
    copies = []
    for k in range(1, n_ep):
        peer = lax.rem(e + k, n_ep)
        target = dst.at[e] if len(dst.shape) == 3 else dst.at[pl.ds(pl.multiple_of(e * SLOT_CAP, 8), SLOT_CAP)]
        copies.append(pltpu.make_async_remote_copy(
            src_ref=src.at[pl.ds(pl.multiple_of(peer * SLOT_CAP, 8), SLOT_CAP)], dst_ref=target, send_sem=send_sem.at[k],
            recv_sem=recv_sem.at[k], device_id=(z, peer), device_id_type=MESH))
    return copies


def ffn_kernel(with_expert, *refs):
    refs = list(refs)
    u_ref, h_ref, gate_hbm, up_hbm, down_hbm = refs[:5]
    del refs[:5]
    if with_expert:
        eg_hbm, eu_hbm, ed_hbm = refs[:3]
        del refs[:3]
    else:
        near_hbm, far_hbm, mat_near, mat_far, u0_ref, zero_ref = refs[:6]
        del refs[:6]
    out_ref = refs.pop(0)
    if with_expert:
        near_hbm, far_hbm = refs[:2]
        del refs[:2]
    blocks, rows_ref, act_ref, gate_w, up_w, down_w, part_buf, z_out, z_in, d_out, d_in, p_out, p_in = refs[:13]
    w_sem, ex_send, ex_recv, z_send, z_recv, d_send, d_recv, p_send, p_recv, own_sem = refs[13:23]
    if with_expert:
        x_buf, h_buf, e_buf, ew_sem, eo_sem = refs[23:]
    else:
        near_in, far_in, n_send, n_recv, far_sem = refs[23:]

    tok, hid = h_ref.shape
    ff = gate_w.shape[0]
    n_full, tail = ff // TILE, ff % TILE
    n_col = hid // COLS
    k_main = (ff // 256) * 256

    z = lax.axis_index('tp')
    e = lax.axis_index('ep')
    y, x, c = e // 4, (e // 2) % 2, e % 2
    zn = (1 - z, e)
    cn = (z, e + 1 - 2 * c)
    base = pl.multiple_of(c * ff, 16)

    def tile_copies(step, rows):
        at = pl.multiple_of(step * TILE, TILE)
        return [pltpu.make_async_copy(hbm.at[pl.ds(pl.multiple_of(base + at, 16), rows)], buf.at[pl.ds(at, rows)], w_sem.at[k, step])
                for k, (hbm, buf) in enumerate(((gate_hbm, gate_w), (up_hbm, up_w)))]

    down_cp = pltpu.make_async_copy(down_hbm.at[pl.ds(base, ff)], down_w, w_sem.at[2, 0])
    for step in range(n_full):
        for cp in tile_copies(step, TILE):
            cp.start()
    for cp in tile_copies(n_full, tail):
        cp.start()

    if with_expert:
        me = z * 8 + e
        xn = (z, e + 2 - 4 * x)
        yn = (z, e + 4 - 8 * y)
        peers = (zn, cn, xn, yn)
    else:
        n_ep = near_in.shape[0]
        peers = (zn,) + tuple((z, lax.rem(e + k, n_ep)) for k in range(1, n_ep))
    barrier = pltpu.get_barrier_semaphore()
    for peer in peers:
        pl.semaphore_signal(barrier, inc=1, device_id=peer, device_id_type=MESH)
    pl.semaphore_wait(barrier, len(peers))

    def remote(k, src, dst, peer):
        return pltpu.make_async_remote_copy(src_ref=src, dst_ref=dst, send_sem=ex_send.at[k], recv_sem=ex_recv.at[k],
                                            device_id=peer, device_id_type=MESH)

    if with_expert:
        half = tok // 2
        lo, hi = pl.ds(0, half), pl.ds(half, half)

        def plane(z_at):
            first = z_at * 8
            return (first + e, first + e + 2 - 4 * x, first + e + 4 - 8 * y,
                    first + (1 - y) * 4 + (1 - x) * 2 + c)

        def plane_sends(first, blks, own_src):
            own, xb, yb, db = blks
            return {
                'x': remote(first, own_src, blocks.at[own], xn),
                'y': remote(first + 1, own_src, blocks.at[own], yn),
                'xr': remote(first + 2, blocks.at[yb, hi], blocks.at[yb, hi], xn),
                'yr': remote(first + 3, blocks.at[xb, lo], blocks.at[xb, lo], yn),
                'c0': remote(first + 4, own_src, blocks.at[own], cn),
                'c1': remote(first + 5, blocks.at[xb], blocks.at[xb], cn),
                'c2': remote(first + 6, blocks.at[yb], blocks.at[yb], cn),
                'c3': remote(first + 7, blocks.at[db], blocks.at[db], cn),
            }

        def start_relay(s):
            s['x'].wait_recv()
            s['y'].wait_recv()
            s['xr'].start()
            s['yr'].start()
            s['c1'].start()
            s['c2'].start()

        def start_last(s):
            s['xr'].wait_recv()
            s['yr'].wait_recv()
            s['c3'].start()

        z_blk = (1 - z) * 8 + e
        c_blk = z * 8 + e + 1 - 2 * c
        zc_blk = (1 - z) * 8 + e + 1 - 2 * c
        sa = plane_sends(1, plane(z), u_ref)
        sb = plane_sends(9, plane(1 - z), blocks.at[z_blk])
        z_copy = remote(0, u_ref, blocks.at[me], zn)
        ca_copy, cb_copy = sa['c0'], sb['c0']
        own_cp = pltpu.make_async_copy(u_ref, blocks.at[me], own_sem.at[0])
        own_cp.start()
    else:
        z_blk, c_blk, zc_blk = 0, 1, 2
        z_copy = remote(0, u_ref, blocks.at[0], zn)
        ca_copy = remote(1, u_ref, blocks.at[1], cn)
        cb_copy = remote(2, blocks.at[0], blocks.at[2], cn)
        near_copies = exchange_copies(near_hbm, near_in, n_send, n_recv, z, e)
        own_cp = pltpu.make_async_copy(near_hbm.at[pl.ds(e * SLOT_CAP, SLOT_CAP)], near_in.at[e], own_sem.at[0])
        far_cp = pltpu.make_async_copy(far_hbm, far_in, far_sem.at[0])

    z_copy.start()
    ca_copy.start()
    if with_expert:
        sa['x'].start()
        sa['y'].start()
    else:
        for cp in near_copies:
            cp.start()
    rows_ref[pl.ds(0, tok)] = u_ref[:, pl.ds(0, hid)]
    ca_copy.wait_recv()
    rows_ref[pl.ds(tok, tok)] = blocks[c_blk, :, pl.ds(0, hid)]

    def swiglu_tile(first, at, rows):
        lhs = rows_ref[pl.ds(first, 2 * tok)]
        gate_val = dot_t(lhs, gate_w[pl.ds(at, rows)])
        up_val = dot_t(lhs, up_w[pl.ds(at, rows)])
        act_ref[pl.ds(first, 2 * tok), pl.ds(at, rows)] = (jax.nn.silu(gate_val) * up_val).astype(BF16)

    @pl.loop(0, n_full)
    def _(step):
        for cp in tile_copies(step, TILE):
            cp.wait()
        swiglu_tile(0, pl.multiple_of(step * TILE, TILE), TILE)

        @pl.when(step == 2)
        def _():
            down_cp.start()

    for cp in tile_copies(n_full, tail):
        cp.wait()
    swiglu_tile(0, n_full * TILE, tail)

    z_copy.wait_recv()
    cb_copy.start()
    if with_expert:
        start_relay(sa)
        sb['x'].start()
        sb['y'].start()
    else:
        own_cp.start()
        far_cp.start()
    rows_ref[pl.ds(2 * tok, tok)] = blocks[z_blk, :, pl.ds(0, hid)]
    cb_copy.wait_recv()
    rows_ref[pl.ds(3 * tok, tok)] = blocks[zc_blk, :, pl.ds(0, hid)]

    @pl.loop(0, n_full)
    def _(step):
        swiglu_tile(2 * tok, pl.multiple_of(step * TILE, TILE), TILE)

    swiglu_tile(2 * tok, n_full * TILE, tail)

    if with_expert:
        eg, eu, ed = (gate_w.at[pl.ds(0, hid), pl.ds(0, eg_hbm.shape[2])], up_w.at[pl.ds(0, hid), pl.ds(0, eg_hbm.shape[2])],
                      down_w.at[pl.ds(0, ed_hbm.shape[1])])
        eg_cp, eu_cp, ed_cp = (pltpu.make_async_copy(s.at[0], d, ew_sem.at[k])
                               for k, (s, d) in enumerate(((eg_hbm, eg), (eu_hbm, eu), (ed_hbm, ed))))
        eg_cp.start()
        eu_cp.start()
        start_last(sa)

    def link(src, dst, sems, rems, col, peer):
        return pltpu.make_async_remote_copy(src_ref=src.at[col], dst_ref=dst.at[col], send_sem=sems.at[col],
                                            recv_sem=rems.at[col], device_id=peer, device_id_type=MESH)

    def z_link(col):
        return link(z_out, z_in, z_send, z_recv, col, zn)

    def d_link(col):
        return link(d_out, d_in, d_send, d_recv, col, cn)

    def p_link(col):
        return link(p_out, p_in, p_send, p_recv, col, cn)

    def down_tile(first, col):
        cols = pl.ds(pl.multiple_of(col * COLS, COLS), COLS)
        lhs = act_ref.at[pl.ds(first, 2 * tok)]
        val = dot_n(lhs[:, pl.ds(0, k_main)], down_w[pl.ds(0, k_main), cols])
        return val + dot_n(lhs[:, pl.ds(k_main, ff - k_main)], down_w[pl.ds(k_main, ff - k_main), cols])

    def mixed(mat, back):
        val = dot_n(mat[...], back)
        return (val[2 * tok:] + val[tok:2 * tok]) + val[:tok]

    def send_z(col):
        d_link(col).wait_recv()
        total = z_out[col] + d_in[col]
        if not with_expert:
            total += mixed(mat_far, far_in[:, pl.ds(pl.multiple_of(col * COLS, COLS), COLS)])
        z_out[col] = total
        z_link(col).start()

    down_cp.wait()
    if not with_expert:
        far_cp.wait()

    @pl.loop(0, n_col)
    def _(col):
        val = down_tile(2 * tok, col)
        z_out[col] = val[:tok]
        d_out[col] = val[tok:]
        d_link(col).start()

        @pl.when(col >= 2)
        def _():
            send_z(col - 2)

    send_z(n_col - 2)
    send_z(n_col - 1)

    @pl.loop(0, n_col)
    def _(col):
        val = down_tile(0, col)
        part_buf[col] = val[:tok]
        p_out[col] = val[tok:]
        p_link(col).start()

    if with_expert:
        ed_cp.start()
        own_cp.wait()
        eg_cp.wait()
        eu_cp.wait()
        lane = lax.broadcasted_iota(jnp.int32, (tok, 128), 1)
        slot_id = lax.broadcasted_iota(jnp.int32, (tok, 2 * SLOT_CAP), 1).astype(F32)
        q_rows = 4 * SLOT_CAP

        def eo_copy(it, buf, dst, yq):
            return pltpu.make_async_copy(e_buf.at[buf], dst.at[pl.ds(pl.multiple_of(yq * q_rows, q_rows), q_rows)], eo_sem.at[buf])

        @pl.loop(0, 4)
        def _(it):
            @pl.when(it == 0)
            def _():
                sa['c1'].wait_recv()

            @pl.when(it == 1)
            def _():
                start_relay(sb)
                sa['c2'].wait_recv()
                sa['c3'].wait_recv()

            @pl.when(it == 2)
            def _():
                start_last(sb)
                sb['c1'].wait_recv()

            @pl.when(it == 3)
            def _():
                sb['c2'].wait_recv()
                sb['c3'].wait_recv()

            zq = lax.rem(z + it // 2, 2)
            yq = lax.rem(y + it, 2)
            buf = lax.rem(it, 2)
            for pair in range(2):
                acc = None
                for k in range(2):
                    blk = zq * 8 + yq * 4 + pair * 2 + k
                    table = blocks[blk, :, pl.ds(hid, 128)].astype(F32)
                    rank = jnp.sum(jnp.where(lane == me, table, 0.0), axis=1, keepdims=True)
                    want = jnp.where(rank >= 0.0, rank + k * SLOT_CAP, -1.0)
                    hot = jnp.where(slot_id == want, 1.0, 0.0).astype(BF16)
                    got = lax.dot_general(hot, blocks[blk, :, pl.ds(0, hid)], (((0,), (0,)), ((), ())),
                                          preferred_element_type=F32)
                    acc = got if acc is None else acc + got
                x_buf[pl.ds(pair * 2 * SLOT_CAP, 2 * SLOT_CAP)] = acc.astype(BF16)
            for off, width in ((0, 512), (512, 512), (1024, 384)):
                gate_val = dot_n(x_buf[...], eg[:, pl.ds(off, width)])
                up_val = dot_n(x_buf[...], eu[:, pl.ds(off, width)])
                h_buf[:, pl.ds(off, width)] = (jax.nn.silu(gate_val) * up_val).astype(BF16)

            @pl.when(it == 0)
            def _():
                ed_cp.wait()

            @pl.when(it >= 2)
            def _():
                eo_copy(it, buf, near_hbm, yq).wait()

            for off in range(0, hid, 512):
                e_buf[buf, :, pl.ds(off, 512)] = dot_n(h_buf[...], ed[:, pl.ds(off, 512)]).astype(BF16)

            @pl.when(it < 2)
            def _():
                eo_copy(it, buf, near_hbm, yq).start()

            @pl.when(it >= 2)
            def _():
                eo_copy(it, buf, far_hbm, yq).start()

        eo_copy(0, 0, far_hbm, 0).wait()
        eo_copy(0, 1, far_hbm, 0).wait()

    if not with_expert:
        own_cp.wait()
        for cp in near_copies:
            cp.wait_recv()

    @pl.loop(0, n_col)
    def _(col):
        p_link(col).wait()
        d_link(col).wait_send()
        z_link(col).wait()
        cols = pl.ds(pl.multiple_of(col * COLS, COLS), COLS)
        total = h_ref[:, cols].astype(F32) + ((part_buf[col] + p_in[col]) + z_in[col])
        if not with_expert:
            back = jnp.concatenate([near_in[k, :, cols] for k in range(n_ep)], axis=0)
            total += mixed(mat_near, back) + zero_ref[...] * u0_ref[:, cols].astype(F32)
        out_ref[:, cols] = total.astype(out_ref.dtype)

    z_copy.wait_send()
    if with_expert:
        for s in (sa, sb):
            for cp in s.values():
                cp.wait_send()
    else:
        ca_copy.wait_send()
        cb_copy.wait_send()
        for cp in near_copies:
            cp.wait_send()


def dense_call(u, h, w_gate_t, w_up_t, w_down, expert=None, mix=None):
    tok, hid = h.shape
    ff = w_gate_t.shape[0] // 2
    width = u.shape[1]
    with_expert = expert is not None
    vmem, hbm = pl.BlockSpec(memory_space=pltpu.VMEM), pl.BlockSpec(memory_space=pl.ANY)
    n_col = hid // COLS
    n_step = ff // TILE + 1
    args = [u, h, w_gate_t, w_up_t, w_down]
    in_specs = [vmem, vmem, hbm, hbm, hbm]
    out_shape = [jax.ShapeDtypeStruct((tok, hid), BF16)]
    out_specs = [vmem]
    n_ex = 17 if with_expert else 3
    dma = pltpu.SemaphoreType.DMA
    scratch = [pltpu.VMEM((16 if with_expert else 3, tok, width), BF16), pltpu.VMEM((4 * tok, hid), BF16),
               pltpu.VMEM((4 * tok, n_step * TILE), BF16),
               pltpu.VMEM((ff, hid), BF16), pltpu.VMEM((ff, hid), BF16), pltpu.VMEM((ff, hid), BF16)]
    scratch += [pltpu.VMEM((n_col, tok, COLS), F32)] * 7
    scratch += [dma((3, n_step)), dma((n_ex,)), dma((n_ex,))] + [dma((n_col,))] * 6 + [dma((1,))]
    flops = 2 * 2 * tok * hid * ff * 6
    if with_expert:
        inner = expert[0].shape[2]
        args += list(expert)
        in_specs += [hbm, hbm, hbm]
        out_shape += [jax.ShapeDtypeStruct((8 * SLOT_CAP, hid), BF16)] * 2
        out_specs += [hbm, hbm]
        scratch += [pltpu.VMEM((4 * SLOT_CAP, hid), BF16), pltpu.VMEM((4 * SLOT_CAP, inner), BF16),
                    pltpu.VMEM((2, 4 * SLOT_CAP, hid), BF16), dma((3,)), dma((2,))]
        flops += 2 * 16 * SLOT_CAP * hid * inner * 3
    else:
        args += list(mix)
        in_specs += [hbm, hbm, vmem, vmem, vmem, vmem]
        n_ep = mix[0].shape[0] // SLOT_CAP
        scratch += [pltpu.VMEM((n_ep, SLOT_CAP, hid), BF16), pltpu.VMEM((n_ep * SLOT_CAP, hid), BF16),
                    dma((n_ep,)), dma((n_ep,)), dma((1,))]
    return pl.pallas_call(
        functools.partial(ffn_kernel, with_expert),
        out_shape=out_shape, in_specs=in_specs, out_specs=out_specs, scratch_shapes=scratch,
        compiler_params=pltpu.CompilerParams(collective_id=0 if with_expert else 1, has_side_effects=True,
                                             vmem_limit_bytes=VMEM_LIMIT),
        cost_estimate=pl.CostEstimate(flops=flops, bytes_accessed=6 * hid * ff, transcendentals=0),
        name='dense_expert' if with_expert else 'dense',
    )(*args)


GROUP = 16
RING = 4
SUB = 16


def att_kernel(with_table, with_far, *refs):
    refs = list(refs)
    lens_ref, x_ref, cos_ref, sin_ref = refs[:4]
    del refs[:4]
    table_ref = refs.pop(0) if with_table else None
    far_hbm = refs.pop(0) if with_far else None
    wq_hbm, uk_hbm, uv_hbm, wo_hbm, cache_hbm, h_ref, u_ref = refs[:7]
    del refs[:7]
    back_hbm = refs.pop(0) if with_far else None
    wq, uk, uv, wo, ring, xn_buf, q_buf, o_buf, ov_buf, p_buf, w_sem, ring_sem = refs[:12]
    if with_far:
        own_buf, own_sem, f_send, f_recv = refs[12:]
    tok, hid = x_ref.shape
    heads, nope, latent = uk.shape
    qk_dim = wq.shape[1]
    rope = qk_dim - nope
    scale = qk_dim ** -0.5
    n_group = tok // GROUP
    span = latent + rope

    def head_copy(quad):
        return pltpu.make_async_copy(wq_hbm.at[pl.ds(quad * 4, 4)], wq.at[pl.ds(quad * 4, 4)], w_sem.at[quad])

    def ring_copy(group, slot):
        return pltpu.make_async_copy(cache_hbm.at[pl.ds(group * GROUP, GROUP)], ring.at[slot], ring_sem.at[slot])

    uk_cp = pltpu.make_async_copy(uk_hbm, uk, w_sem.at[4])
    uv_cp = pltpu.make_async_copy(uv_hbm, uv, w_sem.at[5])
    wo_cp = pltpu.make_async_copy(wo_hbm, wo, w_sem.at[6])
    head_copy(0).start()
    uk_cp.start()
    for quad in range(1, heads // 4):
        head_copy(quad).start()

    if with_far:
        z = lax.axis_index('tp')
        e = lax.axis_index('ep')
        n_ep = far_hbm.shape[0] // SLOT_CAP
        barrier = pltpu.get_barrier_semaphore()
        for k in range(1, n_ep):
            pl.semaphore_signal(barrier, inc=1, device_id=(z, lax.rem(e + k, n_ep)), device_id_type=MESH)
        pl.semaphore_wait(barrier, n_ep - 1)
        far_copies = exchange_copies(far_hbm, back_hbm, f_send, f_recv, z, e)
        for cp in far_copies:
            cp.start()
        own_rows = pl.ds(pl.multiple_of(e * SLOT_CAP, 8), SLOT_CAP)
        own_in = pltpu.make_async_copy(far_hbm.at[own_rows], own_buf, own_sem.at[0])
        own_out = pltpu.make_async_copy(own_buf, back_hbm.at[own_rows], own_sem.at[1])
        own_in.start()

    def norm(val):
        return (val * lax.rsqrt(jnp.mean(val * val, axis=-1, keepdims=True) + 1e-6)).astype(BF16)

    xn_buf[...] = norm(x_ref[...].astype(F32))
    uk_cp.wait()
    lane = lax.broadcasted_iota(jnp.int32, (tok, 128), 1)
    first_half = lax.rem(lane, rope) < rope // 2

    @pl.loop(0, heads // 4)
    def _(quad):
        head_copy(quad).wait()

        @pl.when(quad == 0)
        def _():
            for group in range(RING):
                ring_copy(group, group).start()

        @pl.when(quad == 3)
        def _():
            uv_cp.start()
            wo_cp.start()

        w_nope = jnp.concatenate([wq[quad * 4 + k, pl.ds(0, nope)] for k in range(4)], axis=0)
        w_rope = jnp.concatenate([wq[quad * 4 + k, pl.ds(nope, rope)] for k in range(4)], axis=0)
        q_nope = dot_t(xn_buf[...], w_nope).astype(BF16)
        q_rope = dot_t(xn_buf[...], w_rope).astype(BF16).astype(F32)
        for k in range(4):
            q_lat = dot_n(q_nope[:, k * nope:(k + 1) * nope], uk[quad * 4 + k]).astype(BF16).astype(F32)
            for j in range(latent // 128):
                q_buf[j, pl.ds(quad * 4 + k, tok, stride=heads)] = q_lat[:, j * 128:(j + 1) * 128]
        for k in range(2):
            val = q_rope[:, k * 128:(k + 1) * 128]
            swap = jnp.where(first_half, pltpu.roll(val, 128 - rope // 2, 1), pltpu.roll(val, rope // 2, 1))
            rot = (val * cos_ref[...] + swap * sin_ref[...]).astype(BF16).astype(F32)
            q_buf[latent // 128, pl.ds(quad * 4 + 2 * k, tok, stride=heads)] = rot
            q_buf[latent // 128, pl.ds(quad * 4 + 2 * k + 1, tok, stride=heads)] = pltpu.roll(rot, rope, 1)

    place = lax.broadcasted_iota(jnp.int32, (heads, cache_hbm.shape[2]), 1)

    @pl.loop(0, n_group)
    def _(group):
        slot = lax.rem(group, RING)
        ring_copy(group, slot).wait()
        @pl.loop(0, GROUP // SUB)
        def _(sub):
            for k in range(SUB):
                at = sub * SUB + k
                t = group * GROUP + at
                rows = pl.ds(pl.multiple_of(t * heads, heads), heads)
                q_cat = jnp.concatenate([q_buf[j, rows] for j in range(latent // 128 + 1)], axis=1)[:, :span].astype(BF16)
                score = dot_n(q_cat, ring[slot, at]) * scale
                score = jnp.where(place < lens_ref[t], score, -1e30)
                top = jnp.max(score, axis=1, keepdims=True)
                num = jnp.exp(score - top)
                p_buf[at] = (num * (1.0 / jnp.sum(num, axis=1, keepdims=True))).astype(BF16)

        @pl.loop(0, GROUP // SUB)
        def _(sub):
            for k in range(SUB):
                at = sub * SUB + k
                rows = pl.ds(pl.multiple_of((group * GROUP + at) * heads, heads), heads)
                o_lat = dot_t(p_buf[at], ring[slot, at, pl.ds(0, latent)])
                for j in range(latent // 128):
                    o_buf[j, rows] = o_lat[:, j * 128:(j + 1) * 128]

        @pl.when(group + RING < n_group)
        def _():
            ring_copy(group + RING, slot).start()


    uv_cp.wait()
    if with_far:
        own_in.wait()
        own_out.start()

    @pl.loop(0, heads, unroll=8)
    def _(h):
        o_lat = jnp.concatenate([o_buf[j, pl.ds(h, tok, stride=heads)] for j in range(latent // 128)], axis=1).astype(BF16)
        vals = dot_n(o_lat, uv[h]).astype(BF16)
        ov_buf[:, pl.ds(pl.multiple_of(h * nope, nope), nope)] = vals

    wo_cp.wait()
    for off in range(0, hid, 512):
        cols = pl.ds(off, 512)
        att = dot_n(ov_buf[...], wo[:, cols])
        h_ref[:, cols] = (x_ref[:, cols].astype(F32) + att).astype(BF16)
    u_ref[:, pl.ds(0, hid)] = norm(h_ref[...].astype(F32))
    if with_table:
        u_ref[:, pl.ds(hid, 128)] = table_ref[...]
    if with_far:
        own_out.wait()
        for cp in far_copies:
            cp.wait()


def att_call(x, cache, kv_lens, cos, sin, w_q, w_uk, w_uv, w_o, table=None, far=None):
    tok, hid = x.shape
    heads, nope, latent = w_uk.shape
    val_dim = w_uv.shape[2]
    assert val_dim == nope
    qk_dim = w_q.shape[2]
    pos = cache.shape[1]
    span = cache.shape[2]
    with_table = table is not None
    vmem, hbm = pl.BlockSpec(memory_space=pltpu.VMEM), pl.BlockSpec(memory_space=pl.ANY)
    smem = pl.BlockSpec(memory_space=pltpu.SMEM)
    with_far = far is not None
    args = [kv_lens, x, cos, sin] + ([table] if with_table else []) + ([far] if with_far else [])
    args += [w_q.transpose(1, 2, 0), w_uk, w_uv, w_o.reshape(heads * val_dim, hid), cache.transpose(0, 2, 1)]
    width = hid + (128 if with_table else 0)
    out_shape = [jax.ShapeDtypeStruct((tok, hid), BF16), jax.ShapeDtypeStruct((tok, width), BF16)]
    out_specs = [vmem, vmem]
    extra, params = [], {}
    if with_far:
        n_ep = far.shape[0] // SLOT_CAP
        out_shape.append(jax.ShapeDtypeStruct(far.shape, BF16))
        out_specs.append(hbm)
        dma = pltpu.SemaphoreType.DMA
        extra = [pltpu.VMEM((SLOT_CAP, hid), BF16), dma((2,)), dma((n_ep,)), dma((n_ep,))]
        params = {'collective_id': 2, 'has_side_effects': True}
    return pl.pallas_call(
        functools.partial(att_kernel, with_table, with_far),
        out_shape=out_shape,
        in_specs=[smem] + [vmem] * (4 if with_table else 3) + [hbm] * (6 if with_far else 5),
        out_specs=out_specs,
        scratch_shapes=[
            pltpu.VMEM((heads, qk_dim, hid), BF16),
            pltpu.VMEM((heads, nope, latent), BF16),
            pltpu.VMEM((heads, latent, val_dim), BF16),
            pltpu.VMEM((heads * val_dim, hid), BF16),
            pltpu.VMEM((RING, GROUP, span, pos), BF16),
            pltpu.VMEM((tok, hid), BF16),
            pltpu.VMEM((latent // 128 + 1, tok * heads, 128), F32),
            pltpu.VMEM((latent // 128, tok * heads, 128), F32),
            pltpu.VMEM((tok, heads * val_dim), BF16),
            pltpu.VMEM((GROUP, heads, pos), BF16),
            pltpu.SemaphoreType.DMA((7,)),
            pltpu.SemaphoreType.DMA((RING,)),
        ] + extra,
        compiler_params=pltpu.CompilerParams(vmem_limit_bytes=VMEM_LIMIT, **params),
        cost_estimate=pl.CostEstimate(flops=6 * tok * hid * 3072, bytes_accessed=54_000_000, transcendentals=0),
        name='latent_attention',
    )(*args)


def rope_tables(kv_lens, rope):
    half = rope // 2
    inv_freq = 10000.0 ** (-2.0 * jnp.arange(half, dtype=F32) / rope)
    angle = kv_lens.astype(F32)[:, None] * inv_freq
    cos, sin = jnp.cos(angle), jnp.sin(angle)
    return jnp.concatenate([cos] * 4, axis=1), jnp.concatenate([-sin, sin, -sin, sin], axis=1)


def by_expert(route_ids, vals, n_dev):
    return jnp.sum(jnp.where(route_ids[:, :, None] == jnp.arange(n_dev)[None, None, :], vals[:, :, None], 0.0), axis=1)


def slot_ranks(route_ids, n_dev):
    tok = route_ids.shape[0]
    member = jnp.any(route_ids[:, :, None] == jnp.arange(n_dev)[None, None, :], axis=1)
    before = (jnp.arange(tok)[:, None] > jnp.arange(tok)[None, :]).astype(BF16)
    rank = jnp.dot(before, member.astype(BF16), preferred_element_type=F32)
    return jnp.where(member, rank, -1.0)


def mix_matrix(ranks, wts):
    tok, n_exp = ranks.shape
    pieces, rest = [], wts
    for _ in range(3):
        top = lax.reduce_precision(rest, 8, 7)
        pieces.append(top)
        rest = rest - top
    hit = ranks[:, :, None] == jnp.arange(SLOT_CAP, dtype=F32)[None, None, :]
    return jnp.concatenate([jnp.where(hit, p[:, :, None], 0.0).astype(BF16).reshape(tok, n_exp * SLOT_CAP) for p in pieces], axis=0)


def solution(mesh):
    n_dev = mesh.shape['tp'] * mesh.shape['ep']
    n_ep = mesh.shape['ep']
    rows_spec = P(FLAT_AXES, None)
    cube_spec = P(FLAT_AXES, None, None)
    whole_spec = P(None, None, None)
    col_split = P(None, 'tp')
    row_split = P('tp', None)
    in_specs = (rows_spec, cube_spec, cube_spec, P(FLAT_AXES), rows_spec, rows_spec,
                whole_spec, whole_spec, whole_spec, whole_spec, whole_spec, whole_spec, whole_spec, whole_spec,
                col_split, col_split, row_split, col_split, col_split, row_split,
                cube_spec, cube_spec, cube_spec)

    def body(hidden_in, cache0, cache1, kv_lens, route_ids, route_wts, att0_q, att0_uk, att0_uv, att0_o, att1_q, att1_uk, att1_uv, att1_o, ffn0_gate, ffn0_up, ffn0_down, ffn1_gate, ffn1_up, ffn1_down, exp_gate, exp_up, exp_down):
        ranks = slot_ranks(route_ids, n_dev)
        wts = by_expert(route_ids, route_wts, n_dev)
        zero_wt = jnp.sum(jnp.where(route_ids >= n_dev, route_wts, 0.0), axis=1)
        table = jnp.pad(ranks, ((0, 0), (0, 128 - n_dev))).astype(BF16)
        mine = jnp.concatenate([ranks, wts], axis=1)
        theirs = lax.ppermute(mine, 'tp', [(0, 1), (1, 0)])
        low_plane = lax.axis_index('tp') == 0

        def plane_matrix(pair):
            ranks_at = jnp.where(low_plane, pair[:, :n_ep], pair[:, n_ep:n_dev])
            wts_at = jnp.where(low_plane, pair[:, n_dev:n_dev + n_ep], pair[:, n_dev + n_ep:])
            return mix_matrix(ranks_at, wts_at)

        mat_near, mat_far = plane_matrix(mine), plane_matrix(theirs)
        cos, sin = rope_tables(kv_lens, att0_q.shape[2] - att0_uk.shape[1])
        h_zero, u_ext = att_call(hidden_in, cache0, kv_lens, cos, sin, att0_q, att0_uk, att0_uv, att0_o, table)
        f_zero, near, far = dense_call(u_ext, h_zero, ffn0_gate.T, ffn0_up.T, ffn0_down, expert=(exp_gate, exp_up, exp_down))
        h_one, u_one, back_far = att_call(f_zero, cache1, kv_lens, cos, sin, att1_q, att1_uk, att1_uv, att1_o, far=far)
        out, = dense_call(u_one, h_one, ffn1_gate.T, ffn1_up.T, ffn1_down,
                          mix=(near, back_far, mat_near, mat_far, u_ext, zero_wt[:, None]))
        return out

    return jax.shard_map(body, mesh=mesh, in_specs=in_specs, out_specs=rows_spec, check_vma=False)
```

```python
import functools

import jax
import jax.numpy as jnp
from jax import lax
from jax.experimental import pallas as pl
from jax.experimental.pallas import tpu as pltpu
from jax.sharding import PartitionSpec as P

FLAT_AXES = ('tp', 'ep')
MESH = pl.DeviceIdType.MESH
F32, BF16 = jnp.float32, jnp.bfloat16
SLOT_CAP = 72
VMEM_LIMIT = 66_000_000


def dot_t(lhs, rhs):
    return lax.dot_general(lhs, rhs, (((1,), (1,)), ((), ())), preferred_element_type=F32)


def dot_n(lhs, rhs):
    return jnp.dot(lhs, rhs, preferred_element_type=F32)


TILE = 512
COLS = 256


def exchange_copies(src, dst, send_sem, recv_sem, z, e, diagonal):
    y, x, c = e // 4, (e // 2) % 2, e % 2
    copies = []
    for k in range(1, 8):
        if (k >= 6) not in diagonal:
            continue
        peer = lax.rem(y + k // 4, 2) * 4 + lax.rem(x + (k // 2) % 2, 2) * 2 + lax.rem(c + k % 2, 2)
        copies.append(pltpu.make_async_remote_copy(
            src_ref=src.at[pl.ds(pl.multiple_of(peer * SLOT_CAP, 8), SLOT_CAP)],
            dst_ref=dst.at[e] if len(dst.shape) == 3 else dst.at[pl.ds(pl.multiple_of(e * SLOT_CAP, 8), SLOT_CAP)],
            send_sem=send_sem.at[k], recv_sem=recv_sem.at[k], device_id=(z, peer), device_id_type=MESH))
    return copies


def ffn_kernel(with_expert, *refs):
    refs = list(refs)
    u_ref, h_ref, gate_hbm, up_hbm, down_hbm = refs[:5]
    del refs[:5]
    if with_expert:
        eg_hbm, eu_hbm, ed_hbm = refs[:3]
        del refs[:3]
    else:
        near_hbm, far_hbm, back_hbm, u0_ref, their_ref = refs[:5]
        del refs[:5]
    out_ref = refs.pop(0)
    if with_expert:
        near_hbm, far_hbm, their_ref = refs[:3]
        del refs[:3]
    blocks, rows_ref, act_ref, gate_w, up_w, down_w, part_buf, z_out, z_in, d_out, d_in, p_out, p_in = refs[:13]
    w_sem, ex_send, ex_recv, z_send, z_recv, d_send, d_recv, p_send, p_recv, own_sem = refs[13:23]
    if with_expert:
        x_buf, h_buf, e_buf, ew_sem, eo_sem = refs[23:]
    else:
        near_in, far_in, mat_near, mat_far, n_send, n_recv, f_send, f_recv, far_sem = refs[23:]

    tok, hid = h_ref.shape
    ff = gate_w.shape[0]
    n_full, tail = ff // TILE, ff % TILE
    n_col = hid // COLS
    k_main = (ff // 256) * 256

    z = lax.axis_index('tp')
    e = lax.axis_index('ep')
    y, x, c = e // 4, (e // 2) % 2, e % 2
    zn = (1 - z, e)
    cn = (z, e + 1 - 2 * c)
    base = pl.multiple_of(c * ff, 16)

    def tile_copies(step, rows):
        at = pl.multiple_of(step * TILE, TILE)
        return [pltpu.make_async_copy(hbm.at[pl.ds(pl.multiple_of(base + at, 16), rows)], buf.at[pl.ds(at, rows)], w_sem.at[k, step])
                for k, (hbm, buf) in enumerate(((gate_hbm, gate_w), (up_hbm, up_w)))]

    down_cp = pltpu.make_async_copy(down_hbm.at[pl.ds(base, ff)], down_w, w_sem.at[2, 0])
    for step in range(n_full):
        for cp in tile_copies(step, TILE):
            cp.start()
    for cp in tile_copies(n_full, tail):
        cp.start()

    if with_expert:
        me = z * 8 + e
        xn = (z, e + 2 - 4 * x)
        yn = (z, e + 4 - 8 * y)
        peers = (zn, cn, xn, yn)
    else:
        n_ep = near_in.shape[0]
        peers = (zn,) + tuple((z, lax.rem(e + k, n_ep)) for k in range(1, n_ep))
    barrier = pltpu.get_barrier_semaphore()
    for peer in peers:
        pl.semaphore_signal(barrier, inc=1, device_id=peer, device_id_type=MESH)
    pl.semaphore_wait(barrier, len(peers))

    def remote(k, src, dst, peer):
        return pltpu.make_async_remote_copy(src_ref=src, dst_ref=dst, send_sem=ex_send.at[k], recv_sem=ex_recv.at[k],
                                            device_id=peer, device_id_type=MESH)

    if with_expert:
        half = tok // 2
        lo, hi = pl.ds(0, half), pl.ds(half, half)

        def plane(z_at):
            first = z_at * 8
            return (first + e, first + e + 2 - 4 * x, first + e + 4 - 8 * y,
                    first + (1 - y) * 4 + (1 - x) * 2 + c)

        def plane_sends(first, blks, own_src):
            own, xb, yb, db = blks
            return {
                'x': remote(first, own_src, blocks.at[own], xn),
                'y': remote(first + 1, own_src, blocks.at[own], yn),
                'xr': remote(first + 2, blocks.at[yb, hi], blocks.at[yb, hi], xn),
                'yr': remote(first + 3, blocks.at[xb, lo], blocks.at[xb, lo], yn),
                'c0': remote(first + 4, own_src, blocks.at[own], cn),
                'c1': remote(first + 5, blocks.at[xb], blocks.at[xb], cn),
                'c2': remote(first + 6, blocks.at[yb], blocks.at[yb], cn),
                'c3': remote(first + 7, blocks.at[db], blocks.at[db], cn),
            }

        def start_relay(s):
            s['x'].wait_recv()
            s['y'].wait_recv()
            s['xr'].start()
            s['yr'].start()
            s['c1'].start()
            s['c2'].start()

        def start_last(s):
            s['xr'].wait_recv()
            s['yr'].wait_recv()
            s['c3'].start()

        z_blk = (1 - z) * 8 + e
        c_blk = z * 8 + e + 1 - 2 * c
        zc_blk = (1 - z) * 8 + e + 1 - 2 * c
        sa = plane_sends(1, plane(z), u_ref)
        sb = plane_sends(9, plane(1 - z), blocks.at[z_blk])
        z_copy = remote(0, u_ref, blocks.at[me], zn)
        ca_copy, cb_copy = sa['c0'], sb['c0']
        own_cp = pltpu.make_async_copy(u_ref, blocks.at[me], own_sem.at[0])
        own_cp.start()
    else:
        z_blk, c_blk, zc_blk = 0, 1, 2
        z_copy = remote(0, u_ref, blocks.at[0], zn)
        ca_copy = remote(1, u_ref, blocks.at[1], cn)
        cb_copy = remote(2, blocks.at[0], blocks.at[2], cn)
        near_copies = exchange_copies(near_hbm, near_in, n_send, n_recv, z, e, (False, True))
        far_copies = exchange_copies(far_hbm, far_in, f_send, f_recv, z, e, (True,))
        own_cp = pltpu.make_async_copy(near_hbm.at[pl.ds(pl.multiple_of(e * SLOT_CAP, 8), SLOT_CAP)], near_in.at[e], own_sem.at[0])
        far_local = []
        for k in range(6):
            at = lax.rem(y + k // 4, 2) * 4 + lax.rem(x + (k // 2) % 2, 2) * 2 + lax.rem(c + k % 2, 2)
            far_local.append(pltpu.make_async_copy(back_hbm.at[pl.ds(pl.multiple_of(at * SLOT_CAP, 8), SLOT_CAP)], far_in.at[at], far_sem.at[k]))

    lane = lax.broadcasted_iota(jnp.int32, (tok, 128), 1)

    def fill_mix(mat, table_vals):
        vals = table_vals.astype(F32)
        slot = lax.broadcasted_iota(jnp.int32, (tok, SLOT_CAP), 1).astype(F32)
        for k in range(n_ep):
            def column(part):
                return jnp.sum(jnp.where(lane == part * 16 + z * n_ep + k, vals, 0.0), axis=1, keepdims=True)
            hit = slot == column(0)
            for part in range(3):
                mat[k, pl.ds(part * tok, tok)] = jnp.where(hit, column(part + 1), 0.0).astype(BF16)

    z_copy.start()
    ca_copy.start()
    if with_expert:
        sa['x'].start()
        sa['y'].start()
    else:
        for cp in far_copies + near_copies:
            cp.start()
    rows_ref[pl.ds(0, tok)] = u_ref[:, pl.ds(0, hid)]
    ca_copy.wait_recv()
    rows_ref[pl.ds(tok, tok)] = blocks[c_blk, :, pl.ds(0, hid)]

    def swiglu_tile(first, at, rows):
        lhs = rows_ref[pl.ds(first, 2 * tok)]
        gate_val = dot_t(lhs, gate_w[pl.ds(at, rows)])
        up_val = dot_t(lhs, up_w[pl.ds(at, rows)])
        act_ref[pl.ds(first, 2 * tok), pl.ds(at, rows)] = (jax.nn.silu(gate_val) * up_val).astype(BF16)

    @pl.loop(0, n_full)
    def _(step):
        for cp in tile_copies(step, TILE):
            cp.wait()
        swiglu_tile(0, pl.multiple_of(step * TILE, TILE), TILE)

        @pl.when(step == 2)
        def _():
            down_cp.start()

    for cp in tile_copies(n_full, tail):
        cp.wait()
    swiglu_tile(0, n_full * TILE, tail)

    z_copy.wait_recv()
    cb_copy.start()
    if with_expert:
        start_relay(sa)
        sb['x'].start()
        sb['y'].start()
    else:
        own_cp.start()
        for cp in far_local:
            cp.start()
        fill_mix(mat_near, u0_ref[:, pl.ds(hid, 128)])
        fill_mix(mat_far, their_ref[...])
    rows_ref[pl.ds(2 * tok, tok)] = blocks[z_blk, :, pl.ds(0, hid)]
    cb_copy.wait_recv()
    rows_ref[pl.ds(3 * tok, tok)] = blocks[zc_blk, :, pl.ds(0, hid)]

    @pl.loop(0, n_full)
    def _(step):
        swiglu_tile(2 * tok, pl.multiple_of(step * TILE, TILE), TILE)

    swiglu_tile(2 * tok, n_full * TILE, tail)

    if with_expert:
        eg, eu, ed = (gate_w.at[pl.ds(0, hid), pl.ds(0, eg_hbm.shape[2])], up_w.at[pl.ds(0, hid), pl.ds(0, eg_hbm.shape[2])],
                      down_w.at[pl.ds(0, ed_hbm.shape[1])])
        eg_cp, eu_cp, ed_cp = (pltpu.make_async_copy(s.at[0], d, ew_sem.at[k])
                               for k, (s, d) in enumerate(((eg_hbm, eg), (eu_hbm, eu), (ed_hbm, ed))))
        eg_cp.start()
        eu_cp.start()
        start_last(sa)

    def link(src, dst, sems, rems, col, peer):
        return pltpu.make_async_remote_copy(src_ref=src.at[col], dst_ref=dst.at[col], send_sem=sems.at[col],
                                            recv_sem=rems.at[col], device_id=peer, device_id_type=MESH)

    def z_link(col):
        return link(z_out, z_in, z_send, z_recv, col, zn)

    def d_link(col):
        return link(d_out, d_in, d_send, d_recv, col, cn)

    def p_link(col):
        return link(p_out, p_in, p_send, p_recv, col, cn)

    def down_tile(first, col):
        cols = pl.ds(pl.multiple_of(col * COLS, COLS), COLS)
        lhs = act_ref.at[pl.ds(first, 2 * tok)]
        val = dot_n(lhs[:, pl.ds(0, k_main)], down_w[pl.ds(0, k_main), cols])
        return val + dot_n(lhs[:, pl.ds(k_main, ff - k_main)], down_w[pl.ds(k_main, ff - k_main), cols])

    def mixed(mat, back, cols):
        val = dot_n(mat[0], back[0, :, cols])
        for k in range(1, n_ep):
            val += dot_n(mat[k], back[k, :, cols])
        return (val[2 * tok:] + val[tok:2 * tok]) + val[:tok]

    def send_z(col):
        d_link(col).wait_recv()
        total = z_out[col] + d_in[col]
        if not with_expert:
            total += mixed(mat_far, far_in, pl.ds(pl.multiple_of(col * COLS, COLS), COLS))
        z_out[col] = total
        z_link(col).start()

    down_cp.wait()
    if not with_expert:
        for cp in far_local:
            cp.wait()
        for cp in far_copies:
            cp.wait_recv()

    @pl.loop(0, n_col)
    def _(col):
        val = down_tile(2 * tok, col)
        z_out[col] = val[:tok]
        d_out[col] = val[tok:]
        d_link(col).start()

        @pl.when(col >= 2)
        def _():
            send_z(col - 2)

    send_z(n_col - 2)
    send_z(n_col - 1)

    @pl.loop(0, n_col)
    def _(col):
        val = down_tile(0, col)
        part_buf[col] = val[:tok]
        p_out[col] = val[tok:]
        p_link(col).start()

    if with_expert:
        ed_cp.start()
        own_cp.wait()
        eg_cp.wait()
        eu_cp.wait()
        their_ref[...] = blocks[z_blk, :, pl.ds(hid, 128)]
        slot_id = lax.broadcasted_iota(jnp.int32, (tok, 2 * SLOT_CAP), 1).astype(F32)
        q_rows = 4 * SLOT_CAP

        def eo_copy(it, buf, dst, yq):
            return pltpu.make_async_copy(e_buf.at[buf], dst.at[pl.ds(pl.multiple_of(yq * q_rows, q_rows), q_rows)], eo_sem.at[buf])

        @pl.loop(0, 4)
        def _(it):
            @pl.when(it == 0)
            def _():
                sa['c1'].wait_recv()

            @pl.when(it == 1)
            def _():
                start_relay(sb)
                sa['c2'].wait_recv()
                sa['c3'].wait_recv()

            @pl.when(it == 2)
            def _():
                start_last(sb)
                sb['c1'].wait_recv()

            @pl.when(it == 3)
            def _():
                sb['c2'].wait_recv()
                sb['c3'].wait_recv()

            zq = lax.rem(z + it // 2, 2)
            yq = lax.rem(y + it, 2)
            buf = lax.rem(it, 2)
            for pair in range(2):
                acc = None
                for k in range(2):
                    blk = zq * 8 + yq * 4 + pair * 2 + k
                    table = blocks[blk, :, pl.ds(hid, 128)].astype(F32)
                    rank = jnp.sum(jnp.where(lane == me, table, 0.0), axis=1, keepdims=True)
                    want = jnp.where(rank >= 0.0, rank + k * SLOT_CAP, -1.0)
                    hot = jnp.where(slot_id == want, 1.0, 0.0).astype(BF16)
                    got = lax.dot_general(hot, blocks[blk, :, pl.ds(0, hid)], (((0,), (0,)), ((), ())),
                                          preferred_element_type=F32)
                    acc = got if acc is None else acc + got
                x_buf[pl.ds(pair * 2 * SLOT_CAP, 2 * SLOT_CAP)] = acc.astype(BF16)
            for off, width in ((0, 512), (512, 512), (1024, 384)):
                gate_val = dot_n(x_buf[...], eg[:, pl.ds(off, width)])
                up_val = dot_n(x_buf[...], eu[:, pl.ds(off, width)])
                h_buf[:, pl.ds(off, width)] = (jax.nn.silu(gate_val) * up_val).astype(BF16)

            @pl.when(it == 0)
            def _():
                ed_cp.wait()

            @pl.when(it >= 2)
            def _():
                eo_copy(it, buf, near_hbm, yq).wait()

            for off in range(0, hid, 512):
                e_buf[buf, :, pl.ds(off, 512)] = dot_n(h_buf[...], ed[:, pl.ds(off, 512)]).astype(BF16)

            @pl.when(it < 2)
            def _():
                eo_copy(it, buf, near_hbm, yq).start()

            @pl.when(it >= 2)
            def _():
                eo_copy(it, buf, far_hbm, yq).start()

        eo_copy(0, 0, far_hbm, 0).wait()
        eo_copy(0, 1, far_hbm, 0).wait()

    if not with_expert:
        own_cp.wait()
        for cp in near_copies:
            cp.wait_recv()
        zero_wt = jnp.sum(jnp.where((lane >= 64) & (lane < 67), u0_ref[:, pl.ds(hid, 128)].astype(F32), 0.0), axis=1, keepdims=True)

    @pl.loop(0, n_col)
    def _(col):
        p_link(col).wait()
        d_link(col).wait_send()
        z_link(col).wait()
        cols = pl.ds(pl.multiple_of(col * COLS, COLS), COLS)
        total = h_ref[:, cols].astype(F32) + ((part_buf[col] + p_in[col]) + z_in[col])
        if not with_expert:
            total += mixed(mat_near, near_in, cols) + zero_wt * u0_ref[:, cols].astype(F32)
        out_ref[:, cols] = total.astype(out_ref.dtype)

    z_copy.wait_send()
    if with_expert:
        for s in (sa, sb):
            for cp in s.values():
                cp.wait_send()
    else:
        ca_copy.wait_send()
        cb_copy.wait_send()
        for cp in far_copies + near_copies:
            cp.wait_send()


def dense_call(u, h, w_gate_t, w_up_t, w_down, expert=None, mix=None):
    tok, hid = h.shape
    ff = w_gate_t.shape[0] // 2
    width = u.shape[1]
    with_expert = expert is not None
    vmem, hbm = pl.BlockSpec(memory_space=pltpu.VMEM), pl.BlockSpec(memory_space=pl.ANY)
    n_col = hid // COLS
    n_step = ff // TILE + 1
    args = [u, h, w_gate_t, w_up_t, w_down]
    in_specs = [vmem, vmem, hbm, hbm, hbm]
    out_shape = [jax.ShapeDtypeStruct((tok, hid), BF16)]
    out_specs = [vmem]
    n_ex = 17 if with_expert else 3
    dma = pltpu.SemaphoreType.DMA
    scratch = [pltpu.VMEM((16 if with_expert else 3, tok, width), BF16), pltpu.VMEM((4 * tok, hid), BF16),
               pltpu.VMEM((4 * tok, n_step * TILE), BF16),
               pltpu.VMEM((ff, hid), BF16), pltpu.VMEM((ff, hid), BF16), pltpu.VMEM((ff, hid), BF16)]
    scratch += [pltpu.VMEM((n_col, tok, COLS), F32)] * 7
    scratch += [dma((3, n_step)), dma((n_ex,)), dma((n_ex,))] + [dma((n_col,))] * 6 + [dma((1,))]
    flops = 2 * 2 * tok * hid * ff * 6
    if with_expert:
        inner = expert[0].shape[2]
        args += list(expert)
        in_specs += [hbm, hbm, hbm]
        out_shape += [jax.ShapeDtypeStruct((8 * SLOT_CAP, hid), BF16)] * 2 + [jax.ShapeDtypeStruct((tok, 128), BF16)]
        out_specs += [hbm, hbm, vmem]
        scratch += [pltpu.VMEM((4 * SLOT_CAP, hid), BF16), pltpu.VMEM((4 * SLOT_CAP, inner), BF16),
                    pltpu.VMEM((2, 4 * SLOT_CAP, hid), BF16), dma((3,)), dma((2,))]
        flops += 2 * 16 * SLOT_CAP * hid * inner * 3
    else:
        args += list(mix)
        in_specs += [hbm, hbm, hbm, vmem, vmem]
        n_ep = mix[0].shape[0] // SLOT_CAP
        scratch += [pltpu.VMEM((n_ep, SLOT_CAP, hid), BF16)] * 2 + [pltpu.VMEM((n_ep, 3 * tok, SLOT_CAP), BF16)] * 2
        scratch += [dma((n_ep,))] * 4 + [dma((6,))]
    return pl.pallas_call(
        functools.partial(ffn_kernel, with_expert),
        out_shape=out_shape, in_specs=in_specs, out_specs=out_specs, scratch_shapes=scratch,
        compiler_params=pltpu.CompilerParams(collective_id=0 if with_expert else 1, has_side_effects=True,
                                             vmem_limit_bytes=VMEM_LIMIT),
        cost_estimate=pl.CostEstimate(flops=flops, bytes_accessed=6 * hid * ff, transcendentals=0),
        name='dense_expert' if with_expert else 'dense',
    )(*args)


GROUP = 16
RING = 4
SUB = 16


def route_table(ids, wts):
    tok, top_k = ids.shape
    lane = lax.broadcasted_iota(jnp.int32, (tok, 128), 1)
    weight = jnp.zeros((tok, 128), F32)
    member = jnp.zeros((tok, 128), F32)
    for j in range(top_k):
        col = ids[:, j:j + 1]
        hit = ((lane < 64) & (col == lax.rem(lane, 16))) | ((lane >= 64) & (col >= 16))
        weight += jnp.where(hit, wts[:, j:j + 1], 0.0)
        member += jnp.where(hit, 1.0, 0.0)
    before = lax.broadcasted_iota(jnp.int32, (tok, tok), 0) > lax.broadcasted_iota(jnp.int32, (tok, tok), 1)
    rank = dot_n(jnp.where(before, 1.0, 0.0).astype(BF16), member.astype(BF16))
    rank = jnp.where(member > 0.0, rank, -1.0)
    first = weight.astype(BF16).astype(F32)
    second = (weight - first).astype(BF16).astype(F32)
    third = (weight - first) - second
    part = jnp.where(lane < 64, lane // 16 - 1, lane - 64)
    term = jnp.where(part == 0, first, jnp.where(part == 1, second, third))
    return jnp.where(lane < 16, rank, jnp.where(lane < 67, term, 0.0)).astype(BF16)


def att_kernel(with_table, with_far, *refs):
    refs = list(refs)
    lens_ref, x_ref, cos_ref, sin_ref = refs[:4]
    del refs[:4]
    if with_table:
        ids_ref, wts_ref = refs[:2]
        del refs[:2]
    far_hbm = refs.pop(0) if with_far else None
    wq_hbm, uk_hbm, uv_hbm, wo_hbm, cache_hbm, h_ref, u_ref = refs[:7]
    del refs[:7]
    back_hbm = refs.pop(0) if with_far else None
    wq, uk, uv, wo, ring, xn_buf, q_buf, o_buf, ov_buf, p_buf, w_sem, ring_sem = refs[:12]
    if with_far:
        own_buf, own_sem, f_send, f_recv = refs[12:]
    tok, hid = x_ref.shape
    heads, nope, latent = uk.shape
    qk_dim = wq.shape[1]
    rope = qk_dim - nope
    scale = qk_dim ** -0.5
    n_group = tok // GROUP
    span = latent + rope

    def head_copy(quad):
        return pltpu.make_async_copy(wq_hbm.at[pl.ds(quad * 4, 4)], wq.at[pl.ds(quad * 4, 4)], w_sem.at[quad])

    def ring_copy(group, slot):
        return pltpu.make_async_copy(cache_hbm.at[pl.ds(group * GROUP, GROUP)], ring.at[slot], ring_sem.at[slot])

    uk_cp = pltpu.make_async_copy(uk_hbm, uk, w_sem.at[4])
    uv_cp = pltpu.make_async_copy(uv_hbm, uv, w_sem.at[5])
    wo_cp = pltpu.make_async_copy(wo_hbm, wo, w_sem.at[6])
    head_copy(0).start()
    uk_cp.start()
    for quad in range(1, heads // 4):
        head_copy(quad).start()

    if with_far:
        z = lax.axis_index('tp')
        e = lax.axis_index('ep')
        n_ep = far_hbm.shape[0] // SLOT_CAP
        barrier = pltpu.get_barrier_semaphore()
        for k in range(1, n_ep):
            pl.semaphore_signal(barrier, inc=1, device_id=(z, lax.rem(e + k, n_ep)), device_id_type=MESH)
        pl.semaphore_wait(barrier, n_ep - 1)
        far_copies = exchange_copies(far_hbm, back_hbm, f_send, f_recv, z, e, (False,))
        for cp in far_copies:
            cp.start()
        own_rows = pl.ds(pl.multiple_of(e * SLOT_CAP, 8), SLOT_CAP)
        own_in = pltpu.make_async_copy(far_hbm.at[own_rows], own_buf, own_sem.at[0])
        own_out = pltpu.make_async_copy(own_buf, back_hbm.at[own_rows], own_sem.at[1])
        own_in.start()

    def norm(val):
        return (val * lax.rsqrt(jnp.mean(val * val, axis=-1, keepdims=True) + 1e-6)).astype(BF16)

    xn_buf[...] = norm(x_ref[...].astype(F32))
    uk_cp.wait()
    lane = lax.broadcasted_iota(jnp.int32, (tok, 128), 1)
    first_half = lax.rem(lane, rope) < rope // 2

    @pl.loop(0, heads // 4)
    def _(quad):
        head_copy(quad).wait()

        @pl.when(quad == 0)
        def _():
            for group in range(RING):
                ring_copy(group, group).start()

        @pl.when(quad == 3)
        def _():
            uv_cp.start()
            wo_cp.start()

        w_nope = jnp.concatenate([wq[quad * 4 + k, pl.ds(0, nope)] for k in range(4)], axis=0)
        w_rope = jnp.concatenate([wq[quad * 4 + k, pl.ds(nope, rope)] for k in range(4)], axis=0)
        q_nope = dot_t(xn_buf[...], w_nope).astype(BF16)
        q_rope = dot_t(xn_buf[...], w_rope).astype(BF16).astype(F32)
        for k in range(4):
            q_lat = dot_n(q_nope[:, k * nope:(k + 1) * nope], uk[quad * 4 + k]).astype(BF16).astype(F32)
            for j in range(latent // 128):
                q_buf[j, pl.ds(quad * 4 + k, tok, stride=heads)] = q_lat[:, j * 128:(j + 1) * 128]
        for k in range(2):
            val = q_rope[:, k * 128:(k + 1) * 128]
            swap = jnp.where(first_half, pltpu.roll(val, 128 - rope // 2, 1), pltpu.roll(val, rope // 2, 1))
            rot = (val * cos_ref[...] + swap * sin_ref[...]).astype(BF16).astype(F32)
            q_buf[latent // 128, pl.ds(quad * 4 + 2 * k, tok, stride=heads)] = rot
            q_buf[latent // 128, pl.ds(quad * 4 + 2 * k + 1, tok, stride=heads)] = pltpu.roll(rot, rope, 1)

    place = lax.broadcasted_iota(jnp.int32, (heads, cache_hbm.shape[2]), 1)

    @pl.loop(0, n_group)
    def _(group):
        slot = lax.rem(group, RING)
        ring_copy(group, slot).wait()
        @pl.loop(0, GROUP // SUB)
        def _(sub):
            for k in range(SUB):
                at = sub * SUB + k
                t = group * GROUP + at
                rows = pl.ds(pl.multiple_of(t * heads, heads), heads)
                q_cat = jnp.concatenate([q_buf[j, rows] for j in range(latent // 128 + 1)], axis=1)[:, :span].astype(BF16)
                score = dot_n(q_cat, ring[slot, at]) * scale
                score = jnp.where(place < lens_ref[t], score, -1e30)
                top = jnp.max(score, axis=1, keepdims=True)
                num = jnp.exp(score - top)
                p_buf[at] = (num * (1.0 / jnp.sum(num, axis=1, keepdims=True))).astype(BF16)

        @pl.loop(0, GROUP // SUB)
        def _(sub):
            for k in range(SUB):
                at = sub * SUB + k
                rows = pl.ds(pl.multiple_of((group * GROUP + at) * heads, heads), heads)
                o_lat = dot_t(p_buf[at], ring[slot, at, pl.ds(0, latent)])
                for j in range(latent // 128):
                    o_buf[j, rows] = o_lat[:, j * 128:(j + 1) * 128]

        @pl.when(group + RING < n_group)
        def _():
            ring_copy(group + RING, slot).start()


    uv_cp.wait()
    if with_far:
        own_in.wait()
        own_out.start()

    @pl.loop(0, heads, unroll=8)
    def _(h):
        o_lat = jnp.concatenate([o_buf[j, pl.ds(h, tok, stride=heads)] for j in range(latent // 128)], axis=1).astype(BF16)
        vals = dot_n(o_lat, uv[h]).astype(BF16)
        ov_buf[:, pl.ds(pl.multiple_of(h * nope, nope), nope)] = vals

    wo_cp.wait()
    for off in range(0, hid, 512):
        cols = pl.ds(off, 512)
        att = dot_n(ov_buf[...], wo[:, cols])
        h_ref[:, cols] = (x_ref[:, cols].astype(F32) + att).astype(BF16)
    u_ref[:, pl.ds(0, hid)] = norm(h_ref[...].astype(F32))
    if with_table:
        u_ref[:, pl.ds(hid, 128)] = route_table(ids_ref[...], wts_ref[...])
    if with_far:
        own_out.wait()
        for cp in far_copies:
            cp.wait()


def att_call(x, cache, kv_lens, cos, sin, w_q, w_uk, w_uv, w_o, route=None, far=None):
    tok, hid = x.shape
    heads, nope, latent = w_uk.shape
    val_dim = w_uv.shape[2]
    assert val_dim == nope
    qk_dim = w_q.shape[2]
    pos = cache.shape[1]
    span = cache.shape[2]
    with_table = route is not None
    vmem, hbm = pl.BlockSpec(memory_space=pltpu.VMEM), pl.BlockSpec(memory_space=pl.ANY)
    smem = pl.BlockSpec(memory_space=pltpu.SMEM)
    with_far = far is not None
    args = [kv_lens, x, cos, sin] + (list(route) if with_table else []) + ([far] if with_far else [])
    args += [w_q.transpose(1, 2, 0), w_uk, w_uv, w_o.reshape(heads * val_dim, hid), cache.transpose(0, 2, 1)]
    width = hid + (128 if with_table else 0)
    out_shape = [jax.ShapeDtypeStruct((tok, hid), BF16), jax.ShapeDtypeStruct((tok, width), BF16)]
    out_specs = [vmem, vmem]
    extra, params = [], {}
    if with_far:
        n_ep = far.shape[0] // SLOT_CAP
        out_shape.append(jax.ShapeDtypeStruct(far.shape, BF16))
        out_specs.append(hbm)
        dma = pltpu.SemaphoreType.DMA
        extra = [pltpu.VMEM((SLOT_CAP, hid), BF16), dma((2,)), dma((n_ep,)), dma((n_ep,))]
        params = {'collective_id': 2, 'has_side_effects': True}
    return pl.pallas_call(
        functools.partial(att_kernel, with_table, with_far),
        out_shape=out_shape,
        in_specs=[smem] + [vmem] * (5 if with_table else 3) + [hbm] * (6 if with_far else 5),
        out_specs=out_specs,
        scratch_shapes=[
            pltpu.VMEM((heads, qk_dim, hid), BF16),
            pltpu.VMEM((heads, nope, latent), BF16),
            pltpu.VMEM((heads, latent, val_dim), BF16),
            pltpu.VMEM((heads * val_dim, hid), BF16),
            pltpu.VMEM((RING, GROUP, span, pos), BF16),
            pltpu.VMEM((tok, hid), BF16),
            pltpu.VMEM((latent // 128 + 1, tok * heads, 128), F32),
            pltpu.VMEM((latent // 128, tok * heads, 128), F32),
            pltpu.VMEM((tok, heads * val_dim), BF16),
            pltpu.VMEM((GROUP, heads, pos), BF16),
            pltpu.SemaphoreType.DMA((7,)),
            pltpu.SemaphoreType.DMA((RING,)),
        ] + extra,
        compiler_params=pltpu.CompilerParams(vmem_limit_bytes=VMEM_LIMIT, **params),
        cost_estimate=pl.CostEstimate(flops=6 * tok * hid * 3072, bytes_accessed=54_000_000, transcendentals=0),
        name='latent_attention',
    )(*args)


def rope_tables(kv_lens, rope):
    lane = jnp.arange(128)
    inv_freq = 10000.0 ** (-2.0 * (lane % (rope // 2)).astype(F32) / rope)
    angle = kv_lens.astype(F32)[:, None] * inv_freq[None, :]
    return jnp.cos(angle), jnp.where(lane % rope < rope // 2, -1.0, 1.0) * jnp.sin(angle)


def solution(mesh):
    assert mesh.shape['tp'] == 2 and mesh.shape['ep'] == 8
    rows_spec = P(FLAT_AXES, None)
    cube_spec = P(FLAT_AXES, None, None)
    whole_spec = P(None, None, None)
    col_split = P(None, 'tp')
    row_split = P('tp', None)
    in_specs = (rows_spec, cube_spec, cube_spec, P(FLAT_AXES), rows_spec, rows_spec,
                whole_spec, whole_spec, whole_spec, whole_spec, whole_spec, whole_spec, whole_spec, whole_spec,
                col_split, col_split, row_split, col_split, col_split, row_split,
                cube_spec, cube_spec, cube_spec)

    def body(hidden_in, cache0, cache1, kv_lens, route_ids, route_wts, att0_q, att0_uk, att0_uv, att0_o, att1_q, att1_uk, att1_uv, att1_o, ffn0_gate, ffn0_up, ffn0_down, ffn1_gate, ffn1_up, ffn1_down, exp_gate, exp_up, exp_down):
        cos, sin = rope_tables(kv_lens, att0_q.shape[2] - att0_uk.shape[1])
        h_zero, u_ext = att_call(hidden_in, cache0, kv_lens, cos, sin, att0_q, att0_uk, att0_uv, att0_o, route=(route_ids, route_wts))
        f_zero, near, far, theirs = dense_call(u_ext, h_zero, ffn0_gate.T, ffn0_up.T, ffn0_down, expert=(exp_gate, exp_up, exp_down))
        h_one, u_one, back = att_call(f_zero, cache1, kv_lens, cos, sin, att1_q, att1_uk, att1_uv, att1_o, far=far)
        out, = dense_call(u_one, h_one, ffn1_gate.T, ffn1_up.T, ffn1_down, mix=(near, far, back, u_ext, theirs))
        return out

    return jax.shard_map(body, mesh=mesh, in_specs=in_specs, out_specs=rows_spec, check_vma=False)
```

```python
import functools

import jax
import jax.numpy as jnp
from jax import lax
from jax.experimental import pallas as pl
from jax.experimental.pallas import tpu as pltpu
from jax.sharding import PartitionSpec as P

FLAT_AXES = ('tp', 'ep')
MESH = pl.DeviceIdType.MESH
F32, BF16 = jnp.float32, jnp.bfloat16
SLOT_CAP = 72
VMEM_LIMIT = 66_000_000


def dot_t(lhs, rhs):
    return lax.dot_general(lhs, rhs, (((1,), (1,)), ((), ())), preferred_element_type=F32)


def dot_n(lhs, rhs):
    return jnp.dot(lhs, rhs, preferred_element_type=F32)


TILE = 512
COLS = 256


def exchange_copies(src, dst, send_sem, recv_sem, z, e, diagonal):
    y, x, c = e // 4, (e // 2) % 2, e % 2
    copies = []
    for k in range(1, 8):
        if (k >= 6) not in diagonal:
            continue
        peer = lax.rem(y + k // 4, 2) * 4 + lax.rem(x + (k // 2) % 2, 2) * 2 + lax.rem(c + k % 2, 2)
        copies.append(pltpu.make_async_remote_copy(
            src_ref=src.at[pl.ds(pl.multiple_of(peer * SLOT_CAP, 8), SLOT_CAP)],
            dst_ref=dst.at[e] if len(dst.shape) == 3 else dst.at[pl.ds(pl.multiple_of(e * SLOT_CAP, 8), SLOT_CAP)],
            send_sem=send_sem.at[k], recv_sem=recv_sem.at[k], device_id=(z, peer), device_id_type=MESH))
    return copies


def ffn_kernel(with_expert, *refs):
    refs = list(refs)
    u_ref, h_ref, gate_hbm, up_hbm, down_hbm = refs[:5]
    del refs[:5]
    if with_expert:
        eg_hbm, eu_hbm, ed_hbm = refs[:3]
        del refs[:3]
    else:
        near_hbm, far_hbm, back_hbm, u0_ref, their_ref = refs[:5]
        del refs[:5]
    out_ref = refs.pop(0)
    if with_expert:
        near_hbm, far_hbm, their_ref = refs[:3]
        del refs[:3]
    blocks, rows_ref, act_ref, gate_w, up_w, down_w, part_buf, z_out, z_in, d_out, d_in, p_out, p_in = refs[:13]
    w_sem, ex_send, ex_recv, z_send, z_recv, d_send, d_recv, p_send, p_recv, own_sem = refs[13:23]
    if with_expert:
        x_buf, h_buf, e_buf, ew_sem, eo_sem = refs[23:]
    else:
        near_in, far_in, mat_near, mat_far, n_send, n_recv, f_send, f_recv, far_sem = refs[23:]

    tok, hid = h_ref.shape
    ff = gate_w.shape[0]
    n_full, tail = ff // TILE, ff % TILE
    n_col = hid // COLS
    k_main = (ff // 256) * 256

    z = lax.axis_index('tp')
    e = lax.axis_index('ep')
    y, x, c = e // 4, (e // 2) % 2, e % 2
    zn = (1 - z, e)
    cn = (z, e + 1 - 2 * c)
    base = pl.multiple_of(c * ff, 16)

    def tile_copies(step, rows):
        at = pl.multiple_of(step * TILE, TILE)
        return [pltpu.make_async_copy(hbm.at[pl.ds(pl.multiple_of(base + at, 16), rows)], buf.at[pl.ds(at, rows)], w_sem.at[k, step])
                for k, (hbm, buf) in enumerate(((gate_hbm, gate_w), (up_hbm, up_w)))]

    down_cp = pltpu.make_async_copy(down_hbm.at[pl.ds(base, ff)], down_w, w_sem.at[2, 0])
    for step in range(n_full):
        for cp in tile_copies(step, TILE):
            cp.start()
    for cp in tile_copies(n_full, tail):
        cp.start()

    if with_expert:
        me = z * 8 + e
        xn = (z, e + 2 - 4 * x)
        yn = (z, e + 4 - 8 * y)
        peers = (zn, cn, xn, yn)
    else:
        n_ep = near_in.shape[0]
        peers = (zn,) + tuple((z, lax.rem(e + k, n_ep)) for k in range(1, n_ep))
    barrier = pltpu.get_barrier_semaphore()
    for peer in peers:
        pl.semaphore_signal(barrier, inc=1, device_id=peer, device_id_type=MESH)
    pl.semaphore_wait(barrier, len(peers))

    def remote(k, src, dst, peer):
        return pltpu.make_async_remote_copy(src_ref=src, dst_ref=dst, send_sem=ex_send.at[k], recv_sem=ex_recv.at[k],
                                            device_id=peer, device_id_type=MESH)

    if with_expert:
        half = tok // 2
        lo, hi = pl.ds(0, half), pl.ds(half, half)

        def plane(z_at):
            first = z_at * 8
            return (first + e, first + e + 2 - 4 * x, first + e + 4 - 8 * y,
                    first + (1 - y) * 4 + (1 - x) * 2 + c)

        def plane_sends(first, blks, own_src):
            own, xb, yb, db = blks
            return {
                'x': remote(first, own_src, blocks.at[own], xn),
                'y': remote(first + 1, own_src, blocks.at[own], yn),
                'xr': remote(first + 2, blocks.at[yb, hi], blocks.at[yb, hi], xn),
                'yr': remote(first + 3, blocks.at[xb, lo], blocks.at[xb, lo], yn),
                'c0': remote(first + 4, own_src, blocks.at[own], cn),
                'c1': remote(first + 5, blocks.at[xb], blocks.at[xb], cn),
                'c2': remote(first + 6, blocks.at[yb], blocks.at[yb], cn),
                'c3': remote(first + 7, blocks.at[db], blocks.at[db], cn),
            }

        def start_relay(s):
            s['x'].wait_recv()
            s['y'].wait_recv()
            s['xr'].start()
            s['yr'].start()
            s['c1'].start()
            s['c2'].start()

        def start_last(s):
            s['xr'].wait_recv()
            s['yr'].wait_recv()
            s['c3'].start()

        z_blk = (1 - z) * 8 + e
        c_blk = z * 8 + e + 1 - 2 * c
        zc_blk = (1 - z) * 8 + e + 1 - 2 * c
        sa = plane_sends(1, plane(z), u_ref)
        sb = plane_sends(9, plane(1 - z), blocks.at[z_blk])
        z_copy = remote(0, u_ref, blocks.at[me], zn)
        ca_copy, cb_copy = sa['c0'], sb['c0']
        own_cp = pltpu.make_async_copy(u_ref, blocks.at[me], own_sem.at[0])
        own_cp.start()
    else:
        z_blk, c_blk, zc_blk = 0, 1, 2
        z_copy = remote(0, u_ref, blocks.at[0], zn)
        ca_copy = remote(1, u_ref, blocks.at[1], cn)
        cb_copy = remote(2, blocks.at[0], blocks.at[2], cn)
        near_copies = exchange_copies(near_hbm, near_in, n_send, n_recv, z, e, (False, True))
        far_copies = exchange_copies(far_hbm, far_in, f_send, f_recv, z, e, (True,))
        own_cp = pltpu.make_async_copy(near_hbm.at[pl.ds(pl.multiple_of(e * SLOT_CAP, 8), SLOT_CAP)], near_in.at[e], own_sem.at[0])
        far_local = []
        for k in range(6):
            at = lax.rem(y + k // 4, 2) * 4 + lax.rem(x + (k // 2) % 2, 2) * 2 + lax.rem(c + k % 2, 2)
            far_local.append(pltpu.make_async_copy(back_hbm.at[pl.ds(pl.multiple_of(at * SLOT_CAP, 8), SLOT_CAP)], far_in.at[at], far_sem.at[k]))

    lane = lax.broadcasted_iota(jnp.int32, (tok, 128), 1)

    def fill_mix(mat, table_vals):
        vals = table_vals.astype(F32)
        slot = lax.broadcasted_iota(jnp.int32, (tok, SLOT_CAP), 1).astype(F32)
        for k in range(n_ep):
            def column(part):
                return jnp.sum(jnp.where(lane == part * 16 + z * n_ep + k, vals, 0.0), axis=1, keepdims=True)
            hit = slot == column(0)
            for part in range(3):
                mat[k, pl.ds(part * tok, tok)] = jnp.where(hit, column(part + 1), 0.0).astype(BF16)

    z_copy.start()
    ca_copy.start()
    if with_expert:
        sa['x'].start()
        sa['y'].start()
    else:
        for cp in far_copies + near_copies:
            cp.start()
    rows_ref[pl.ds(0, tok)] = u_ref[:, pl.ds(0, hid)]
    ca_copy.wait_recv()
    rows_ref[pl.ds(tok, tok)] = blocks[c_blk, :, pl.ds(0, hid)]

    def swiglu_tile(first, at, rows):
        lhs = rows_ref[pl.ds(first, 2 * tok)]
        gate_val = dot_t(lhs, gate_w[pl.ds(at, rows)])
        up_val = dot_t(lhs, up_w[pl.ds(at, rows)])
        act_ref[pl.ds(first, 2 * tok), pl.ds(at, rows)] = (jax.nn.silu(gate_val) * up_val).astype(BF16)

    @pl.loop(0, n_full)
    def _(step):
        for cp in tile_copies(step, TILE):
            cp.wait()
        swiglu_tile(0, pl.multiple_of(step * TILE, TILE), TILE)

        @pl.when(step == 2)
        def _():
            down_cp.start()

    for cp in tile_copies(n_full, tail):
        cp.wait()
    swiglu_tile(0, n_full * TILE, tail)

    if not with_expert:
        fill_mix(mat_far, their_ref[...])
    z_copy.wait_recv()
    cb_copy.start()
    if with_expert:
        start_relay(sa)
        sb['x'].start()
        sb['y'].start()
    else:
        own_cp.start()
        for cp in far_local:
            cp.start()
    rows_ref[pl.ds(2 * tok, tok)] = blocks[z_blk, :, pl.ds(0, hid)]
    cb_copy.wait_recv()
    rows_ref[pl.ds(3 * tok, tok)] = blocks[zc_blk, :, pl.ds(0, hid)]

    @pl.loop(0, n_full)
    def _(step):
        swiglu_tile(2 * tok, pl.multiple_of(step * TILE, TILE), TILE)

    swiglu_tile(2 * tok, n_full * TILE, tail)

    if with_expert:
        eg, eu, ed = (gate_w.at[pl.ds(0, hid), pl.ds(0, eg_hbm.shape[2])], up_w.at[pl.ds(0, hid), pl.ds(0, eg_hbm.shape[2])],
                      down_w.at[pl.ds(0, ed_hbm.shape[1])])
        eg_cp, eu_cp, ed_cp = (pltpu.make_async_copy(s.at[0], d, ew_sem.at[k])
                               for k, (s, d) in enumerate(((eg_hbm, eg), (eu_hbm, eu), (ed_hbm, ed))))
        eg_cp.start()
        eu_cp.start()
        start_last(sa)

    def link(src, dst, sems, rems, col, peer):
        return pltpu.make_async_remote_copy(src_ref=src.at[col], dst_ref=dst.at[col], send_sem=sems.at[col],
                                            recv_sem=rems.at[col], device_id=peer, device_id_type=MESH)

    def z_link(col):
        return link(z_out, z_in, z_send, z_recv, col, zn)

    def d_link(col):
        return link(d_out, d_in, d_send, d_recv, col, cn)

    def p_link(col):
        return link(p_out, p_in, p_send, p_recv, col, cn)

    def down_tile(first, col):
        cols = pl.ds(pl.multiple_of(col * COLS, COLS), COLS)
        lhs = act_ref.at[pl.ds(first, 2 * tok)]
        val = dot_n(lhs[:, pl.ds(0, k_main)], down_w[pl.ds(0, k_main), cols])
        return val + dot_n(lhs[:, pl.ds(k_main, ff - k_main)], down_w[pl.ds(k_main, ff - k_main), cols])

    def mixed(mat, back, cols):
        val = dot_n(mat[0], back[0, :, cols])
        for k in range(1, n_ep):
            val += dot_n(mat[k], back[k, :, cols])
        return (val[2 * tok:] + val[tok:2 * tok]) + val[:tok]

    def send_z(col):
        d_link(col).wait_recv()
        total = z_out[col] + d_in[col]
        if not with_expert:
            total += mixed(mat_far, far_in, pl.ds(pl.multiple_of(col * COLS, COLS), COLS))
        z_out[col] = total
        z_link(col).start()

    down_cp.wait()
    if not with_expert:
        for cp in far_local:
            cp.wait()
        for cp in far_copies:
            cp.wait_recv()

    @pl.loop(0, n_col)
    def _(col):
        val = down_tile(2 * tok, col)
        z_out[col] = val[:tok]
        d_out[col] = val[tok:]
        d_link(col).start()

        @pl.when(col >= 1)
        def _():
            send_z(col - 1)

    send_z(n_col - 1)
    if not with_expert:
        fill_mix(mat_near, u0_ref[:, pl.ds(hid, 128)])

    @pl.loop(0, n_col)
    def _(col):
        val = down_tile(0, col)
        part_buf[col] = val[:tok]
        p_out[col] = val[tok:]
        p_link(col).start()

    if with_expert:
        ed_cp.start()
        own_cp.wait()
        eg_cp.wait()
        eu_cp.wait()
        their_ref[...] = blocks[z_blk, :, pl.ds(hid, 128)]
        slot_id = lax.broadcasted_iota(jnp.int32, (tok, 2 * SLOT_CAP), 1).astype(F32)
        q_rows = 4 * SLOT_CAP

        def eo_copy(it, buf, dst, yq):
            return pltpu.make_async_copy(e_buf.at[buf], dst.at[pl.ds(pl.multiple_of(yq * q_rows, q_rows), q_rows)], eo_sem.at[buf])

        @pl.loop(0, 4)
        def _(it):
            @pl.when(it == 0)
            def _():
                sa['c1'].wait_recv()

            @pl.when(it == 1)
            def _():
                start_relay(sb)
                sa['c2'].wait_recv()
                sa['c3'].wait_recv()

            @pl.when(it == 2)
            def _():
                start_last(sb)
                sb['c1'].wait_recv()

            @pl.when(it == 3)
            def _():
                sb['c2'].wait_recv()
                sb['c3'].wait_recv()

            zq = lax.rem(z + it // 2, 2)
            yq = lax.rem(y + it, 2)
            buf = lax.rem(it, 2)
            for pair in range(2):
                acc = None
                for k in range(2):
                    blk = zq * 8 + yq * 4 + pair * 2 + k
                    table = blocks[blk, :, pl.ds(hid, 128)].astype(F32)
                    rank = jnp.sum(jnp.where(lane == me, table, 0.0), axis=1, keepdims=True)
                    want = jnp.where(rank >= 0.0, rank + k * SLOT_CAP, -1.0)
                    hot = jnp.where(slot_id == want, 1.0, 0.0).astype(BF16)
                    got = lax.dot_general(hot, blocks[blk, :, pl.ds(0, hid)], (((0,), (0,)), ((), ())),
                                          preferred_element_type=F32)
                    acc = got if acc is None else acc + got
                x_buf[pl.ds(pair * 2 * SLOT_CAP, 2 * SLOT_CAP)] = acc.astype(BF16)
            for off, width in ((0, 512), (512, 512), (1024, 256)):
                gate_val = dot_n(x_buf[...], eg[:, pl.ds(off, width)])
                up_val = dot_n(x_buf[...], eu[:, pl.ds(off, width)])
                h_buf[:, pl.ds(off, width)] = (jax.nn.silu(gate_val) * up_val).astype(BF16)
            both = dot_n(x_buf[...], jnp.concatenate([eg[:, pl.ds(1280, 128)], eu[:, pl.ds(1280, 128)]], axis=1))
            h_buf[:, pl.ds(1280, 128)] = (jax.nn.silu(both[:, :128]) * both[:, 128:]).astype(BF16)

            @pl.when(it == 0)
            def _():
                ed_cp.wait()

            @pl.when(it >= 2)
            def _():
                eo_copy(it, buf, near_hbm, yq).wait()

            for off in range(0, hid, 512):
                e_buf[buf, :, pl.ds(off, 512)] = dot_n(h_buf[...], ed[:, pl.ds(off, 512)]).astype(BF16)

            @pl.when(it < 2)
            def _():
                eo_copy(it, buf, near_hbm, yq).start()

            @pl.when(it >= 2)
            def _():
                eo_copy(it, buf, far_hbm, yq).start()

        eo_copy(0, 0, far_hbm, 0).wait()
        eo_copy(0, 1, far_hbm, 0).wait()

    if not with_expert:
        own_cp.wait()
        for cp in near_copies:
            cp.wait_recv()
        zero_wt = jnp.sum(jnp.where((lane >= 64) & (lane < 67), u0_ref[:, pl.ds(hid, 128)].astype(F32), 0.0), axis=1, keepdims=True)

    @pl.loop(0, n_col)
    def _(col):
        p_link(col).wait()
        d_link(col).wait_send()
        z_link(col).wait()
        cols = pl.ds(pl.multiple_of(col * COLS, COLS), COLS)
        total = h_ref[:, cols].astype(F32) + ((part_buf[col] + p_in[col]) + z_in[col])
        if not with_expert:
            total += mixed(mat_near, near_in, cols) + zero_wt * u0_ref[:, cols].astype(F32)
        out_ref[:, cols] = total.astype(out_ref.dtype)

    z_copy.wait_send()
    if with_expert:
        for s in (sa, sb):
            for cp in s.values():
                cp.wait_send()
    else:
        ca_copy.wait_send()
        cb_copy.wait_send()
        for cp in far_copies + near_copies:
            cp.wait_send()


def dense_call(u, h, w_gate_t, w_up_t, w_down, expert=None, mix=None):
    tok, hid = h.shape
    ff = w_gate_t.shape[0] // 2
    width = u.shape[1]
    with_expert = expert is not None
    vmem, hbm = pl.BlockSpec(memory_space=pltpu.VMEM), pl.BlockSpec(memory_space=pl.ANY)
    n_col = hid // COLS
    n_step = ff // TILE + 1
    args = [u, h, w_gate_t, w_up_t, w_down]
    in_specs = [vmem, vmem, hbm, hbm, hbm]
    out_shape = [jax.ShapeDtypeStruct((tok, hid), BF16 if with_expert else F32)]
    out_specs = [vmem]
    n_ex = 17 if with_expert else 3
    dma = pltpu.SemaphoreType.DMA
    scratch = [pltpu.VMEM((16 if with_expert else 3, tok, width), BF16), pltpu.VMEM((4 * tok, hid), BF16),
               pltpu.VMEM((4 * tok, n_step * TILE), BF16),
               pltpu.VMEM((ff, hid), BF16), pltpu.VMEM((ff, hid), BF16), pltpu.VMEM((ff, hid), BF16)]
    scratch += [pltpu.VMEM((n_col, tok, COLS), F32)] * 7
    scratch += [dma((3, n_step)), dma((n_ex,)), dma((n_ex,))] + [dma((n_col,))] * 6 + [dma((1,))]
    flops = 2 * 2 * tok * hid * ff * 6
    if with_expert:
        inner = expert[0].shape[2]
        args += list(expert)
        in_specs += [hbm, hbm, hbm]
        out_shape += [jax.ShapeDtypeStruct((8 * SLOT_CAP, hid), BF16)] * 2 + [jax.ShapeDtypeStruct((tok, 128), BF16)]
        out_specs += [hbm, hbm, vmem]
        scratch += [pltpu.VMEM((4 * SLOT_CAP, hid), BF16), pltpu.VMEM((4 * SLOT_CAP, inner), BF16),
                    pltpu.VMEM((2, 4 * SLOT_CAP, hid), BF16), dma((3,)), dma((2,))]
        flops += 2 * 16 * SLOT_CAP * hid * inner * 3
    else:
        args += list(mix)
        in_specs += [hbm, hbm, hbm, vmem, vmem]
        n_ep = mix[0].shape[0] // SLOT_CAP
        scratch += [pltpu.VMEM((n_ep, SLOT_CAP, hid), BF16)] * 2 + [pltpu.VMEM((n_ep, 3 * tok, SLOT_CAP), BF16)] * 2
        scratch += [dma((n_ep,))] * 4 + [dma((6,))]
    return pl.pallas_call(
        functools.partial(ffn_kernel, with_expert),
        out_shape=out_shape, in_specs=in_specs, out_specs=out_specs, scratch_shapes=scratch,
        compiler_params=pltpu.CompilerParams(collective_id=0 if with_expert else 1, has_side_effects=True,
                                             vmem_limit_bytes=VMEM_LIMIT),
        cost_estimate=pl.CostEstimate(flops=flops, bytes_accessed=6 * hid * ff, transcendentals=0),
        name='dense_expert' if with_expert else 'dense',
    )(*args)


GROUP = 16
RING = 4
SUB = 16


def route_table(route, top_k):
    tok = route.shape[0]
    lane = lax.broadcasted_iota(jnp.int32, (tok, 128), 1)
    lane16 = lax.rem(lane, 16).astype(F32)
    weight = jnp.zeros((tok, 128), F32)
    member = jnp.zeros((tok, 128), F32)
    for j in range(top_k):
        col = route[:, j:j + 1]
        hit = ((lane < 64) & (col == lane16)) | ((lane >= 64) & (col >= 16.0))
        weight += jnp.where(hit, route[:, 8 + j:9 + j], 0.0)
        member += jnp.where(hit, 1.0, 0.0)
    before = lax.broadcasted_iota(jnp.int32, (tok, tok), 0) > lax.broadcasted_iota(jnp.int32, (tok, tok), 1)
    rank = dot_n(jnp.where(before, 1.0, 0.0).astype(BF16), member.astype(BF16))
    rank = jnp.where(member > 0.0, rank, -1.0)
    first = weight.astype(BF16).astype(F32)
    second = (weight - first).astype(BF16).astype(F32)
    third = (weight - first) - second
    part = jnp.where(lane < 64, lane // 16 - 1, lane - 64)
    term = jnp.where(part == 0, first, jnp.where(part == 1, second, third))
    return jnp.where(lane < 16, rank, jnp.where(lane < 67, term, 0.0)).astype(BF16)


def att_kernel(top_k, with_far, *refs):
    refs = list(refs)
    with_table = top_k > 0
    lens_ref, x_ref, cos_ref, sin_ref = refs[:4]
    del refs[:4]
    if with_table:
        route_ref = refs.pop(0)
    far_hbm = refs.pop(0) if with_far else None
    wq_hbm, uk_hbm, uv_hbm, wo_hbm, cache_hbm, h_ref, u_ref = refs[:7]
    del refs[:7]
    back_hbm = refs.pop(0) if with_far else None
    wq, uk, uv, wo, ring, xn_buf, q_buf, o_buf, ov_buf, p_buf, w_sem, ring_sem = refs[:12]
    if with_far:
        own_buf, own_sem, f_send, f_recv = refs[12:]
    tok, hid = x_ref.shape
    heads, nope, latent = uk.shape
    qk_dim = wq.shape[1]
    rope = qk_dim - nope
    scale = qk_dim ** -0.5
    n_group = tok // GROUP
    span = latent + rope

    def head_copy(quad):
        return pltpu.make_async_copy(wq_hbm.at[pl.ds(quad * 4, 4)], wq.at[pl.ds(quad * 4, 4)], w_sem.at[quad])

    def ring_copy(group, slot):
        return pltpu.make_async_copy(cache_hbm.at[pl.ds(group * GROUP, GROUP)], ring.at[slot], ring_sem.at[slot])

    uk_cp = pltpu.make_async_copy(uk_hbm, uk, w_sem.at[4])
    uv_cp = pltpu.make_async_copy(uv_hbm, uv, w_sem.at[5])
    wo_cp = pltpu.make_async_copy(wo_hbm, wo, w_sem.at[6])
    head_copy(0).start()
    uk_cp.start()
    for quad in range(1, heads // 4):
        head_copy(quad).start()

    if with_far:
        z = lax.axis_index('tp')
        e = lax.axis_index('ep')
        n_ep = far_hbm.shape[0] // SLOT_CAP
        barrier = pltpu.get_barrier_semaphore()
        for k in range(1, n_ep):
            pl.semaphore_signal(barrier, inc=1, device_id=(z, lax.rem(e + k, n_ep)), device_id_type=MESH)
        pl.semaphore_wait(barrier, n_ep - 1)
        far_copies = exchange_copies(far_hbm, back_hbm, f_send, f_recv, z, e, (False,))
        for cp in far_copies:
            cp.start()
        own_rows = pl.ds(pl.multiple_of(e * SLOT_CAP, 8), SLOT_CAP)
        own_in = pltpu.make_async_copy(far_hbm.at[own_rows], own_buf, own_sem.at[0])
        own_out = pltpu.make_async_copy(own_buf, back_hbm.at[own_rows], own_sem.at[1])
        own_in.start()

    def norm(val):
        return (val * lax.rsqrt(jnp.mean(val * val, axis=-1, keepdims=True) + 1e-6)).astype(BF16)

    xn_buf[...] = norm(x_ref[...].astype(F32))
    uk_cp.wait()
    lane = lax.broadcasted_iota(jnp.int32, (tok, 128), 1)
    first_half = lax.rem(lane, rope) < rope // 2

    @pl.loop(0, heads // 4)
    def _(quad):
        head_copy(quad).wait()

        @pl.when(quad == 0)
        def _():
            for group in range(RING):
                ring_copy(group, group).start()

        @pl.when(quad == 3)
        def _():
            uv_cp.start()
            wo_cp.start()

        w_nope = jnp.concatenate([wq[quad * 4 + k, pl.ds(0, nope)] for k in range(4)], axis=0)
        w_rope = jnp.concatenate([wq[quad * 4 + k, pl.ds(nope, rope)] for k in range(4)], axis=0)
        q_nope = dot_t(xn_buf[...], w_nope).astype(BF16)
        q_rope = dot_t(xn_buf[...], w_rope).astype(BF16).astype(F32)
        for k in range(4):
            q_lat = dot_n(q_nope[:, k * nope:(k + 1) * nope], uk[quad * 4 + k]).astype(BF16).astype(F32)
            for j in range(latent // 128):
                q_buf[j, pl.ds(quad * 4 + k, tok, stride=heads)] = q_lat[:, j * 128:(j + 1) * 128]
        for k in range(2):
            val = q_rope[:, k * 128:(k + 1) * 128]
            swap = jnp.where(first_half, pltpu.roll(val, 128 - rope // 2, 1), pltpu.roll(val, rope // 2, 1))
            rot = (val * cos_ref[...] + swap * sin_ref[...]).astype(BF16).astype(F32)
            q_buf[latent // 128, pl.ds(quad * 4 + 2 * k, tok, stride=heads)] = rot
            q_buf[latent // 128, pl.ds(quad * 4 + 2 * k + 1, tok, stride=heads)] = pltpu.roll(rot, rope, 1)

    place = lax.broadcasted_iota(jnp.int32, (heads, cache_hbm.shape[2]), 1)

    @pl.loop(0, n_group)
    def _(group):
        slot = lax.rem(group, RING)
        ring_copy(group, slot).wait()
        @pl.loop(0, GROUP // SUB)
        def _(sub):
            for k in range(SUB):
                at = sub * SUB + k
                t = group * GROUP + at
                rows = pl.ds(pl.multiple_of(t * heads, heads), heads)
                q_cat = jnp.concatenate([q_buf[j, rows] for j in range(latent // 128 + 1)], axis=1)[:, :span].astype(BF16)
                score = dot_n(q_cat, ring[slot, at]) * scale
                score = jnp.where(place < lens_ref[t], score, -1e30)
                top = jnp.max(score, axis=1, keepdims=True)
                num = jnp.exp(score - top)
                p_buf[at] = (num * (1.0 / jnp.sum(num, axis=1, keepdims=True))).astype(BF16)

        @pl.loop(0, GROUP // SUB)
        def _(sub):
            for k in range(SUB):
                at = sub * SUB + k
                rows = pl.ds(pl.multiple_of((group * GROUP + at) * heads, heads), heads)
                o_lat = dot_t(p_buf[at], ring[slot, at, pl.ds(0, latent)])
                for j in range(latent // 128):
                    o_buf[j, rows] = o_lat[:, j * 128:(j + 1) * 128]

        @pl.when(group + RING < n_group)
        def _():
            ring_copy(group + RING, slot).start()


    uv_cp.wait()
    if with_far:
        own_in.wait()
        own_out.start()

    @pl.loop(0, heads, unroll=8)
    def _(h):
        o_lat = jnp.concatenate([o_buf[j, pl.ds(h, tok, stride=heads)] for j in range(latent // 128)], axis=1).astype(BF16)
        vals = dot_n(o_lat, uv[h]).astype(BF16)
        ov_buf[:, pl.ds(pl.multiple_of(h * nope, nope), nope)] = vals

    wo_cp.wait()
    for off in range(0, hid, 512):
        cols = pl.ds(off, 512)
        att = dot_n(ov_buf[...], wo[:, cols])
        h_ref[:, cols] = (x_ref[:, cols].astype(F32) + att).astype(BF16)
    u_ref[:, pl.ds(0, hid)] = norm(h_ref[...].astype(F32))
    if with_table:
        u_ref[:, pl.ds(hid, 128)] = route_table(route_ref[...].T[:tok], top_k)
    if with_far:
        own_out.wait()
        for cp in far_copies:
            cp.wait()


def pack_route(ids, wts):
    tok, top_k = ids.shape
    pad = ((0, 8 - top_k), (0, 128 - tok))
    return jnp.concatenate([jnp.pad(ids.T.astype(F32), pad), jnp.pad(wts.T, pad)], axis=0)


def att_call(x, cache, kv_lens, cos, sin, w_q, w_uk, w_uv, w_o, route=None, far=None):
    tok, hid = x.shape
    heads, nope, latent = w_uk.shape
    val_dim = w_uv.shape[2]
    assert val_dim == nope
    qk_dim = w_q.shape[2]
    pos = cache.shape[1]
    span = cache.shape[2]
    with_table = route is not None
    vmem, hbm = pl.BlockSpec(memory_space=pltpu.VMEM), pl.BlockSpec(memory_space=pl.ANY)
    smem = pl.BlockSpec(memory_space=pltpu.SMEM)
    with_far = far is not None
    top_k = route[0].shape[1] if with_table else 0
    args = [kv_lens, x, cos, sin] + ([pack_route(*route)] if with_table else []) + ([far] if with_far else [])
    args += [w_q.transpose(1, 2, 0), w_uk, w_uv, w_o.reshape(heads * val_dim, hid), cache.transpose(0, 2, 1)]
    width = hid + (128 if with_table else 0)
    out_shape = [jax.ShapeDtypeStruct((tok, hid), BF16), jax.ShapeDtypeStruct((tok, width), BF16)]
    out_specs = [vmem, vmem]
    extra, params = [], {}
    if with_far:
        n_ep = far.shape[0] // SLOT_CAP
        out_shape.append(jax.ShapeDtypeStruct(far.shape, BF16))
        out_specs.append(hbm)
        dma = pltpu.SemaphoreType.DMA
        extra = [pltpu.VMEM((SLOT_CAP, hid), BF16), dma((2,)), dma((n_ep,)), dma((n_ep,))]
        params = {'collective_id': 2, 'has_side_effects': True}
    return pl.pallas_call(
        functools.partial(att_kernel, top_k, with_far),
        out_shape=out_shape,
        in_specs=[smem] + [vmem] * (4 if with_table else 3) + [hbm] * (6 if with_far else 5),
        out_specs=out_specs,
        scratch_shapes=[
            pltpu.VMEM((heads, qk_dim, hid), BF16),
            pltpu.VMEM((heads, nope, latent), BF16),
            pltpu.VMEM((heads, latent, val_dim), BF16),
            pltpu.VMEM((heads * val_dim, hid), BF16),
            pltpu.VMEM((RING, GROUP, span, pos), BF16),
            pltpu.VMEM((tok, hid), BF16),
            pltpu.VMEM((latent // 128 + 1, tok * heads, 128), F32),
            pltpu.VMEM((latent // 128, tok * heads, 128), F32),
            pltpu.VMEM((tok, heads * val_dim), BF16),
            pltpu.VMEM((GROUP, heads, pos), BF16),
            pltpu.SemaphoreType.DMA((7,)),
            pltpu.SemaphoreType.DMA((RING,)),
        ] + extra,
        compiler_params=pltpu.CompilerParams(vmem_limit_bytes=VMEM_LIMIT, **params),
        cost_estimate=pl.CostEstimate(flops=6 * tok * hid * 3072, bytes_accessed=54_000_000, transcendentals=0),
        name='latent_attention',
    )(*args)


def rope_tables(kv_lens, rope):
    lane = jnp.arange(128)
    inv_freq = 10000.0 ** (-2.0 * (lane % (rope // 2)).astype(F32) / rope)
    angle = kv_lens.astype(F32)[:, None] * inv_freq[None, :]
    return jnp.cos(angle), jnp.where(lane % rope < rope // 2, -1.0, 1.0) * jnp.sin(angle)


def solution(mesh):
    assert mesh.shape['tp'] == 2 and mesh.shape['ep'] == 8
    rows_spec = P(FLAT_AXES, None)
    cube_spec = P(FLAT_AXES, None, None)
    whole_spec = P(None, None, None)
    col_split = P(None, 'tp')
    row_split = P('tp', None)
    in_specs = (rows_spec, cube_spec, cube_spec, P(FLAT_AXES), rows_spec, rows_spec,
                whole_spec, whole_spec, whole_spec, whole_spec, whole_spec, whole_spec, whole_spec, whole_spec,
                col_split, col_split, row_split, col_split, col_split, row_split,
                cube_spec, cube_spec, cube_spec)

    def body(hidden_in, cache0, cache1, kv_lens, route_ids, route_wts, att0_q, att0_uk, att0_uv, att0_o, att1_q, att1_uk, att1_uv, att1_o, ffn0_gate, ffn0_up, ffn0_down, ffn1_gate, ffn1_up, ffn1_down, exp_gate, exp_up, exp_down):
        cos, sin = rope_tables(kv_lens, att0_q.shape[2] - att0_uk.shape[1])
        h_zero, u_ext = att_call(hidden_in, cache0, kv_lens, cos, sin, att0_q, att0_uk, att0_uv, att0_o, route=(route_ids, route_wts))
        f_zero, near, far, theirs = dense_call(u_ext, h_zero, ffn0_gate.T, ffn0_up.T, ffn0_down, expert=(exp_gate, exp_up, exp_down))
        h_one, u_one, back = att_call(f_zero, cache1, kv_lens, cos, sin, att1_q, att1_uk, att1_uv, att1_o, far=far)
        out, = dense_call(u_one, h_one, ffn1_gate.T, ffn1_up.T, ffn1_down, mix=(near, far, back, u_ext, theirs))
        return out.astype(BF16)

    return jax.shard_map(body, mesh=mesh, in_specs=in_specs, out_specs=rows_spec, check_vma=False)
```

```python
import functools

import jax
import jax.numpy as jnp
import numpy as np
from jax import lax
from jax.experimental import pallas as pl
from jax.experimental.pallas import tpu as pltpu
from jax.sharding import PartitionSpec as P

FLAT_AXES = ('tp', 'ep')
MESH = pl.DeviceIdType.MESH
F32, BF16 = jnp.float32, jnp.bfloat16
SLOT_CAP = 72
VMEM_LIMIT = 66_000_000


def dot_t(lhs, rhs):
    return lax.dot_general(lhs, rhs, (((1,), (1,)), ((), ())), preferred_element_type=F32)


def dot_n(lhs, rhs):
    return jnp.dot(lhs, rhs, preferred_element_type=F32)


TILE = 512
COLS = 256


def exchange_copies(src, dst, send_sem, recv_sem, z, e, diagonal):
    y, x, c = e // 4, (e // 2) % 2, e % 2
    copies = []
    for k in range(1, 8):
        if (k >= 6) not in diagonal:
            continue
        peer = lax.rem(y + k // 4, 2) * 4 + lax.rem(x + (k // 2) % 2, 2) * 2 + lax.rem(c + k % 2, 2)
        copies.append(pltpu.make_async_remote_copy(
            src_ref=src.at[pl.ds(pl.multiple_of(peer * SLOT_CAP, 8), SLOT_CAP)],
            dst_ref=dst.at[e] if len(dst.shape) == 3 else dst.at[pl.ds(pl.multiple_of(e * SLOT_CAP, 8), SLOT_CAP)],
            send_sem=send_sem.at[k], recv_sem=recv_sem.at[k], device_id=(z, peer), device_id_type=MESH))
    return copies


def ffn_kernel(with_expert, *refs):
    refs = list(refs)
    u_ref, h_ref, gate_hbm, up_hbm, down_hbm = refs[:5]
    del refs[:5]
    if with_expert:
        eg_hbm, eu_hbm, ed_hbm = refs[:3]
        del refs[:3]
    else:
        near_hbm, far_hbm, back_hbm, u0_ref, their_ref = refs[:5]
        del refs[:5]
    out_ref = refs.pop(0)
    if with_expert:
        near_hbm, far_hbm, their_ref = refs[:3]
        del refs[:3]
    blocks, rows_ref, act_ref, gate_w, up_w, down_w, part_buf, z_out, z_in, d_out, d_in, p_out, p_in = refs[:13]
    w_sem, ex_send, ex_recv, z_send, z_recv, d_send, d_recv, p_send, p_recv, own_sem = refs[13:23]
    if with_expert:
        x_buf, h_buf, e_buf, ew_sem, eo_sem = refs[23:]
    else:
        near_in, far_in, mat_near, mat_far, n_send, n_recv, f_send, f_recv, far_sem = refs[23:]

    tok, hid = h_ref.shape
    ff = gate_w.shape[0]
    n_full, tail = ff // TILE, ff % TILE
    n_col = hid // COLS
    k_main = (ff // 256) * 256

    z = lax.axis_index('tp')
    e = lax.axis_index('ep')
    y, x, c = e // 4, (e // 2) % 2, e % 2
    zn = (1 - z, e)
    cn = (z, e + 1 - 2 * c)
    base = pl.multiple_of(c * ff, 16)

    def tile_copies(step, rows):
        at = pl.multiple_of(step * TILE, TILE)
        return [pltpu.make_async_copy(hbm.at[pl.ds(pl.multiple_of(base + at, 16), rows)], buf.at[pl.ds(at, rows)], w_sem.at[k, step])
                for k, (hbm, buf) in enumerate(((gate_hbm, gate_w), (up_hbm, up_w)))]

    down_cp = pltpu.make_async_copy(down_hbm.at[pl.ds(base, ff)], down_w, w_sem.at[2, 0])
    for step in range(n_full):
        for cp in tile_copies(step, TILE):
            cp.start()
    for cp in tile_copies(n_full, tail):
        cp.start()

    if with_expert:
        me = z * 8 + e
        xn = (z, e + 2 - 4 * x)
        yn = (z, e + 4 - 8 * y)
        peers = (zn, cn, xn, yn)
    else:
        n_ep = near_in.shape[0]
        peers = (zn,) + tuple((z, lax.rem(e + k, n_ep)) for k in range(1, n_ep))
    barrier = pltpu.get_barrier_semaphore()
    for peer in peers:
        pl.semaphore_signal(barrier, inc=1, device_id=peer, device_id_type=MESH)
    pl.semaphore_wait(barrier, len(peers))

    def remote(k, src, dst, peer):
        return pltpu.make_async_remote_copy(src_ref=src, dst_ref=dst, send_sem=ex_send.at[k], recv_sem=ex_recv.at[k],
                                            device_id=peer, device_id_type=MESH)

    if with_expert:
        half = tok // 2
        lo, hi = pl.ds(0, half), pl.ds(half, half)

        def plane(z_at):
            first = z_at * 8
            return (first + e, first + e + 2 - 4 * x, first + e + 4 - 8 * y,
                    first + (1 - y) * 4 + (1 - x) * 2 + c)

        def plane_sends(first, blks, own_src):
            own, xb, yb, db = blks
            return {
                'x': remote(first, own_src, blocks.at[own], xn),
                'y': remote(first + 1, own_src, blocks.at[own], yn),
                'xr': remote(first + 2, blocks.at[yb, hi], blocks.at[yb, hi], xn),
                'yr': remote(first + 3, blocks.at[xb, lo], blocks.at[xb, lo], yn),
                'c0': remote(first + 4, own_src, blocks.at[own], cn),
                'c1': remote(first + 5, blocks.at[xb], blocks.at[xb], cn),
                'c2': remote(first + 6, blocks.at[yb], blocks.at[yb], cn),
                'c3': remote(first + 7, blocks.at[db], blocks.at[db], cn),
            }

        def start_relay(s):
            s['x'].wait_recv()
            s['y'].wait_recv()
            s['xr'].start()
            s['yr'].start()
            s['c1'].start()
            s['c2'].start()

        def start_last(s):
            s['xr'].wait_recv()
            s['yr'].wait_recv()
            s['c3'].start()

        z_blk = (1 - z) * 8 + e
        c_blk = z * 8 + e + 1 - 2 * c
        zc_blk = (1 - z) * 8 + e + 1 - 2 * c
        sa = plane_sends(1, plane(z), u_ref)
        sb = plane_sends(9, plane(1 - z), blocks.at[z_blk])
        z_copy = remote(0, u_ref, blocks.at[me], zn)
        ca_copy, cb_copy = sa['c0'], sb['c0']
        own_cp = pltpu.make_async_copy(u_ref, blocks.at[me], own_sem.at[0])
        own_cp.start()
    else:
        z_blk, c_blk, zc_blk = 0, 1, 2
        z_copy = remote(0, u_ref, blocks.at[0], zn)
        ca_copy = remote(1, u_ref, blocks.at[1], cn)
        cb_copy = remote(2, blocks.at[0], blocks.at[2], cn)
        near_copies = exchange_copies(near_hbm, near_in, n_send, n_recv, z, e, (False, True))
        far_copies = exchange_copies(far_hbm, far_in, f_send, f_recv, z, e, (True,))
        own_cp = pltpu.make_async_copy(near_hbm.at[pl.ds(pl.multiple_of(e * SLOT_CAP, 8), SLOT_CAP)], near_in.at[e], own_sem.at[0])
        far_local = []
        for k in range(6):
            at = lax.rem(y + k // 4, 2) * 4 + lax.rem(x + (k // 2) % 2, 2) * 2 + lax.rem(c + k % 2, 2)
            far_local.append(pltpu.make_async_copy(back_hbm.at[pl.ds(pl.multiple_of(at * SLOT_CAP, 8), SLOT_CAP)], far_in.at[at], far_sem.at[k]))

    lane = lax.broadcasted_iota(jnp.int32, (tok, 128), 1)

    def fill_mix(mat, table_vals):
        vals = table_vals.astype(F32)
        slot = lax.broadcasted_iota(jnp.int32, (tok, SLOT_CAP), 1).astype(F32)
        for k in range(n_ep):
            def column(part):
                return jnp.sum(jnp.where(lane == part * 16 + z * n_ep + k, vals, 0.0), axis=1, keepdims=True)
            hit = slot == column(0)
            for part in range(3):
                mat[k, pl.ds(part * tok, tok)] = jnp.where(hit, column(part + 1), 0.0).astype(BF16)

    z_copy.start()
    ca_copy.start()
    if with_expert:
        sa['x'].start()
        sa['y'].start()
    else:
        for cp in far_copies + near_copies:
            cp.start()
    rows_ref[pl.ds(0, tok)] = u_ref[:, pl.ds(0, hid)]
    ca_copy.wait_recv()
    rows_ref[pl.ds(tok, tok)] = blocks[c_blk, :, pl.ds(0, hid)]

    def swiglu_tile(first, at, rows):
        lhs = rows_ref[pl.ds(first, 2 * tok)]
        gate_val = dot_t(lhs, gate_w[pl.ds(at, rows)])
        up_val = dot_t(lhs, up_w[pl.ds(at, rows)])
        act_ref[pl.ds(first, 2 * tok), pl.ds(at, rows)] = (jax.nn.silu(gate_val) * up_val).astype(BF16)

    @pl.loop(0, n_full)
    def _(step):
        for cp in tile_copies(step, TILE):
            cp.wait()
        swiglu_tile(0, pl.multiple_of(step * TILE, TILE), TILE)

        @pl.when(step == 2)
        def _():
            down_cp.start()

    for cp in tile_copies(n_full, tail):
        cp.wait()
    swiglu_tile(0, n_full * TILE, tail)

    if not with_expert:
        fill_mix(mat_far, their_ref[...])
    z_copy.wait_recv()
    cb_copy.start()
    if with_expert:
        start_relay(sa)
        sb['x'].start()
        sb['y'].start()
    else:
        own_cp.start()
        for cp in far_local:
            cp.start()
    rows_ref[pl.ds(2 * tok, tok)] = blocks[z_blk, :, pl.ds(0, hid)]
    cb_copy.wait_recv()
    rows_ref[pl.ds(3 * tok, tok)] = blocks[zc_blk, :, pl.ds(0, hid)]

    @pl.loop(0, n_full)
    def _(step):
        swiglu_tile(2 * tok, pl.multiple_of(step * TILE, TILE), TILE)

    swiglu_tile(2 * tok, n_full * TILE, tail)

    if with_expert:
        eg, eu, ed = (gate_w.at[pl.ds(0, hid), pl.ds(0, eg_hbm.shape[2])], up_w.at[pl.ds(0, hid), pl.ds(0, eg_hbm.shape[2])],
                      down_w.at[pl.ds(0, ed_hbm.shape[1])])
        eg_cp, eu_cp, ed_cp = (pltpu.make_async_copy(s.at[0], d, ew_sem.at[k])
                               for k, (s, d) in enumerate(((eg_hbm, eg), (eu_hbm, eu), (ed_hbm, ed))))
        eg_cp.start()
        eu_cp.start()
        start_last(sa)

    def link(src, dst, sems, rems, col, peer):
        return pltpu.make_async_remote_copy(src_ref=src.at[col], dst_ref=dst.at[col], send_sem=sems.at[col],
                                            recv_sem=rems.at[col], device_id=peer, device_id_type=MESH)

    def z_link(col):
        return link(z_out, z_in, z_send, z_recv, col, zn)

    def d_link(col):
        return link(d_out, d_in, d_send, d_recv, col, cn)

    def p_link(col):
        return link(p_out, p_in, p_send, p_recv, col, cn)

    def down_tile(first, col):
        cols = pl.ds(pl.multiple_of(col * COLS, COLS), COLS)
        lhs = act_ref.at[pl.ds(first, 2 * tok)]
        val = dot_n(lhs[:, pl.ds(0, k_main)], down_w[pl.ds(0, k_main), cols])
        return val + dot_n(lhs[:, pl.ds(k_main, ff - k_main)], down_w[pl.ds(k_main, ff - k_main), cols])

    def mixed(mat, back, cols):
        val = dot_n(mat[0], back[0, :, cols])
        for k in range(1, n_ep):
            val += dot_n(mat[k], back[k, :, cols])
        return (val[2 * tok:] + val[tok:2 * tok]) + val[:tok]

    def send_z(col):
        d_link(col).wait_recv()
        total = z_out[col] + d_in[col]
        if not with_expert:
            total += mixed(mat_far, far_in, pl.ds(pl.multiple_of(col * COLS, COLS), COLS))
        z_out[col] = total
        z_link(col).start()

    down_cp.wait()
    if not with_expert:
        for cp in far_local:
            cp.wait()
        for cp in far_copies:
            cp.wait_recv()

    @pl.loop(0, n_col)
    def _(col):
        val = down_tile(2 * tok, col)
        z_out[col] = val[:tok]
        d_out[col] = val[tok:]
        d_link(col).start()

        @pl.when(col >= 2)
        def _():
            send_z(col - 2)

    send_z(n_col - 2)
    send_z(n_col - 1)
    if not with_expert:
        fill_mix(mat_near, u0_ref[:, pl.ds(hid, 128)])

    @pl.loop(0, n_col)
    def _(col):
        val = down_tile(0, col)
        part_buf[col] = val[:tok]
        p_out[col] = val[tok:]
        p_link(col).start()

    if with_expert:
        ed_cp.start()
        own_cp.wait()
        eg_cp.wait()
        eu_cp.wait()
        their_ref[...] = blocks[z_blk, :, pl.ds(hid, 128)]
        slot_id = lax.broadcasted_iota(jnp.int32, (tok, 2 * SLOT_CAP), 1).astype(F32)
        q_rows = 4 * SLOT_CAP

        def eo_copy(it, buf, dst, yq):
            return pltpu.make_async_copy(e_buf.at[buf], dst.at[pl.ds(pl.multiple_of(yq * q_rows, q_rows), q_rows)], eo_sem.at[buf])

        @pl.loop(0, 4)
        def _(it):
            @pl.when(it == 0)
            def _():
                sa['c1'].wait_recv()

            @pl.when(it == 1)
            def _():
                start_relay(sb)
                sa['c2'].wait_recv()
                sa['c3'].wait_recv()

            @pl.when(it == 2)
            def _():
                start_last(sb)
                sb['c1'].wait_recv()

            @pl.when(it == 3)
            def _():
                sb['c2'].wait_recv()
                sb['c3'].wait_recv()

            zq = lax.rem(z + it // 2, 2)
            yq = lax.rem(y + it, 2)
            buf = lax.rem(it, 2)
            for pair in range(2):
                acc = None
                for k in range(2):
                    blk = zq * 8 + yq * 4 + pair * 2 + k
                    table = blocks[blk, :, pl.ds(hid, 128)].astype(F32)
                    rank = jnp.sum(jnp.where(lane == me, table, 0.0), axis=1, keepdims=True)
                    want = jnp.where(rank >= 0.0, rank + k * SLOT_CAP, -1.0)
                    hot = jnp.where(slot_id == want, 1.0, 0.0).astype(BF16)
                    got = lax.dot_general(hot, blocks[blk, :, pl.ds(0, hid)], (((0,), (0,)), ((), ())),
                                          preferred_element_type=F32)
                    acc = got if acc is None else acc + got
                x_buf[pl.ds(pair * 2 * SLOT_CAP, 2 * SLOT_CAP)] = acc.astype(BF16)
            for off, width in ((0, 512), (512, 512), (1024, 384)):
                gate_val = dot_n(x_buf[...], eg[:, pl.ds(off, width)])
                up_val = dot_n(x_buf[...], eu[:, pl.ds(off, width)])
                h_buf[:, pl.ds(off, width)] = (jax.nn.silu(gate_val) * up_val).astype(BF16)

            @pl.when(it == 0)
            def _():
                ed_cp.wait()

            @pl.when(it >= 2)
            def _():
                eo_copy(it, buf, near_hbm, yq).wait()

            for off in range(0, hid, 512):
                e_buf[buf, :, pl.ds(off, 512)] = dot_n(h_buf[...], ed[:, pl.ds(off, 512)]).astype(BF16)

            @pl.when(it < 2)
            def _():
                eo_copy(it, buf, near_hbm, yq).start()

            @pl.when(it >= 2)
            def _():
                eo_copy(it, buf, far_hbm, yq).start()

        eo_copy(0, 0, far_hbm, 0).wait()
        eo_copy(0, 1, far_hbm, 0).wait()

    if not with_expert:
        own_cp.wait()
        for cp in near_copies:
            cp.wait_recv()
        zero_wt = jnp.sum(jnp.where((lane >= 64) & (lane < 67), u0_ref[:, pl.ds(hid, 128)].astype(F32), 0.0), axis=1, keepdims=True)

    @pl.loop(0, n_col)
    def _(col):
        p_link(col).wait()
        d_link(col).wait_send()
        z_link(col).wait()
        cols = pl.ds(pl.multiple_of(col * COLS, COLS), COLS)
        total = h_ref[:, cols].astype(F32) + ((part_buf[col] + p_in[col]) + z_in[col])
        if not with_expert:
            total += mixed(mat_near, near_in, cols) + zero_wt * u0_ref[:, cols].astype(F32)
        out_ref[:, cols] = total.astype(out_ref.dtype)

    z_copy.wait_send()
    if with_expert:
        for s in (sa, sb):
            for cp in s.values():
                cp.wait_send()
    else:
        ca_copy.wait_send()
        cb_copy.wait_send()
        for cp in far_copies + near_copies:
            cp.wait_send()


def dense_call(u, h, w_gate_t, w_up_t, w_down, expert=None, mix=None):
    tok, hid = h.shape
    ff = w_gate_t.shape[0] // 2
    width = u.shape[1]
    with_expert = expert is not None
    vmem, hbm = pl.BlockSpec(memory_space=pltpu.VMEM), pl.BlockSpec(memory_space=pl.ANY)
    n_col = hid // COLS
    n_step = ff // TILE + 1
    args = [u, h, w_gate_t, w_up_t, w_down]
    in_specs = [vmem, vmem, hbm, hbm, hbm]
    out_shape = [jax.ShapeDtypeStruct((tok, hid), BF16)]
    out_specs = [vmem]
    n_ex = 17 if with_expert else 3
    dma = pltpu.SemaphoreType.DMA
    scratch = [pltpu.VMEM((16 if with_expert else 3, tok, width), BF16), pltpu.VMEM((4 * tok, hid), BF16),
               pltpu.VMEM((4 * tok, n_step * TILE), BF16),
               pltpu.VMEM((ff, hid), BF16), pltpu.VMEM((ff, hid), BF16), pltpu.VMEM((ff, hid), BF16)]
    scratch += [pltpu.VMEM((n_col, tok, COLS), F32)] * 7
    scratch += [dma((3, n_step)), dma((n_ex,)), dma((n_ex,))] + [dma((n_col,))] * 6 + [dma((1,))]
    flops = 2 * 2 * tok * hid * ff * 6
    if with_expert:
        inner = expert[0].shape[2]
        args += list(expert)
        in_specs += [hbm, hbm, hbm]
        out_shape += [jax.ShapeDtypeStruct((8 * SLOT_CAP, hid), BF16)] * 2 + [jax.ShapeDtypeStruct((tok, 128), BF16)]
        out_specs += [hbm, hbm, vmem]
        scratch += [pltpu.VMEM((4 * SLOT_CAP, hid), BF16), pltpu.VMEM((4 * SLOT_CAP, inner), BF16),
                    pltpu.VMEM((2, 4 * SLOT_CAP, hid), BF16), dma((3,)), dma((2,))]
        flops += 2 * 16 * SLOT_CAP * hid * inner * 3
    else:
        args += list(mix)
        in_specs += [hbm, hbm, hbm, vmem, vmem]
        n_ep = mix[0].shape[0] // SLOT_CAP
        scratch += [pltpu.VMEM((n_ep, SLOT_CAP, hid), BF16)] * 2 + [pltpu.VMEM((n_ep, 3 * tok, SLOT_CAP), BF16)] * 2
        scratch += [dma((n_ep,))] * 4 + [dma((6,))]
    return pl.pallas_call(
        functools.partial(ffn_kernel, with_expert),
        out_shape=out_shape, in_specs=in_specs, out_specs=out_specs, scratch_shapes=scratch,
        compiler_params=pltpu.CompilerParams(collective_id=0 if with_expert else 1, has_side_effects=True,
                                             vmem_limit_bytes=VMEM_LIMIT),
        cost_estimate=pl.CostEstimate(flops=flops, bytes_accessed=6 * hid * ff, transcendentals=0),
        name='dense_expert' if with_expert else 'dense',
    )(*args)


GROUP = 16
RING = 4
SUB = 16


def route_table(route, top_k):
    tok = route.shape[0]
    lane = lax.broadcasted_iota(jnp.int32, (tok, 128), 1)
    lane16 = lax.rem(lane, 16).astype(F32)
    weight = jnp.zeros((tok, 128), F32)
    member = jnp.zeros((tok, 128), F32)
    for j in range(top_k):
        col = route[:, j:j + 1]
        hit = ((lane < 64) & (col == lane16)) | ((lane >= 64) & (col >= 16.0))
        weight += jnp.where(hit, route[:, 8 + j:9 + j], 0.0)
        member += jnp.where(hit, 1.0, 0.0)
    before = lax.broadcasted_iota(jnp.int32, (tok, tok), 0) > lax.broadcasted_iota(jnp.int32, (tok, tok), 1)
    rank = dot_n(jnp.where(before, 1.0, 0.0).astype(BF16), member.astype(BF16))
    rank = jnp.where(member > 0.0, rank, -1.0)
    first = weight.astype(BF16).astype(F32)
    second = (weight - first).astype(BF16).astype(F32)
    third = (weight - first) - second
    part = jnp.where(lane < 64, lane // 16 - 1, lane - 64)
    term = jnp.where(part == 0, first, jnp.where(part == 1, second, third))
    return jnp.where(lane < 16, rank, jnp.where(lane < 67, term, 0.0)).astype(BF16)


def att_kernel(top_k, with_far, *refs):
    refs = list(refs)
    with_table = top_k > 0
    lens_ref, x_ref = refs[:2]
    del refs[:2]
    if with_table:
        route_ref = refs.pop(0)
    else:
        cos_ref, sin_ref = refs[:2]
        del refs[:2]
    far_hbm = refs.pop(0) if with_far else None
    wq_hbm, uk_hbm, uv_hbm, wo_hbm, cache_hbm, h_ref, u_ref = refs[:7]
    del refs[:7]
    back_hbm = refs.pop(0) if with_far else None
    if with_table:
        cos_ref, sin_ref = refs[:2]
        del refs[:2]
    wq, uk, uv, wo, ring, xn_buf, q_buf, o_buf, ov_buf, p_buf, w_sem, ring_sem = refs[:12]
    if with_far:
        own_buf, own_sem, f_send, f_recv = refs[12:]
    tok, hid = x_ref.shape
    heads, nope, latent = uk.shape
    qk_dim = wq.shape[1]
    rope = qk_dim - nope
    scale = qk_dim ** -0.5
    n_group = tok // GROUP
    span = latent + rope

    def head_copy(quad):
        return pltpu.make_async_copy(wq_hbm.at[pl.ds(quad * 4, 4)], wq.at[pl.ds(quad * 4, 4)], w_sem.at[quad])

    def ring_copy(group, slot):
        return pltpu.make_async_copy(cache_hbm.at[pl.ds(group * GROUP, GROUP)], ring.at[slot], ring_sem.at[slot])

    uk_cp = pltpu.make_async_copy(uk_hbm, uk, w_sem.at[4])
    uv_cp = pltpu.make_async_copy(uv_hbm, uv, w_sem.at[5])
    wo_cp = pltpu.make_async_copy(wo_hbm, wo, w_sem.at[6])
    head_copy(0).start()
    uk_cp.start()
    for quad in range(1, heads // 4):
        head_copy(quad).start()

    if with_far:
        z = lax.axis_index('tp')
        e = lax.axis_index('ep')
        n_ep = far_hbm.shape[0] // SLOT_CAP
        barrier = pltpu.get_barrier_semaphore()
        for k in range(1, n_ep):
            pl.semaphore_signal(barrier, inc=1, device_id=(z, lax.rem(e + k, n_ep)), device_id_type=MESH)
        pl.semaphore_wait(barrier, n_ep - 1)
        far_copies = exchange_copies(far_hbm, back_hbm, f_send, f_recv, z, e, (False,))
        for cp in far_copies:
            cp.start()
        own_rows = pl.ds(pl.multiple_of(e * SLOT_CAP, 8), SLOT_CAP)
        own_in = pltpu.make_async_copy(far_hbm.at[own_rows], own_buf, own_sem.at[0])
        own_out = pltpu.make_async_copy(own_buf, back_hbm.at[own_rows], own_sem.at[1])
        own_in.start()

    def norm(val):
        return (val * lax.rsqrt(jnp.mean(val * val, axis=-1, keepdims=True) + 1e-6)).astype(BF16)

    xn_buf[...] = norm(x_ref[...].astype(F32))
    if with_table:
        angle = route_ref[...].T[:tok, 6:7] * route_ref[pl.ds(14, 1)]
        cos_ref[...] = jnp.cos(angle)
        sin_ref[...] = route_ref[pl.ds(15, 1)] * jnp.sin(angle)
    uk_cp.wait()
    lane = lax.broadcasted_iota(jnp.int32, (tok, 128), 1)
    first_half = lax.rem(lane, rope) < rope // 2

    @pl.loop(0, heads // 4)
    def _(quad):
        head_copy(quad).wait()

        @pl.when(quad == 0)
        def _():
            for group in range(RING):
                ring_copy(group, group).start()

        @pl.when(quad == 3)
        def _():
            uv_cp.start()
            wo_cp.start()

        w_nope = jnp.concatenate([wq[quad * 4 + k, pl.ds(0, nope)] for k in range(4)], axis=0)
        w_rope = jnp.concatenate([wq[quad * 4 + k, pl.ds(nope, rope)] for k in range(4)], axis=0)
        q_nope = dot_t(xn_buf[...], w_nope).astype(BF16)
        q_rope = dot_t(xn_buf[...], w_rope).astype(BF16).astype(F32)
        for k in range(4):
            q_lat = dot_n(q_nope[:, k * nope:(k + 1) * nope], uk[quad * 4 + k]).astype(BF16).astype(F32)
            for j in range(latent // 128):
                q_buf[j, pl.ds(quad * 4 + k, tok, stride=heads)] = q_lat[:, j * 128:(j + 1) * 128]
        for k in range(2):
            val = q_rope[:, k * 128:(k + 1) * 128]
            swap = jnp.where(first_half, pltpu.roll(val, 128 - rope // 2, 1), pltpu.roll(val, rope // 2, 1))
            rot = (val * cos_ref[...] + swap * sin_ref[...]).astype(BF16).astype(F32)
            q_buf[latent // 128, pl.ds(quad * 4 + 2 * k, tok, stride=heads)] = rot
            q_buf[latent // 128, pl.ds(quad * 4 + 2 * k + 1, tok, stride=heads)] = pltpu.roll(rot, rope, 1)

    place = lax.broadcasted_iota(jnp.int32, (heads, cache_hbm.shape[2]), 1)

    @pl.loop(0, n_group)
    def _(group):
        slot = lax.rem(group, RING)
        ring_copy(group, slot).wait()
        @pl.loop(0, GROUP // SUB)
        def _(sub):
            for k in range(SUB):
                at = sub * SUB + k
                t = group * GROUP + at
                rows = pl.ds(pl.multiple_of(t * heads, heads), heads)
                q_cat = jnp.concatenate([q_buf[j, rows] for j in range(latent // 128 + 1)], axis=1)[:, :span].astype(BF16)
                score = dot_n(q_cat, ring[slot, at]) * scale
                score = jnp.where(place < lens_ref[t], score, -1e30)
                top = jnp.max(score, axis=1, keepdims=True)
                num = jnp.exp(score - top)
                p_buf[at] = (num * (1.0 / jnp.sum(num, axis=1, keepdims=True))).astype(BF16)

        @pl.loop(0, GROUP // SUB)
        def _(sub):
            for k in range(SUB):
                at = sub * SUB + k
                rows = pl.ds(pl.multiple_of((group * GROUP + at) * heads, heads), heads)
                o_lat = dot_t(p_buf[at], ring[slot, at, pl.ds(0, latent)])
                for j in range(latent // 128):
                    o_buf[j, rows] = o_lat[:, j * 128:(j + 1) * 128]

        @pl.when(group + RING < n_group)
        def _():
            ring_copy(group + RING, slot).start()


    uv_cp.wait()
    if with_far:
        own_in.wait()
        own_out.start()

    @pl.loop(0, heads, unroll=8)
    def _(h):
        o_lat = jnp.concatenate([o_buf[j, pl.ds(h, tok, stride=heads)] for j in range(latent // 128)], axis=1).astype(BF16)
        vals = dot_n(o_lat, uv[h]).astype(BF16)
        ov_buf[:, pl.ds(pl.multiple_of(h * nope, nope), nope)] = vals

    wo_cp.wait()
    for off in range(0, hid, 512):
        cols = pl.ds(off, 512)
        att = dot_n(ov_buf[...], wo[:, cols])
        h_ref[:, cols] = (x_ref[:, cols].astype(F32) + att).astype(BF16)
    u_ref[:, pl.ds(0, hid)] = norm(h_ref[...].astype(F32))
    if with_table:
        u_ref[:, pl.ds(hid, 128)] = route_table(route_ref[...].T[:tok], top_k)
    if with_far:
        own_out.wait()
        for cp in far_copies:
            cp.wait()


def pack_route(ids, wts, kv_lens, rope):
    tok, top_k = ids.shape
    lane = np.arange(128)
    freq = 10000.0 ** (-2.0 * (lane % (rope // 2)) / rope)
    sign = np.where(lane % rope < rope // 2, -1.0, 1.0)
    pad = ((0, 0), (0, 128 - tok))
    top = jnp.pad(jnp.concatenate([ids.T, kv_lens[None, :], kv_lens[None, :]], axis=0).astype(F32), pad)
    return jnp.concatenate([top, jnp.pad(wts.T, pad), jnp.asarray(np.stack([freq, sign]), F32)], axis=0)


def att_call(x, cache, kv_lens, w_q, w_uk, w_uv, w_o, route=None, rotary=None, far=None):
    tok, hid = x.shape
    heads, nope, latent = w_uk.shape
    val_dim = w_uv.shape[2]
    assert val_dim == nope
    qk_dim = w_q.shape[2]
    pos = cache.shape[1]
    span = cache.shape[2]
    with_table = route is not None
    vmem, hbm = pl.BlockSpec(memory_space=pltpu.VMEM), pl.BlockSpec(memory_space=pl.ANY)
    smem = pl.BlockSpec(memory_space=pltpu.SMEM)
    with_far = far is not None
    top_k = route[0].shape[1] if with_table else 0
    args = [kv_lens, x] + ([pack_route(*route, kv_lens, w_q.shape[2] - w_uk.shape[1])] if with_table else list(rotary)) + ([far] if with_far else [])
    args += [w_q.transpose(1, 2, 0), w_uk, w_uv, w_o.reshape(heads * val_dim, hid), cache.transpose(0, 2, 1)]
    width = hid + (128 if with_table else 0)
    out_shape = [jax.ShapeDtypeStruct((tok, hid), BF16), jax.ShapeDtypeStruct((tok, width), BF16)]
    out_specs = [vmem, vmem]
    extra, params = [], {}
    if with_table:
        out_shape += [jax.ShapeDtypeStruct((tok, 128), F32)] * 2
        out_specs += [vmem, vmem]
    if with_far:
        n_ep = far.shape[0] // SLOT_CAP
        out_shape.append(jax.ShapeDtypeStruct(far.shape, BF16))
        out_specs.append(hbm)
        dma = pltpu.SemaphoreType.DMA
        extra = [pltpu.VMEM((SLOT_CAP, hid), BF16), dma((2,)), dma((n_ep,)), dma((n_ep,))]
        params = {'collective_id': 2, 'has_side_effects': True}
    return pl.pallas_call(
        functools.partial(att_kernel, top_k, with_far),
        out_shape=out_shape,
        in_specs=[smem] + [vmem] * (2 if with_table else 3) + [hbm] * (6 if with_far else 5),
        out_specs=out_specs,
        scratch_shapes=[
            pltpu.VMEM((heads, qk_dim, hid), BF16),
            pltpu.VMEM((heads, nope, latent), BF16),
            pltpu.VMEM((heads, latent, val_dim), BF16),
            pltpu.VMEM((heads * val_dim, hid), BF16),
            pltpu.VMEM((RING, GROUP, span, pos), BF16),
            pltpu.VMEM((tok, hid), BF16),
            pltpu.VMEM((latent // 128 + 1, tok * heads, 128), F32),
            pltpu.VMEM((latent // 128, tok * heads, 128), F32),
            pltpu.VMEM((tok, heads * val_dim), BF16),
            pltpu.VMEM((GROUP, heads, pos), BF16),
            pltpu.SemaphoreType.DMA((7,)),
            pltpu.SemaphoreType.DMA((RING,)),
        ] + extra,
        compiler_params=pltpu.CompilerParams(vmem_limit_bytes=VMEM_LIMIT, **params),
        cost_estimate=pl.CostEstimate(flops=6 * tok * hid * 3072, bytes_accessed=54_000_000, transcendentals=0),
        name='latent_attention',
    )(*args)


def solution(mesh):
    assert mesh.shape['tp'] == 2 and mesh.shape['ep'] == 8
    rows_spec = P(FLAT_AXES, None)
    cube_spec = P(FLAT_AXES, None, None)
    whole_spec = P(None, None, None)
    col_split = P(None, 'tp')
    row_split = P('tp', None)
    in_specs = (rows_spec, cube_spec, cube_spec, P(FLAT_AXES), rows_spec, rows_spec,
                whole_spec, whole_spec, whole_spec, whole_spec, whole_spec, whole_spec, whole_spec, whole_spec,
                col_split, col_split, row_split, col_split, col_split, row_split,
                cube_spec, cube_spec, cube_spec)

    def body(hidden_in, cache0, cache1, kv_lens, route_ids, route_wts, att0_q, att0_uk, att0_uv, att0_o, att1_q, att1_uk, att1_uv, att1_o, ffn0_gate, ffn0_up, ffn0_down, ffn1_gate, ffn1_up, ffn1_down, exp_gate, exp_up, exp_down):
        h_zero, u_ext, cos, sin = att_call(hidden_in, cache0, kv_lens, att0_q, att0_uk, att0_uv, att0_o, route=(route_ids, route_wts))
        f_zero, near, far, theirs = dense_call(u_ext, h_zero, ffn0_gate.T, ffn0_up.T, ffn0_down, expert=(exp_gate, exp_up, exp_down))
        h_one, u_one, back = att_call(f_zero, cache1, kv_lens, att1_q, att1_uk, att1_uv, att1_o, rotary=(cos, sin), far=far)
        out, = dense_call(u_one, h_one, ffn1_gate.T, ffn1_up.T, ffn1_down, mix=(near, far, back, u_ext, theirs))
        return out

    return jax.shard_map(body, mesh=mesh, in_specs=in_specs, out_specs=rows_spec, check_vma=False)
```
